512 devices in a mesh: ep: 128 (over x, z, core), dp: 4 (over y).
Axes of the slice: x: 4, y: 4, z: 16, core: 2. Of those that a mesh axis runs over, the one named last changes fastest.
Arguments:
- tokens: bfloat16 [2048, 3584], P('ep'), may hold values from -6 to 6
- expert_ids: int32 [2048, 8], P('ep'), may hold values from 0 to 127, all different within a row; in each aligned block of 16 rows (0 to 15, 16 to 31, ...) at most 4 rows name the same one
- route_logits: float32 [2048, 8], P('ep'), may hold values from -8 to 8
- expert_gate: bfloat16 [128, 3584, 1024], P('ep', None, 'dp'), may hold values from -0.09375 to 0.09375
- expert_up: bfloat16 [128, 3584, 1024], P('ep', None, 'dp'), may hold values from -0.09375 to 0.09375
- expert_down: bfloat16 [128, 1024, 3584], P('ep', 'dp'), may hold values from -0.1875 to 0.1875
Outputs:
- mixed: bfloat16 [2048, 3584], P(('ep', 'dp'))
The draws below stay inside these ranges and needn't reach their ends.
Inputs may be any that keep to these rules, and one draw needn't show every extreme that they name: `expert_ids`: each row names 8 different experts of 0 to 127 and every expert is named by some row. Within the rows of one index of ep (aligned blocks of 16 rows) no expert is named more than 4 times, and some block names one expert exactly 4 times. Loads are heavy-tailed: a few experts take several times the mean.
All inputs are finite; a program needn't handle non-finite values.
Results may differ from the reference program's by a relative error of at most 0.015.
Values may be sent and summed in bfloat16 or wider, within the bound.
A program may use at most 64 MiB of HBM per device.

```python
import math
import jax
import jax.numpy as jnp
import numpy as np
from jax import lax

D = 3584
FF = 1024
TOP = 8
TOK_EP = 16
EXPERTS = 128
TOKENS = 2048
CAP = 4


def block_levels(own_key, shape, cuts, smallest, largest):
    gain = 1.0
    for position, parts in cuts:
        steps = jax.random.uniform(jax.random.fold_in(jax.random.fold_in(own_key, 6), position), (parts,), jnp.float32, smallest / len(cuts), largest / len(cuts))
        gain = gain * jnp.repeat(jnp.exp(steps), shape[position] // parts).reshape((-1,) + (1,) * (len(shape) - 1 - position))
    return gain


def deal_out(key, own, number, rows, amount, top, reach, lean):
    sequence = jax.random.permutation(key, amount)
    heavy_load, usual = load_shares(amount, rows * top, reach, lean, True), load_shares(amount, rows * top, reach, lean, False)
    places = jnp.arange(amount)

    def named(tallies, rotation):
        used = int((tallies > 0).sum())
        fixed = max(1, used // 4)
        shifted = fixed + (places - fixed + rotation * (used - fixed)) % max(1, amount - fixed)
        return jnp.zeros((amount,), jnp.int32).at[sequence[jnp.where(places < fixed, places, shifted)]].set(jnp.asarray(tallies, jnp.int32))

    tallies = jnp.where(number % 4 == 0, named(heavy_load, number // 4), named(usual, number - number // 4 - 1))
    mixed = jax.random.permutation(jax.random.fold_in(own, 3), amount)
    donor, taker = mixed[0:amount // 2 * 2:2], mixed[1:amount // 2 * 2:2]
    margin = jnp.minimum(tallies[donor] - 1, reach - tallies[taker]) // 2
    margin = jnp.where((donor == sequence[0]) | (taker == sequence[0]) | (tallies[taker] == 0), 0, jnp.maximum(margin, 0))
    shifted = jax.random.randint(jax.random.fold_in(own, 4), (amount // 2,), 0, 1 << 20) % (margin + 1)
    tallies = tallies.at[donor].add(-shifted).at[taker].add(shifted)
    members = jnp.searchsorted(jnp.cumsum(tallies), jnp.arange(rows * top), side="right").astype(jnp.int32)
    listing = members.reshape(top, rows).T
    listing = listing[jax.random.permutation(jax.random.fold_in(own, 1), rows)]
    rotation = jax.random.randint(jax.random.fold_in(own, 2), (rows, 1), 0, top)
    return jnp.take_along_axis(listing, (jnp.arange(top)[None, :] + rotation) % top, axis=1)


def load_shares(count, total, bound, slope, full):
    loads = [(1 << 20) // math.isqrt(standing ** slope) + 1 for standing in range(1, count + 1)]
    largest = bound if full else min(bound, max(-(-total // count), total * loads[0] // sum(loads)))
    least = 1 if total - largest >= count - 1 else 0
    given, spare = [largest] + [least] * (count - 1), total - largest - least * (count - 1)
    while spare > 0:
        free = [i for i in range(1, count) if given[i] < largest] or [i for i in range(1, count) if given[i] < bound]
        pool, remaining = sum([loads[i] for i in free]), spare
        for i in free:
            extra = min(bound - given[i], max(1, remaining * loads[i] // pool), spare)
            given[i] = given[i] + extra
            spare = spare - extra
    return np.array(given)


def scatter_about(rng, extent, scale, most, cuts=(), held_as=jnp.bfloat16):
    result = jax.random.normal(rng, extent, jnp.float32) * scale
    if len(cuts) > 0:
        result = block_levels(rng, extent, cuts, -0.22, 0.18) * result
    return jnp.clip(result, min=-most, max=most).astype(held_as)


def setup_inputs(seed: int = 0) -> dict:
    key_of = jax.random.split(jax.random.key(seed), 7)
    tokens = scatter_about(key_of[0], (TOKENS, D), 1.0, 6.0, ((0, 128),))
    expert_ids_keys = jax.random.split(jax.random.fold_in(key_of[1], 1), TOKENS // TOK_EP)
    expert_ids_turns = jax.random.permutation(jax.random.fold_in(key_of[1], 3), TOKENS // TOK_EP)
    expert_ids = jax.vmap(lambda own, number: deal_out(jax.random.fold_in(key_of[1], 2), own, number, TOK_EP, EXPERTS, TOP, CAP, 3))(expert_ids_keys, expert_ids_turns).reshape((TOKENS, TOP))
    route_logits = scatter_about(key_of[2], (TOKENS, TOP), 2.0, 8.0, ((0, 128),), jnp.float32)
    expert_gate = scatter_about(key_of[3], (EXPERTS, D, FF), D ** -0.5, 0.09375, ((0, 128), (2, 4)))
    expert_up = scatter_about(key_of[4], (EXPERTS, D, FF), D ** -0.5, 0.09375, ((0, 128), (2, 4)))
    expert_down = scatter_about(key_of[5], (EXPERTS, FF, D), FF ** -0.5, 0.1875, ((0, 128), (1, 4)))
    return dict(tokens=tokens, expert_ids=expert_ids, route_logits=route_logits, expert_gate=expert_gate, expert_up=expert_up, expert_down=expert_down)


route_scale = 2.5


def expert_rows(rows, w_gate, w_up, w_down):
    gate = jnp.dot(rows, w_gate, preferred_element_type=jnp.float32)
    upper = jnp.dot(rows, w_up, preferred_element_type=jnp.float32)
    hidden = (jax.nn.silu(gate) * upper).astype(jnp.bfloat16)
    return jnp.dot(hidden, w_down, preferred_element_type=jnp.float32).astype(jnp.bfloat16)


def reference(tokens, expert_ids, route_logits, expert_gate, expert_up, expert_down):
    token_count, width = tokens.shape
    top = expert_ids.shape[1]
    experts = expert_gate.shape[0]
    flat_ids = expert_ids.reshape(-1).astype(jnp.int32)
    slots = flat_ids.shape[0]
    block_rows = 64
    counts = jnp.zeros((experts,), jnp.int32).at[flat_ids].add(1).astype(jnp.int32)
    padded = (((counts + block_rows - 1) // block_rows) * block_rows).astype(jnp.int32)
    pad_start = (jnp.cumsum(padded) - padded).astype(jnp.int32)
    seg_start = (jnp.cumsum(counts) - counts).astype(jnp.int32)
    sorted_slots = jnp.argsort(flat_ids, stable=True).astype(jnp.int32)
    sorted_ids = flat_ids[sorted_slots]
    within = (jnp.arange(slots, dtype=jnp.int32) - seg_start[sorted_ids]).astype(jnp.int32)
    target = (pad_start[sorted_ids] + within).astype(jnp.int32)
    nblocks = (slots + experts * (block_rows - 1)) // block_rows + 1
    row_token = jnp.full((nblocks * block_rows,), token_count, jnp.int32).at[target].set((sorted_slots // top).astype(jnp.int32))
    pad_end = pad_start + padded
    block_start = jnp.arange(nblocks, dtype=jnp.int32) * block_rows
    block_expert = jnp.sum((pad_end[None, :] <= block_start[:, None]).astype(jnp.int32), axis=1)
    block_expert = jnp.minimum(block_expert, experts - 1).astype(jnp.int32)
    extended = jnp.concatenate([tokens, jnp.zeros((1, width), tokens.dtype)], axis=0)

    def one_block(inputs):
        block_index, expert = inputs
        picks = lax.dynamic_slice_in_dim(row_token, (block_index * block_rows).astype(jnp.int32), block_rows, 0)
        return expert_rows(extended[picks], expert_gate[expert], expert_up[expert], expert_down[expert])

    outputs = lax.map(one_block, (jnp.arange(nblocks, dtype=jnp.int32), block_expert))
    outputs = outputs.reshape(nblocks * block_rows, width)
    slot_target = jnp.zeros((slots,), jnp.int32).at[sorted_slots].set(target)
    slot_values = outputs[slot_target].reshape(token_count, top, width)
    scores = jax.nn.sigmoid(route_logits)
    weights = route_scale * scores / jnp.sum(scores, axis=1, keepdims=True)
    routed = jnp.sum(weights[:, :, None] * slot_values.astype(jnp.float32), axis=1)
    return routed.astype(jnp.bfloat16)
```

```python
import functools

import jax
import jax.numpy as jnp
from jax import lax
from jax.experimental import pallas as pl
from jax.experimental.pallas import tpu as pltpu
from jax.sharding import PartitionSpec as P

MESH = pl.DeviceIdType.MESH
F32 = jnp.float32
BF16 = jnp.bfloat16
ROUTE_SCALE = 2.5
CAP = 4
CHIPS_X = 4
CORES = 2
N_DP = 4


def kernel(
    nx, nz, ids_ref, logits_ref, tok_ref, wg_hbm, wu_hbm, wd_hbm, out_ref,
    wg, wu, wd, zbuf, swbuf, xsend, ybuf, obuf, r1buf, r2buf, xret, rbuf, part,
    zs1, zs2, zr1, zr2, fbuf,
    w_sem, zag_s, zag_r, x_s, x_r, y1_s, y1_r, y2_s, y2_r, p1_s, p1_r, p2_s, p2_r,
    b_s, b_r, zrs_s, zrs_r, f_s, f_r,
):
    nc, ny = CORES, N_DP
    tile = tok_ref.shape[0]
    width = tok_ref.shape[1]
    quarter = width // ny
    top = ids_ref.shape[1]
    col = nz * tile
    slots = nz * CAP
    group = nc * slots
    half = group // 2
    offsets = {1: (0,), 2: (0, 1), 4: (0, 1, 3, 2)}[nx]
    inverse = [offsets.index((nx - o) % nx) for o in offsets]
    ep = lax.axis_index("ep")
    y = lax.axis_index("dp")
    c = lax.rem(ep, nc)
    z = lax.rem(lax.div(ep, nc), nz)
    x = lax.div(ep, nc * nz)

    def dev(x_, y_, z_, c_):
        return (((x_ * nz + z_) * nc + c_), y_)

    def at_x(r):
        return lax.rem(x + offsets[r], nx)

    def at_y(o):
        return lax.rem(y + (o + ny), ny)

    def at_z(o):
        return lax.rem(z + (o + 2 * nz), nz)

    def rows(start, size):
        if isinstance(start, int):
            return pl.ds(start, size)
        return pl.ds(pl.multiple_of(start, size), size)

    sends = []

    def send(src, dst, ssem, rsem, device):
        copy = pltpu.make_async_remote_copy(
            src_ref=src, dst_ref=dst, send_sem=ssem, recv_sem=rsem,
            device_id=device, device_id_type=MESH,
        )
        copy.start()
        sends.append(copy)
        return copy

    def arrived(ref, rsem):
        pltpu.make_async_remote_copy(
            src_ref=ref, dst_ref=ref, send_sem=rsem, recv_sem=rsem,
            device_id=dev(x, y, z, 1 - c), device_id_type=MESH,
        ).wait_recv()

    loads = [
        pltpu.make_async_copy(s.at[0], d, w_sem.at[i])
        for i, (s, d) in enumerate(((wg_hbm, wg), (wu_hbm, wu), (wd_hbm, wd)))
    ]
    for load in loads:
        load.start()

    scores = 1.0 / (1.0 + jnp.exp(-logits_ref[...]))
    wts = ROUTE_SCALE * scores / jnp.sum(scores, axis=1, keepdims=True)
    lane = lax.broadcasted_iota(jnp.int32, (top, 128), 1)
    sub = lax.broadcasted_iota(jnp.int32, (top, 128), 0)
    put_id = (lane == sub).astype(BF16)
    put_w = (lane == sub + top).astype(BF16)
    meta = jnp.dot(
        ids_ref[...].astype(F32).astype(BF16), put_id, preferred_element_type=F32
    ) + jnp.dot(wts.astype(BF16), put_w, preferred_element_type=F32)
    own = rows(z * tile, tile)
    zbuf[own, 0:quarter] = tok_ref[:, pl.ds(pl.multiple_of(y * quarter, 128), quarter)]
    zbuf[own, quarter : quarter + 128] = meta.astype(BF16)

    barrier = pltpu.get_barrier_semaphore()
    peers = [dev(x, y, at_z(o), c) for o in (1, -1, 2, -2)]
    peers += [dev(at_x(r), y, z, c_) for r in range(1, nx) for c_ in range(nc)]
    peers += [dev(x, y, z, 1 - c)]
    peers += [dev(x, at_y(o), z, c) for o in range(1, ny)]
    for peer in peers:
        pl.semaphore_signal(barrier, inc=1, device_id=peer, device_id_type=MESH)
    pl.semaphore_wait(barrier, len(peers))

    steps = nz // 4

    def zsem(d, k, hop):
        return ((0 if d > 0 else 1) * steps + (k - 1)) * 2 + (hop - 1)

    def zblock(o):
        return zbuf.at[rows(at_z(o) * tile, tile), :]

    pending = {}
    for k in range(1, steps + 1):
        for d in (1, -1):
            if k > 1:
                pending.pop((d, k - 1, 2)).wait_recv()
            for hop in (1, 2):
                if hop == 2 and d < 0 and k == steps:
                    continue
                block = zblock(-d * 2 * (k - 1))
                i = zsem(d, k, hop)
                pending[(d, k, hop)] = send(
                    block, block, zag_s.at[i], zag_r.at[i], dev(x, y, at_z(d * hop), c)
                )
    for copy in pending.values():
        copy.wait_recv()

    pick = (
        lax.broadcasted_iota(jnp.int32, (2 * top, 128), 0)
        == lax.broadcasted_iota(jnp.int32, (2 * top, 128), 1)
    ).astype(BF16)
    by_token = lax.dot_general(
        pick, zbuf[:, quarter : quarter + 128], (((1,), (1,)), ((), ())),
        preferred_element_type=F32,
    )
    lanes = nx * nc
    j = lax.broadcasted_iota(jnp.int32, (lanes, col), 0)
    jr, jc = lax.div(j, nc), lax.rem(j, nc)
    off = jnp.zeros_like(jr)
    for r, o in enumerate(offsets):
        off = jnp.where(jr == r, o, off)
    expert = ((lax.rem(x + off, nx) * nz + z) * nc + jc).astype(F32)
    named = jnp.zeros((lanes, col), F32)
    weight = jnp.zeros((lanes, col), F32)
    for k in range(top):
        hit = by_token[k : k + 1, :] == expert
        named = jnp.where(hit, 1.0, named)
        weight = jnp.where(hit, by_token[top + k : top + k + 1, :], weight)
    t_row = lax.broadcasted_iota(jnp.int32, (col, col), 0)
    t_col = lax.broadcasted_iota(jnp.int32, (col, col), 1)
    before = ((t_row < t_col) & (lax.div(t_row, tile) == lax.div(t_col, tile))).astype(BF16)
    rank = jnp.dot(named.astype(BF16), before, preferred_element_type=F32)
    rank = jnp.where(named > 0.5, rank, -1.0)
    s_row = lax.broadcasted_iota(jnp.int32, (slots, col), 0)
    s_col = lax.broadcasted_iota(jnp.int32, (slots, col), 1)
    in_block = lax.div(s_row, CAP) == lax.div(s_col, tile)
    want = jnp.where(in_block, lax.rem(s_row, CAP).astype(F32), -2.0)

    for r in tuple(range(nx - 1, 0, -1)) + (0,):
        chosen = []
        for c_ in range(nc):
            i = r * nc + c_
            hit = rank[i : i + 1, :] == want
            chosen.append(jnp.where(hit, 1.0, 0.0).astype(BF16))
            swbuf[rows(i * slots, slots), :] = jnp.where(hit, weight[i : i + 1, :], 0.0).astype(BF16)
        base = r * group
        xsend[rows(base, group), :] = jnp.dot(
            jnp.concatenate(chosen, axis=0), zbuf[:, 0:quarter], preferred_element_type=F32
        ).astype(BF16)
        land = ybuf.at[y, rows((inverse[r] * nc + c) * slots, slots), :]
        if r > 0:
            for c_ in range(nc):
                i = r * nc + c_
                send(
                    xsend.at[rows(i * slots, slots), :], land, x_s.at[i],
                    x_r.at[inverse[r] * nc + c], dev(at_x(r), y, z, c_),
                )
        else:
            other = 1 - c
            send(
                xsend.at[rows(other * slots, slots), :], land, x_s.at[0], x_r.at[c],
                dev(x, y, z, other),
            )
            ybuf[y, rows(c * slots, slots), :] = xsend[rows(c * slots, slots), :]

    y_one, y_two, p_one, p_two = {}, {}, {}, {}
    for g in range(nx):
        if g == 0:
            arrived(ybuf.at[y, rows((1 - c) * slots, slots), :], x_r.at[1 - c])
        else:
            for c_ in range(nc):
                i = g * nc + c_
                arrived(ybuf.at[y, rows(i * slots, slots), :], x_r.at[i])
        block = ybuf.at[y, rows(g * group, group), :]
        for n, d in enumerate((1, -1)):
            y_one[g, d] = send(
                block, block, y1_s.at[n * nx + g], y1_r.at[n * nx + g], dev(x, at_y(d), z, c)
            )

    def forward(g):
        for n, d in enumerate((1, -1)):
            y_one[g, d].wait_recv()
        for n, d in enumerate((1, -1)):
            block = ybuf.at[at_y(-d), rows(g * group + n * half, half), :]
            y_two[g, d] = send(
                block, block, y2_s.at[n * nx + g], y2_r.at[n * nx + g], dev(x, at_y(d), z, c)
            )

    def compute(g):
        for d in (1, -1):
            y_two[g, d].wait_recv()
        if g == 0:
            for load in loads:
                load.wait()
        here = rows(g * group, group)
        gate = jnp.zeros((group, wg.shape[1]), F32)
        upper = jnp.zeros((group, wg.shape[1]), F32)
        for q in range(ny):
            piece = ybuf[q, here, :]
            deep = pl.ds(q * quarter, quarter)
            gate += jnp.dot(piece, wg[deep, :], preferred_element_type=F32)
            upper += jnp.dot(piece, wu[deep, :], preferred_element_type=F32)
        hidden = (gate / (1.0 + jnp.exp(-gate)) * upper).astype(BF16)
        for q in range(ny):
            obuf[q, here, :] = jnp.dot(
                hidden, wd[:, q * quarter : (q + 1) * quarter], preferred_element_type=F32
            ).astype(BF16)
        for n, d in enumerate((1, -1)):
            p_one[g, d] = send(
                obuf.at[at_y(2), rows(g * group + n * half, half), :],
                r1buf.at[n, rows(g * half, half), :],
                p1_s.at[n * nx + g], p1_r.at[n * nx + g], dev(x, at_y(d), z, c),
            )

    def reduce_one(g):
        for n, d in enumerate((1, -1)):
            p_one[g, d].wait_recv()
            here = rows(g * group + n * half, half)
            q = at_y(d)
            total = obuf[q, here, :].astype(F32) + r1buf[n, rows(g * half, half), :].astype(F32)
            obuf[q, here, :] = total.astype(BF16)
        for n, d in enumerate((1, -1)):
            p_two[g, d] = send(
                obuf.at[at_y(d), rows(g * group, group), :],
                r2buf.at[n, rows(g * group, group), :],
                p2_s.at[n * nx + g], p2_r.at[n * nx + g], dev(x, at_y(d), z, c),
            )

    def reduce_two(g):
        for d in (1, -1):
            p_two[g, d].wait_recv()
        here = rows(g * group, group)
        total = obuf[y, here, :].astype(F32) + r2buf[0, here, :].astype(F32)
        xret[here, :] = (total + r2buf[1, here, :].astype(F32)).astype(BF16)
        land = rbuf.at[rows((inverse[g] * nc + c) * slots, slots), :]
        if g > 0:
            for c_ in range(nc):
                i = g * nc + c_
                send(
                    xret.at[rows(i * slots, slots), :], land, b_s.at[i],
                    b_r.at[inverse[g] * nc + c], dev(at_x(g), y, z, c_),
                )
        else:
            other = 1 - c
            send(
                xret.at[rows(other * slots, slots), :], land, b_s.at[0], b_r.at[c],
                dev(x, y, z, other),
            )
            rbuf[rows(c * slots, slots), :] = xret[rows(c * slots, slots), :]

    def combine(g):
        r = inverse[g]
        if g == 0:
            arrived(rbuf.at[rows((1 - c) * slots, slots), :], b_r.at[1 - c])
        else:
            for c_ in range(nc):
                i = r * nc + c_
                arrived(rbuf.at[rows(i * slots, slots), :], b_r.at[i])
        here = rows(r * group, group)
        term = lax.dot_general(
            swbuf[here, :], rbuf[here, :], (((0,), (0,)), ((), ())), preferred_element_type=F32
        )
        if g == 0:
            part[...] = term
        else:
            part[...] += term

    stages = (forward, compute, reduce_one, reduce_two, combine)
    for i in range(nx + len(stages) - 1):
        for n, stage in enumerate(stages):
            if 0 <= i - n < nx:
                stage(i - n)

    reach = nz // 2

    def block_of(o):
        return part[rows(at_z(o) * tile, tile), :]

    def zslot(d, k):
        return (0 if d > 0 else 1) * steps + (k - 1)

    got = {}

    def zsend(d, k, hop, value):
        src, dst = (zs1, zr1) if hop == 1 else (zs2, zr2)
        i, n = zsem(d, k, hop), zslot(d, k)
        src[n] = value.astype(BF16)
        got[d, k, hop] = (
            send(src.at[n], dst.at[n], zrs_s.at[i], zrs_r.at[i], dev(x, y, at_z(d * hop), c)), dst, n
        )

    def zget(d, k):
        total = None
        for hop in (1, 2):
            if (d, k, hop) in got:
                copy, dst, n = got[d, k, hop]
                copy.wait_recv()
                value = dst[n].astype(F32)
                total = value if total is None else total + value
        return total

    zsend(1, 1, 2, block_of(reach))
    for k in range(1, steps + 1):
        for d in (1, -1):
            zsend(d, k, 1, block_of(d * (reach + 1 - 2 * k)))
    for k in range(1, steps):
        for d in (1, -1):
            zsend(d, k + 1, 2, block_of(d * (reach - 2 * k)) + zget(d, k))
    final = (block_of(0) + zget(1, steps) + zget(-1, steps)).astype(BF16)

    fbuf[y] = final
    tails = []
    for o in range(1, ny):
        tails.append(
            send(fbuf.at[y], fbuf.at[y], f_s.at[o], f_r.at[o], dev(x, at_y(o), z, c))
        )
    mine = out_ref.shape[0]
    sel = (
        lax.broadcasted_iota(jnp.int32, (8, tile), 1)
        == lax.broadcasted_iota(jnp.int32, (8, tile), 0) + y * mine
    ).astype(BF16)
    for tail in tails:
        tail.wait_recv()
    for q in range(ny):
        full = jnp.dot(sel, fbuf[q], preferred_element_type=F32)
        out_ref[:, q * quarter : (q + 1) * quarter] = full[0:mine, :].astype(BF16)
    for copy in sends:
        copy.wait_send()


def on_device(tokens, expert_ids, route_logits, expert_gate, expert_up, expert_down):
    n_ep, ny = lax.axis_size("ep"), N_DP
    nx, nc = CHIPS_X, CORES
    nz = n_ep // (nx * nc)
    tile, width = tokens.shape
    hidden = expert_gate.shape[2]
    quarter = width // ny
    col, slots = nz * tile, nz * CAP
    every = nx * nc * slots
    steps = nz // 4
    dma = pltpu.SemaphoreType.DMA
    vmem = pl.BlockSpec(memory_space=pltpu.VMEM)
    hbm = pl.BlockSpec(memory_space=pl.ANY)
    flops = 6 * every * width * hidden
    return pl.pallas_call(
        functools.partial(kernel, nx, nz),
        out_shape=jax.ShapeDtypeStruct((tile // ny, width), BF16),
        in_specs=[vmem, vmem, vmem, hbm, hbm, hbm],
        out_specs=vmem,
        scratch_shapes=[
            pltpu.VMEM((width, hidden), BF16),
            pltpu.VMEM((width, hidden), BF16),
            pltpu.VMEM((hidden, width), BF16),
            pltpu.VMEM((col, quarter + 128), BF16),
            pltpu.VMEM((every, col), BF16),
            pltpu.VMEM((every, quarter), BF16),
            pltpu.VMEM((ny, every, quarter), BF16),
            pltpu.VMEM((ny, every, quarter), BF16),
            pltpu.VMEM((2, every // 2, quarter), BF16),
            pltpu.VMEM((2, every, quarter), BF16),
            pltpu.VMEM((every, quarter), BF16),
            pltpu.VMEM((every, quarter), BF16),
            pltpu.VMEM((col, quarter), F32),
            pltpu.VMEM((2 * steps, tile, quarter), BF16),
            pltpu.VMEM((2 * steps, tile, quarter), BF16),
            pltpu.VMEM((2 * steps, tile, quarter), BF16),
            pltpu.VMEM((2 * steps, tile, quarter), BF16),
            pltpu.VMEM((ny, tile, quarter), BF16),
            dma((3,)),
            dma((4 * steps,)), dma((4 * steps,)),
            dma((nx * nc,)), dma((nx * nc,)),
            dma((2 * nx,)), dma((2 * nx,)),
            dma((2 * nx,)), dma((2 * nx,)),
            dma((2 * nx,)), dma((2 * nx,)),
            dma((2 * nx,)), dma((2 * nx,)),
            dma((nx * nc,)), dma((nx * nc,)),
            dma((4 * steps,)), dma((4 * steps,)),
            dma((ny,)), dma((ny,)),
        ],
        compiler_params=pltpu.CompilerParams(
            collective_id=0, has_side_effects=True, vmem_limit_bytes=56 * 1024 * 1024
        ),
        cost_estimate=pl.CostEstimate(flops=flops, bytes_accessed=8 << 20, transcendentals=0),
    )(expert_ids, route_logits, tokens, expert_gate, expert_up, expert_down)


def solution(mesh):
    placed = (
        P("ep", None),
        P("ep", None),
        P("ep", None),
        P("ep", None, "dp"),
        P("ep", None, "dp"),
        P("ep", "dp", None),
    )
    return jax.shard_map(
        on_device, mesh=mesh, in_specs=placed, out_specs=P(("ep", "dp"), None), check_vma=False
    )
```

```python
import functools

import jax
import jax.numpy as jnp
from jax import lax
from jax.experimental import pallas as pl
from jax.experimental.pallas import tpu as pltpu
from jax.sharding import PartitionSpec as P

MESH = pl.DeviceIdType.MESH
F32 = jnp.float32
BF16 = jnp.bfloat16
ROUTE_SCALE = 2.5
CAP = 4
CHIPS_X = 4
CORES = 2
N_DP = 4


def kernel(
    nx, nz, ids_ref, logits_ref, tok_hbm, wg_hbm, wu_hbm, wd_hbm, out_ref,
    wg, wu, wd, zbuf, swbuf, xsend, ybuf, obuf, r1buf, r2buf, xret, rbuf, part,
    zs1, zs2, zr1, zr2, fsend, frecv,
    w_sem, zag_s, zag_r, x_s, x_r, y1_s, y1_r, y2_s, y2_r, p1_s, p1_r, p2_s, p2_r,
    b_s, b_r, zrs_s, zrs_r, f_s, f_r,
):
    nc, ny = CORES, N_DP
    tile, width = tok_hbm.shape
    quarter = width // ny
    top = ids_ref.shape[0]
    col = nz * tile // 2
    near_blocks = nz // 2
    slots = near_blocks * CAP
    pair = 2 * nc * slots
    each = nx * nc * slots
    hp = pair // 2
    pairs = nx // 2
    offsets = {2: (0, 1), 4: (0, 1, 3, 2)}[nx]
    ep = lax.axis_index("ep")
    y = lax.axis_index("dp")
    c = lax.rem(ep, nc)
    z = lax.rem(lax.div(ep, nc), nz)
    x = lax.div(ep, nc * nz)

    def dev(x_, y_, z_, c_):
        return (((x_ * nz + z_) * nc + c_), y_)

    def to_x(g):
        return lax.rem(x + (nx - offsets[g]), nx)

    def from_x(g):
        return lax.rem(x + offsets[g], nx)

    def at_y(o):
        return lax.rem(y + (o + ny), ny)

    def at_z(o):
        return lax.rem(z + (o + nz), nz)

    def place(o):
        return ((o + nz // 4) % nz) * tile

    def rows(start, size):
        if isinstance(start, int):
            return pl.ds(start, size)
        return pl.ds(pl.multiple_of(start, size), size)

    def base(h, g, c_):
        return h * each + (g * nc + c_) * slots

    sends = []

    def send(src, dst, ssem, rsem, device):
        copy = pltpu.make_async_remote_copy(
            src_ref=src, dst_ref=dst, send_sem=ssem, recv_sem=rsem,
            device_id=device, device_id_type=MESH,
        )
        copy.start()
        sends.append(copy)
        return copy

    def arrived(ref, rsem):
        pltpu.make_async_remote_copy(
            src_ref=ref, dst_ref=ref, send_sem=rsem, recv_sem=rsem,
            device_id=dev(x, y, z, 1 - c), device_id_type=MESH,
        ).wait_recv()

    own = pl.ds(place(0), tile)
    mine = pltpu.make_async_copy(
        tok_hbm.at[:, pl.ds(pl.multiple_of(y * quarter, 128), quarter)],
        zbuf.at[own, pl.ds(0, quarter)], w_sem.at[3],
    )
    mine.start()
    scores = 1.0 / (1.0 + jnp.exp(-logits_ref[...]))
    wts = ROUTE_SCALE * scores / jnp.sum(scores, axis=0, keepdims=True)
    lane = lax.broadcasted_iota(jnp.int32, (top, 128), 1)
    sub = lax.broadcasted_iota(jnp.int32, (top, 128), 0)
    put_id = (lane == sub).astype(BF16)
    put_w = (lane == sub + top).astype(BF16)
    across = (((0,), (0,)), ((), ()))
    meta = lax.dot_general(
        ids_ref[...].astype(F32).astype(BF16), put_id, across, preferred_element_type=F32
    ) + lax.dot_general(wts.astype(BF16), put_w, across, preferred_element_type=F32)
    zbuf[own, quarter : quarter + 128] = meta.astype(BF16)

    barrier = pltpu.get_barrier_semaphore()
    peers = [dev(x, y, at_z(o), c) for o in (1, -1, 2, -2)]
    peers += [dev(from_x(g), y, z, c_) for g in range(1, nx) for c_ in range(nc)]
    peers += [dev(x, y, z, 1 - c)]
    peers += [dev(x, at_y(o), z, c) for o in range(1, ny)]
    for peer in peers:
        pl.semaphore_signal(barrier, inc=1, device_id=peer, device_id_type=MESH)

    loads = [
        pltpu.make_async_copy(s.at[0], d, w_sem.at[i])
        for i, (s, d) in enumerate(((wg_hbm, wg), (wu_hbm, wu), (wd_hbm, wd)))
    ]
    for load in loads:
        load.start()
    mine.wait()
    pl.semaphore_wait(barrier, len(peers))

    steps = nz // 4

    def zsem(d, k, hop):
        return ((0 if d > 0 else 1) * steps + (k - 1)) * 2 + (hop - 1)

    gathers = {}

    def gather_send(k, d):
        o = -d * 2 * (k - 1)
        for hop in (2, 1):
            if hop == 2 and d < 0 and k == steps:
                continue
            i = zsem(d, k, hop)
            gathers[k, d, hop] = send(
                zbuf.at[pl.ds(place(o), tile), :], zbuf.at[pl.ds(place(o - d * hop), tile), :],
                zag_s.at[i], zag_r.at[i], dev(x, y, at_z(d * hop), c),
            )

    def gather_wait(k, d, hop):
        if (k, d, hop) in gathers:
            gathers.pop((k, d, hop)).wait_recv()

    def gather_step(k):
        for d in (1, -1):
            gather_wait(k, d, 2)
            if k < steps:
                gather_send(k + 1, d)

    def routes(h):
        pick = (
            lax.broadcasted_iota(jnp.int32, (2 * top, 128), 0)
            == lax.broadcasted_iota(jnp.int32, (2 * top, 128), 1)
        ).astype(BF16)
        by_token = lax.dot_general(
            pick, zbuf[h * col : (h + 1) * col, quarter : quarter + 128],
            (((1,), (1,)), ((), ())), preferred_element_type=F32,
        )
        lanes = nx * nc
        j = lax.broadcasted_iota(jnp.int32, (lanes, col), 0)
        jg, jc = lax.div(j, nc), lax.rem(j, nc)
        off = jnp.zeros_like(jg)
        for g, o in enumerate(offsets):
            off = jnp.where(jg == g, nx - o, off)
        expert = ((lax.rem(x + off, nx) * nz + z) * nc + jc).astype(F32)
        named = jnp.zeros((lanes, col), F32)
        weight = jnp.zeros((lanes, col), F32)
        for k in range(top):
            hit = by_token[k : k + 1, :] == expert
            named = jnp.where(hit, 1.0, named)
            weight = jnp.where(hit, by_token[top + k : top + k + 1, :], weight)
        t_row = lax.broadcasted_iota(jnp.int32, (col, col), 0)
        t_col = lax.broadcasted_iota(jnp.int32, (col, col), 1)
        before = ((t_row < t_col) & (lax.div(t_row, tile) == lax.div(t_col, tile))).astype(BF16)
        rank = jnp.dot(named.astype(BF16), before, preferred_element_type=F32)
        return jnp.where(named > 0.5, rank, -1.0), weight

    s_row = lax.broadcasted_iota(jnp.int32, (slots, col), 0)
    s_col = lax.broadcasted_iota(jnp.int32, (slots, col), 1)
    in_block = lax.div(s_row, CAP) == lax.div(s_col, tile)
    want = jnp.where(in_block, lax.rem(s_row, CAP).astype(F32), -2.0)

    def x_index(h, g, c_):
        return (h * nx + g) * nc + c_

    def select(h, g, rank, weight):
        chosen = []
        for c_ in range(nc):
            i = g * nc + c_
            hit = rank[i : i + 1, :] == want
            chosen.append(jnp.where(hit, 1.0, 0.0).astype(BF16))
            swbuf[pl.ds(base(h, g, c_), slots), :] = jnp.where(
                hit, weight[i : i + 1, :], 0.0
            ).astype(BF16)
        xsend[pl.ds(base(h, g, 0), nc * slots), :] = jnp.dot(
            jnp.concatenate(chosen, axis=0), zbuf[h * col : (h + 1) * col, 0:quarter],
            preferred_element_type=F32,
        ).astype(BF16)
        land = ybuf.at[y, rows(base(h, g, c), slots), :]
        if g > 0:
            for c_ in range(nc):
                send(
                    xsend.at[pl.ds(base(h, g, c_), slots), :], land, x_s.at[x_index(h, g, c_)],
                    x_r.at[x_index(h, g, c)], dev(to_x(g), y, z, c_),
                )
        else:
            other = 1 - c
            send(
                xsend.at[rows(base(h, g, other), slots), :], land, x_s.at[x_index(h, g, 0)],
                x_r.at[x_index(h, g, c)], dev(x, y, z, other),
            )
            here = rows(base(h, g, c), slots)
            ybuf[y, here, :] = xsend[here, :]

    def x_wait(h, g):
        if g == 0:
            arrived(ybuf.at[y, rows(base(h, 0, 1 - c), slots), :], x_r.at[x_index(h, 0, 1 - c)])
        else:
            for c_ in range(nc):
                arrived(ybuf.at[y, pl.ds(base(h, g, c_), slots), :], x_r.at[x_index(h, g, c_)])

    y_one, y_two, p_one, p_two = {}, {}, {}, {}

    def index(h, p, n):
        return (n * 2 + h) * pairs + p

    def spread(h, p):
        x_wait(h, 2 * p)
        x_wait(h, 2 * p + 1)
        block = ybuf.at[y, pl.ds(h * each + p * pair, pair), :]
        for n, d in enumerate((1, -1)):
            i = index(h, p, n)
            y_one[h, p, d] = send(block, block, y1_s.at[i], y1_r.at[i], dev(x, at_y(d), z, c))

    def forward(h, p):
        for n, d in enumerate((1, -1)):
            y_one[h, p, d].wait_recv()
            block = ybuf.at[at_y(-d), pl.ds(h * each + p * pair + n * hp, hp), :]
            i = index(h, p, n)
            y_two[h, p, d] = send(block, block, y2_s.at[i], y2_r.at[i], dev(x, at_y(d), z, c))

    def compute(h, p):
        for d in (1, -1):
            y_two[h, p, d].wait_recv()
        here = pl.ds(h * each + p * pair, pair)
        gate = jnp.zeros((pair, wg.shape[1]), F32)
        upper = jnp.zeros((pair, wg.shape[1]), F32)
        for q in range(ny):
            piece = ybuf[q, here, :]
            deep = pl.ds(q * quarter, quarter)
            gate += jnp.dot(piece, wg[deep, :], preferred_element_type=F32)
            upper += jnp.dot(piece, wu[deep, :], preferred_element_type=F32)
        hidden = (gate / (1.0 + jnp.exp(-gate)) * upper).astype(BF16)
        for q in range(ny):
            obuf[q, here, :] = jnp.dot(
                hidden, wd[:, q * quarter : (q + 1) * quarter], preferred_element_type=F32
            ).astype(BF16)

    def give_one(h, p):
        for n, d in enumerate((1, -1)):
            i = index(h, p, n)
            p_one[h, p, d] = send(
                obuf.at[at_y(2), pl.ds(h * each + p * pair + n * hp, hp), :],
                r1buf.at[n, pl.ds((h * pairs + p) * hp, hp), :],
                p1_s.at[i], p1_r.at[i], dev(x, at_y(d), z, c),
            )

    def give_two(h, p):
        for n, d in enumerate((1, -1)):
            p_one[h, p, d].wait_recv()
            here = pl.ds(h * each + p * pair + n * hp, hp)
            q = at_y(d)
            got = r1buf[n, pl.ds((h * pairs + p) * hp, hp), :]
            obuf[q, here, :] = (obuf[q, here, :].astype(F32) + got.astype(F32)).astype(BF16)
            i = index(h, p, n)
            here = pl.ds(h * each + p * pair, pair)
            p_two[h, p, d] = send(
                obuf.at[q, here, :], r2buf.at[n, here, :],
                p2_s.at[i], p2_r.at[i], dev(x, at_y(d), z, c),
            )

    def give_back(h, p):
        for d in (1, -1):
            p_two[h, p, d].wait_recv()
        here = pl.ds(h * each + p * pair, pair)
        total = obuf[y, here, :].astype(F32) + r2buf[0, here, :].astype(F32)
        xret[here, :] = (total + r2buf[1, here, :].astype(F32)).astype(BF16)
        for g in (2 * p + 1, 2 * p):
            land = rbuf.at[rows(base(h, g, c), slots), :]
            if g > 0:
                for c_ in range(nc):
                    send(
                        xret.at[pl.ds(base(h, g, c_), slots), :], land, b_s.at[x_index(h, g, c_)],
                        b_r.at[x_index(h, g, c)], dev(from_x(g), y, z, c_),
                    )
            else:
                other = 1 - c
                send(
                    xret.at[rows(base(h, g, other), slots), :], land, b_s.at[x_index(h, g, 0)],
                    b_r.at[x_index(h, g, c)], dev(x, y, z, other),
                )
                here = rows(base(h, g, c), slots)
                rbuf[here, :] = xret[here, :]

    def combine(h, p, first):
        for g in (2 * p, 2 * p + 1):
            if g == 0:
                arrived(rbuf.at[rows(base(h, 0, 1 - c), slots), :], b_r.at[x_index(h, 0, 1 - c)])
            else:
                for c_ in range(nc):
                    arrived(rbuf.at[pl.ds(base(h, g, c_), slots), :], b_r.at[x_index(h, g, c_)])
        here = pl.ds(h * each + p * pair, pair)
        term = lax.dot_general(
            swbuf[here, :], rbuf[here, :], across, preferred_element_type=F32
        )
        dest = pl.ds(h * col, col)
        if first:
            part[dest, :] = term
        else:
            part[dest, :] += term

    reach = nz // 2
    got = {}

    def block_of(o):
        return part[pl.ds(place(o), tile), :]

    def zsend(d, k, hop, value):
        src, dst = (zs1, zr1) if hop == 1 else (zs2, zr2)
        i, n = zsem(d, k, hop), (0 if d > 0 else 1) * steps + (k - 1)
        src[n] = value.astype(BF16)
        got[d, k, hop] = (
            send(src.at[n], dst.at[n], zrs_s.at[i], zrs_r.at[i], dev(x, y, at_z(d * hop), c)), dst, n
        )

    def zget(d, k):
        total = None
        for hop in (1, 2):
            if (d, k, hop) in got:
                copy, dst, n = got[d, k, hop]
                copy.wait_recv()
                value = dst[n].astype(F32)
                total = value if total is None else total + value
        return total

    def own_hop(k):
        for d in (1, -1):
            zsend(d, k, 1, block_of(d * (reach + 1 - 2 * k)))

    def next_hop(k):
        for d in (1, -1):
            zsend(d, k + 1, 2, block_of(d * (reach - 2 * k)) + zget(d, k))

    near, far = 0, 1
    mid = steps // 2
    for d in (1, -1):
        gather_send(1, d)
    for k in range(1, mid + 1):
        gather_step(k)
    for k in range(1, mid + 1):
        for d in (1, -1):
            gather_wait(k, d, 1)
    rank, weight = routes(near)
    order = (1, 0) + tuple(range(2, nx))
    for g in order[:2]:
        select(near, g, rank, weight)
    later = list(range(mid + 1, steps + 1))
    for k in later[:-1]:
        gather_step(k)
    for g in order[2:]:
        select(near, g, rank, weight)
    spread(near, 0)
    gather_step(later[-1])
    for k in later:
        for d in (1, -1):
            gather_wait(k, d, 1)
    rank, weight = routes(far)
    for g in order:
        select(far, g, rank, weight)
    for p in range(1, pairs):
        spread(near, p)
    forward(near, 0)
    spread(far, 0)
    for p in range(1, pairs):
        forward(near, p)
    for p in range(1, pairs):
        spread(far, p)
    for load in loads:
        load.wait()
    compute(near, 0)
    forward(far, 0)
    for p in range(1, pairs):
        compute(near, p)
    for p in range(1, pairs):
        forward(far, p)
    for p in range(1, pairs):
        give_one(near, p)
    compute(far, 0)
    give_one(far, 0)
    for p in range(1, pairs):
        compute(far, p)
        give_one(far, p)
    give_one(near, 0)
    back = [(far, p) for p in range(pairs)] + [(near, p) for p in range(pairs - 1, -1, -1)]
    for h, p in back:
        give_two(h, p)
    for p in range(pairs):
        give_back(far, p)
    for p in range(pairs - 1, 0, -1):
        give_back(near, p)
    for p in range(pairs):
        combine(far, p, p == 0)
    zsend(1, 1, 2, block_of(reach))
    for k in range(1, mid + 1):
        own_hop(k)
    give_back(near, 0)
    for k in range(1, mid):
        next_hop(k)
    for p in range(pairs - 1, -1, -1):
        combine(near, p, p == pairs - 1)
    for k in range(mid + 1, steps + 1):
        own_hop(k)
    for k in range(mid, steps):
        next_hop(k)
    final = block_of(0) + zget(1, steps) + zget(-1, steps)

    count = out_ref.shape[0]
    for q in range(ny):
        fsend[q] = final[q * count : (q + 1) * count, :].astype(BF16)
    frecv[y] = fsend[y]
    tails = []
    for o in (2, 1, 3):
        tails.append(
            send(fsend.at[at_y(o)], frecv.at[y], f_s.at[o], f_r.at[o], dev(x, at_y(o), z, c))
        )
    for tail in tails:
        tail.wait_recv()
    for q in range(ny):
        out_ref[:, q * quarter : (q + 1) * quarter] = frecv[q]
    for copy in sends:
        copy.wait_send()


def on_device(tokens, expert_ids, route_logits, expert_gate, expert_up, expert_down):
    n_ep, ny = lax.axis_size("ep"), N_DP
    nx, nc = CHIPS_X, CORES
    nz = n_ep // (nx * nc)
    tile, width = tokens.shape
    hidden = expert_gate.shape[2]
    quarter = width // ny
    col, slots = nz * tile, nz * CAP
    every = nx * nc * slots
    steps = nz // 4
    dma = pltpu.SemaphoreType.DMA
    vmem = pl.BlockSpec(memory_space=pltpu.VMEM)
    hbm = pl.BlockSpec(memory_space=pl.ANY)
    flops = 6 * every * width * hidden
    units = 2 * (nx // 2) * 2
    moves = 2 * nx * nc
    return pl.pallas_call(
        functools.partial(kernel, nx, nz),
        out_shape=jax.ShapeDtypeStruct((tile // ny, width), BF16),
        in_specs=[vmem, vmem, hbm, hbm, hbm, hbm],
        out_specs=vmem,
        scratch_shapes=[
            pltpu.VMEM((width, hidden), BF16),
            pltpu.VMEM((width, hidden), BF16),
            pltpu.VMEM((hidden, width), BF16),
            pltpu.VMEM((col, quarter + 128), BF16),
            pltpu.VMEM((every, col // 2), BF16),
            pltpu.VMEM((every, quarter), BF16),
            pltpu.VMEM((ny, every, quarter), BF16),
            pltpu.VMEM((ny, every, quarter), BF16),
            pltpu.VMEM((2, every // 2, quarter), BF16),
            pltpu.VMEM((2, every, quarter), BF16),
            pltpu.VMEM((every, quarter), BF16),
            pltpu.VMEM((every, quarter), BF16),
            pltpu.VMEM((col, quarter), F32),
            pltpu.VMEM((2 * steps, tile, quarter), BF16),
            pltpu.VMEM((2 * steps, tile, quarter), BF16),
            pltpu.VMEM((2 * steps, tile, quarter), BF16),
            pltpu.VMEM((2 * steps, tile, quarter), BF16),
            pltpu.VMEM((ny, tile // ny, quarter), BF16),
            pltpu.VMEM((ny, tile // ny, quarter), BF16),
            dma((4,)),
            dma((4 * steps,)), dma((4 * steps,)),
            dma((moves,)), dma((moves,)),
            dma((units,)), dma((units,)),
            dma((units,)), dma((units,)),
            dma((units,)), dma((units,)),
            dma((units,)), dma((units,)),
            dma((moves,)), dma((moves,)),
            dma((4 * steps,)), dma((4 * steps,)),
            dma((ny,)), dma((ny,)),
        ],
        compiler_params=pltpu.CompilerParams(
            collective_id=0, has_side_effects=True, vmem_limit_bytes=56 * 1024 * 1024
        ),
        cost_estimate=pl.CostEstimate(flops=flops, bytes_accessed=8 << 20, transcendentals=0),
    )(expert_ids.T, route_logits.T, tokens, expert_gate, expert_up, expert_down)


def solution(mesh):
    placed = (
        P("ep", None),
        P("ep", None),
        P("ep", None),
        P("ep", None, "dp"),
        P("ep", None, "dp"),
        P("ep", "dp", None),
    )
    return jax.shard_map(
        on_device, mesh=mesh, in_specs=placed, out_specs=P(("ep", "dp"), None), check_vma=False
    )
```

```python
import functools

import jax
import jax.numpy as jnp
from jax import lax
from jax.experimental import pallas as pl
from jax.experimental.pallas import tpu as pltpu
from jax.sharding import PartitionSpec as P

MESH = pl.DeviceIdType.MESH
F32 = jnp.float32
BF16 = jnp.bfloat16
ROUTE_SCALE = 2.5
CAP = 4
CHIPS_X = 4
CORES = 2
N_DP = 4


def kernel(
    nx, nz, ids_ref, logits_ref, tok_hbm, wg_hbm, wu_hbm, wd_hbm, out_ref,
    wg, wu, wd, zbuf, swbuf, xsend, ybuf, obuf, r1buf, r2buf, xret, rbuf, rbuf0, part, part0,
    zs1, zs2, zr1, zr2, ws1, ws2, wr1, wr2, fsend, frecv,
    w_sem, zag_s, zag_r, x_s, x_r, y1_s, y1_r, y2_s, y2_r, p1_s, p1_r, p2_s, p2_r,
    b_s, b_r, zrs_s, zrs_r, wrs_s, wrs_r, f_s, f_r,
):
    nc, ny = CORES, N_DP
    tile, width = tok_hbm.shape
    quarter = width // ny
    top = ids_ref.shape[0]
    col = nz * tile // 2
    near_blocks = nz // 2
    slots = near_blocks * CAP
    both = nc * slots
    offsets = {2: (0, 1), 4: (0, 1, 3, 2)}[nx]
    units = {2: ((1,), (0,)), 4: ((1, 2), (3,), (0,))}[nx]
    last = len(units) - 1
    ep = lax.axis_index("ep")
    y = lax.axis_index("dp")
    c = lax.rem(ep, nc)
    z = lax.rem(lax.div(ep, nc), nz)
    x = lax.div(ep, nc * nz)

    def dev(x_, y_, z_, c_):
        return (((x_ * nz + z_) * nc + c_), y_)

    def to_x(g):
        return lax.rem(x + (nx - offsets[g]), nx)

    def from_x(g):
        return lax.rem(x + offsets[g], nx)

    def at_y(o):
        return lax.rem(y + (o + ny), ny)

    def at_z(o):
        return lax.rem(z + (o + nz), nz)

    def place(o):
        return ((o + nz // 4) % nz) * tile

    def rows(start, size):
        if isinstance(start, int):
            return pl.ds(start, size)
        return pl.ds(pl.multiple_of(start, size), size)

    def base(h, g, c_):
        if g == 0:
            return h * both + c_ * slots
        return 2 * both + (h * (nx - 1) + g - 1) * both + c_ * slots

    def span(h, u):
        return base(h, units[u][0], 0), len(units[u]) * both

    sends = []

    def send(src, dst, ssem, rsem, device):
        copy = pltpu.make_async_remote_copy(
            src_ref=src, dst_ref=dst, send_sem=ssem, recv_sem=rsem,
            device_id=device, device_id_type=MESH,
        )
        copy.start()
        sends.append(copy)
        return copy

    def arrived(ref, rsem):
        pltpu.make_async_remote_copy(
            src_ref=ref, dst_ref=ref, send_sem=rsem, recv_sem=rsem,
            device_id=dev(x, y, z, 1 - c), device_id_type=MESH,
        ).wait_recv()

    barrier = pltpu.get_barrier_semaphore()
    peers = [dev(x, y, at_z(o), c) for o in (1, -1, 2, -2)]
    peers += [dev(from_x(g), y, z, c_) for g in range(1, nx) for c_ in range(nc)]
    peers += [dev(x, y, z, 1 - c)]
    peers += [dev(x, at_y(o), z, c) for o in range(1, ny)]
    for peer in peers:
        pl.semaphore_signal(barrier, inc=1, device_id=peer, device_id_type=MESH)

    own = pl.ds(place(0), tile)
    mine = pltpu.make_async_copy(
        tok_hbm.at[:, pl.ds(pl.multiple_of(y * quarter, 128), quarter)],
        zbuf.at[own, pl.ds(0, quarter)], w_sem.at[3],
    )
    mine.start()
    scores = 1.0 / (1.0 + jnp.exp(-logits_ref[...]))
    wts = ROUTE_SCALE * scores / jnp.sum(scores, axis=0, keepdims=True)
    lane = lax.broadcasted_iota(jnp.int32, (top, 128), 1)
    sub = lax.broadcasted_iota(jnp.int32, (top, 128), 0)
    put_id = (lane == sub).astype(BF16)
    put_w = (lane == sub + top).astype(BF16)
    across = (((0,), (0,)), ((), ()))
    meta = lax.dot_general(
        ids_ref[...].astype(F32).astype(BF16), put_id, across, preferred_element_type=F32
    ) + lax.dot_general(wts.astype(BF16), put_w, across, preferred_element_type=F32)
    zbuf[own, quarter : quarter + 128] = meta.astype(BF16)

    loads = [
        pltpu.make_async_copy(s.at[0], d, w_sem.at[i])
        for i, (s, d) in enumerate(((wg_hbm, wg), (wu_hbm, wu), (wd_hbm, wd)))
    ]
    for load in loads:
        load.start()
    mine.wait()
    pl.semaphore_wait(barrier, len(peers))

    steps = nz // 4

    def zsem(d, k, hop):
        return ((0 if d > 0 else 1) * steps + (k - 1)) * 2 + (hop - 1)

    gathers = {}

    def gather_send(k, d):
        o = -d * 2 * (k - 1)
        for hop in (2, 1):
            if hop == 2 and d < 0 and k == steps:
                continue
            i = zsem(d, k, hop)
            gathers[k, d, hop] = send(
                zbuf.at[pl.ds(place(o), tile), :], zbuf.at[pl.ds(place(o - d * hop), tile), :],
                zag_s.at[i], zag_r.at[i], dev(x, y, at_z(d * hop), c),
            )

    def gather_wait(k, d, hop):
        if (k, d, hop) in gathers:
            gathers.pop((k, d, hop)).wait_recv()

    def gather_step(k):
        for d in (1, -1):
            gather_wait(k, d, 2)
            if k < steps:
                gather_send(k + 1, d)

    def routes(h):
        pick = (
            lax.broadcasted_iota(jnp.int32, (2 * top, 128), 0)
            == lax.broadcasted_iota(jnp.int32, (2 * top, 128), 1)
        ).astype(BF16)
        by_token = lax.dot_general(
            pick, zbuf[h * col : (h + 1) * col, quarter : quarter + 128],
            (((1,), (1,)), ((), ())), preferred_element_type=F32,
        )
        lanes = nx * nc
        j = lax.broadcasted_iota(jnp.int32, (lanes, col), 0)
        jg, jc = lax.div(j, nc), lax.rem(j, nc)
        off = jnp.zeros_like(jg)
        for g, o in enumerate(offsets):
            off = jnp.where(jg == g, nx - o, off)
        expert = ((lax.rem(x + off, nx) * nz + z) * nc + jc).astype(F32)
        named = jnp.zeros((lanes, col), F32)
        weight = jnp.zeros((lanes, col), F32)
        for k in range(top):
            hit = by_token[k : k + 1, :] == expert
            named = jnp.where(hit, 1.0, named)
            weight = jnp.where(hit, by_token[top + k : top + k + 1, :], weight)
        t_row = lax.broadcasted_iota(jnp.int32, (col, col), 0)
        t_col = lax.broadcasted_iota(jnp.int32, (col, col), 1)
        before = ((t_row < t_col) & (lax.div(t_row, tile) == lax.div(t_col, tile))).astype(BF16)
        rank = jnp.dot(named.astype(BF16), before, preferred_element_type=F32)
        return jnp.where(named > 0.5, rank, -1.0), weight

    s_row = lax.broadcasted_iota(jnp.int32, (slots, col), 0)
    s_col = lax.broadcasted_iota(jnp.int32, (slots, col), 1)
    in_block = lax.div(s_row, CAP) == lax.div(s_col, tile)
    want = jnp.where(in_block, lax.rem(s_row, CAP).astype(F32), -2.0)

    def x_index(h, g, c_):
        return (h * nx + g) * nc + c_

    def select(h, g, rank, weight):
        chosen = []
        for c_ in range(nc):
            i = g * nc + c_
            hit = rank[i : i + 1, :] == want
            chosen.append(jnp.where(hit, 1.0, 0.0).astype(BF16))
            swbuf[pl.ds(base(h, g, c_), slots), :] = jnp.where(
                hit, weight[i : i + 1, :], 0.0
            ).astype(BF16)
        xsend[pl.ds(base(h, g, 0), nc * slots), :] = jnp.dot(
            jnp.concatenate(chosen, axis=0), zbuf[h * col : (h + 1) * col, 0:quarter],
            preferred_element_type=F32,
        ).astype(BF16)
        land = ybuf.at[y, rows(base(h, g, c), slots), :]
        if g > 0:
            for c_ in range(nc):
                send(
                    xsend.at[pl.ds(base(h, g, c_), slots), :], land, x_s.at[x_index(h, g, c_)],
                    x_r.at[x_index(h, g, c)], dev(to_x(g), y, z, c_),
                )
        else:
            other = 1 - c
            send(
                xsend.at[rows(base(h, g, other), slots), :], land, x_s.at[x_index(h, g, 0)],
                x_r.at[x_index(h, g, c)], dev(x, y, z, other),
            )
            here = rows(base(h, g, c), slots)
            ybuf[y, here, :] = xsend[here, :]

    def x_wait(h, g):
        if g == 0:
            arrived(ybuf.at[y, rows(base(h, 0, 1 - c), slots), :], x_r.at[x_index(h, 0, 1 - c)])
        else:
            for c_ in range(nc):
                arrived(ybuf.at[y, pl.ds(base(h, g, c_), slots), :], x_r.at[x_index(h, g, c_)])

    y_one, y_two, p_one, p_two = {}, {}, {}, {}

    def index(h, u, n):
        return (n * 2 + h) * len(units) + u

    def spread(h, u):
        for g in units[u]:
            x_wait(h, g)
        start, size = span(h, u)
        block = ybuf.at[y, pl.ds(start, size), :]
        for n, d in enumerate((1, -1)):
            i = index(h, u, n)
            y_one[h, u, d] = send(block, block, y1_s.at[i], y1_r.at[i], dev(x, at_y(d), z, c))

    def forward(h, u):
        start, size = span(h, u)
        for n, d in enumerate((1, -1)):
            y_one[h, u, d].wait_recv()
            block = ybuf.at[at_y(-d), pl.ds(start + n * size // 2, size // 2), :]
            i = index(h, u, n)
            y_two[h, u, d] = send(block, block, y2_s.at[i], y2_r.at[i], dev(x, at_y(d), z, c))

    def experts(start, size):
        here = pl.ds(start, size)
        gate = jnp.zeros((size, wg.shape[1]), F32)
        upper = jnp.zeros((size, wg.shape[1]), F32)
        for q in range(ny):
            piece = ybuf[q, here, :]
            deep = pl.ds(q * quarter, quarter)
            gate += jnp.dot(piece, wg[deep, :], preferred_element_type=F32)
            upper += jnp.dot(piece, wu[deep, :], preferred_element_type=F32)
        hidden = (gate / (1.0 + jnp.exp(-gate)) * upper).astype(BF16)
        for q in range(ny):
            obuf[q, here, :] = jnp.dot(
                hidden, wd[:, q * quarter : (q + 1) * quarter], preferred_element_type=F32
            ).astype(BF16)

    def compute(h, u):
        for d in (1, -1):
            y_two[h, u, d].wait_recv()
        experts(*span(h, u))

    home = {}

    def compute_home():
        for h in (0, 1):
            for d in (1, -1):
                y_two[h, last, d].wait_recv()
        experts(0, 2 * both)
        for h in (0, 1):
            other = 1 - c
            home[h] = send(
                obuf.at[:, rows(base(h, 0, other), slots), :],
                rbuf0.at[:, rows(base(h, 0, c), slots), :],
                b_s.at[x_index(h, 0, 0)], b_r.at[x_index(h, 0, c)], dev(x, y, z, other),
            )
            here = rows(base(h, 0, c), slots)
            for q in range(ny):
                rbuf0[q, here, :] = obuf[q, here, :]

    def combine_home():
        for h in (0, 1):
            arrived(
                rbuf0.at[:, rows(base(h, 0, 1 - c), slots), :], b_r.at[x_index(h, 0, 1 - c)]
            )
            here = pl.ds(base(h, 0, 0), both)
            for q in range(ny):
                part0[h * col : (h + 1) * col, q * quarter : (q + 1) * quarter] = lax.dot_general(
                    swbuf[here, :], rbuf0[q, here, :], across, preferred_element_type=F32
                )

    def give_one(h, u):
        start, size = span(h, u)
        for n, d in enumerate((1, -1)):
            i = index(h, u, n)
            p_one[h, u, d] = send(
                obuf.at[at_y(2), pl.ds(start + n * size // 2, size // 2), :],
                r1buf.at[n, pl.ds(start // 2, size // 2), :],
                p1_s.at[i], p1_r.at[i], dev(x, at_y(d), z, c),
            )

    def give_two(h, u):
        start, size = span(h, u)
        for n, d in enumerate((1, -1)):
            p_one[h, u, d].wait_recv()
            here = pl.ds(start + n * size // 2, size // 2)
            q = at_y(d)
            got = r1buf[n, pl.ds(start // 2, size // 2), :]
            obuf[q, here, :] = (obuf[q, here, :].astype(F32) + got.astype(F32)).astype(BF16)
            i = index(h, u, n)
            here = pl.ds(start, size)
            p_two[h, u, d] = send(
                obuf.at[q, here, :], r2buf.at[n, here, :],
                p2_s.at[i], p2_r.at[i], dev(x, at_y(d), z, c),
            )

    def give_back(h, u):
        for d in (1, -1):
            p_two[h, u, d].wait_recv()
        here = pl.ds(*span(h, u))
        total = obuf[y, here, :].astype(F32) + r2buf[0, here, :].astype(F32)
        xret[here, :] = (total + r2buf[1, here, :].astype(F32)).astype(BF16)
        for g in units[u]:
            land = rbuf.at[rows(base(h, g, c), slots), :]
            for c_ in range(nc):
                send(
                    xret.at[pl.ds(base(h, g, c_), slots), :], land, b_s.at[x_index(h, g, c_)],
                    b_r.at[x_index(h, g, c)], dev(from_x(g), y, z, c_),
                )

    def combine(h, u, first):
        for g in units[u]:
            for c_ in range(nc):
                arrived(rbuf.at[pl.ds(base(h, g, c_), slots), :], b_r.at[x_index(h, g, c_)])
        here = pl.ds(*span(h, u))
        term = lax.dot_general(
            swbuf[here, :], rbuf[here, :], across, preferred_element_type=F32
        )
        dest = pl.ds(h * col, col)
        if first:
            part[dest, :] = term
        else:
            part[dest, :] += term

    reach = nz // 2

    def reducer(source, src1, src2, dst1, dst2, ssem, rsem):
        got = {}

        def block_of(o):
            return source[pl.ds(place(o), tile), :]

        def zsend(d, k, hop, value):
            src, dst = (src1, dst1) if hop == 1 else (src2, dst2)
            i, n = zsem(d, k, hop), (0 if d > 0 else 1) * steps + (k - 1)
            src[n] = value.astype(BF16)
            got[d, k, hop] = (
                send(src.at[n], dst.at[n], ssem.at[i], rsem.at[i], dev(x, y, at_z(d * hop), c)), dst, n
            )

        def zget(d, k):
            total = None
            for hop in (1, 2):
                if (d, k, hop) in got:
                    copy, dst, n = got[d, k, hop]
                    copy.wait_recv()
                    value = dst[n].astype(F32)
                    total = value if total is None else total + value
            return total

        def own_hop(k):
            if k == 1:
                zsend(1, 1, 2, block_of(reach))
            for d in (1, -1):
                zsend(d, k, 1, block_of(d * (reach + 1 - 2 * k)))

        def next_hop(k):
            for d in (1, -1):
                zsend(d, k + 1, 2, block_of(d * (reach - 2 * k)) + zget(d, k))

        def finish():
            return block_of(0) + zget(1, steps) + zget(-1, steps)

        return own_hop, next_hop, finish

    own_hop, next_hop, finish = reducer(part, zs1, zs2, zr1, zr2, zrs_s, zrs_r)
    wide_own, wide_next, wide_finish = reducer(part0, ws1, ws2, wr1, wr2, wrs_s, wrs_r)

    near, far = 0, 1
    mid = steps // 2
    zero = last
    rest = tuple(range(1, last))
    later = list(range(mid + 1, steps + 1))
    for d in (1, -1):
        gather_send(1, d)
    for k in range(1, mid + 1):
        gather_step(k)
    for k in range(1, mid + 1):
        for d in (1, -1):
            gather_wait(k, d, 1)
    rank, weight = routes(near)
    for g in range(nx):
        select(near, g, rank, weight)
    spread(near, zero)
    for k in later[:-1]:
        gather_step(k)
    spread(near, 0)
    forward(near, zero)
    gather_step(later[-1])
    for k in later:
        for d in (1, -1):
            gather_wait(k, d, 1)
    rank, weight = routes(far)
    for g in range(nx):
        select(far, g, rank, weight)
    spread(far, zero)
    for u in rest:
        spread(near, u)
    forward(near, 0)
    spread(far, 0)
    forward(far, zero)
    for u in rest:
        forward(near, u)
    for u in rest:
        spread(far, u)
    for load in loads:
        load.wait()
    compute_home()
    forward(far, 0)
    compute(near, 0)
    give_one(near, 0)
    combine_home()
    wide_own(1)
    for u in rest:
        forward(far, u)
    for k in range(2, steps + 1):
        wide_own(k)
    for u in rest:
        compute(near, u)
        give_one(near, u)
    wide_next(1)
    compute(far, 0)
    give_one(far, 0)
    for u in rest:
        compute(far, u)
        give_one(far, u)
    for k in range(2, mid + 1):
        wide_next(k)
    give_two(far, 0)
    for u in rest:
        give_two(far, u)
    for u in rest:
        give_two(near, u)
    give_two(near, 0)
    for k in range(max(mid, 1) + 1, steps):
        wide_next(k)
    give_back(far, 0)
    for u in rest:
        give_back(far, u)
    for u in rest:
        give_back(near, u)
    combine(far, 0, True)
    for u in rest:
        combine(far, u, False)
    for k in range(1, mid + 1):
        own_hop(k)
    wide = wide_finish()
    give_back(near, 0)
    for k in range(1, mid):
        next_hop(k)
    for n, u in enumerate(rest):
        combine(near, u, n == 0)
    combine(near, 0, not rest)
    for k in range(mid, steps):
        if k == mid:
            next_hop(k)
            for j in range(mid + 1, steps + 1):
                own_hop(j)
        else:
            next_hop(k)
    main = finish()

    count = out_ref.shape[0]
    for q in range(ny):
        piece = slice(q * quarter, (q + 1) * quarter)
        share = (wide[:, piece] + jnp.where(y == q, main, 0.0)).astype(BF16)
        for o in range(ny):
            fsend[o, :, piece] = share[o * count : (o + 1) * count, :]
    tails = []
    for o in (2, 1, 3):
        tails.append(
            send(fsend.at[at_y(o)], frecv.at[y], f_s.at[o], f_r.at[o], dev(x, at_y(o), z, c))
        )
    frecv[y] = fsend[y]
    for tail in tails:
        tail.wait_recv()
    total = frecv[0].astype(F32)
    for q in range(1, ny):
        total += frecv[q].astype(F32)
    out_ref[...] = total.astype(BF16)
    for copy in sends:
        copy.wait_send()


def on_device(tokens, expert_ids, route_logits, expert_gate, expert_up, expert_down):
    n_ep, ny = lax.axis_size("ep"), N_DP
    nx, nc = CHIPS_X, CORES
    nz = n_ep // (nx * nc)
    tile, width = tokens.shape
    hidden = expert_gate.shape[2]
    quarter = width // ny
    col, slots = nz * tile, nz * CAP
    every = nx * nc * slots
    steps = nz // 4
    dma = pltpu.SemaphoreType.DMA
    vmem = pl.BlockSpec(memory_space=pltpu.VMEM)
    hbm = pl.BlockSpec(memory_space=pl.ANY)
    flops = 6 * every * width * hidden
    units = 4 * (nx // 2 + 1)
    home = 2 * nc * slots // 2
    moves = 2 * nx * nc
    return pl.pallas_call(
        functools.partial(kernel, nx, nz),
        out_shape=jax.ShapeDtypeStruct((tile // ny, width), BF16),
        in_specs=[vmem, vmem, hbm, hbm, hbm, hbm],
        out_specs=vmem,
        scratch_shapes=[
            pltpu.VMEM((width, hidden), BF16),
            pltpu.VMEM((width, hidden), BF16),
            pltpu.VMEM((hidden, width), BF16),
            pltpu.VMEM((col, quarter + 128), BF16),
            pltpu.VMEM((every, col // 2), BF16),
            pltpu.VMEM((every, quarter), BF16),
            pltpu.VMEM((ny, every, quarter), BF16),
            pltpu.VMEM((ny, every, quarter), BF16),
            pltpu.VMEM((2, every // 2, quarter), BF16),
            pltpu.VMEM((2, every, quarter), BF16),
            pltpu.VMEM((every, quarter), BF16),
            pltpu.VMEM((every, quarter), BF16),
            pltpu.VMEM((ny, home, quarter), BF16),
            pltpu.VMEM((col, quarter), F32),
            pltpu.VMEM((col, width), F32),
            pltpu.VMEM((2 * steps, tile, quarter), BF16),
            pltpu.VMEM((2 * steps, tile, quarter), BF16),
            pltpu.VMEM((2 * steps, tile, quarter), BF16),
            pltpu.VMEM((2 * steps, tile, quarter), BF16),
            pltpu.VMEM((2 * steps, tile, width), BF16),
            pltpu.VMEM((2 * steps, tile, width), BF16),
            pltpu.VMEM((2 * steps, tile, width), BF16),
            pltpu.VMEM((2 * steps, tile, width), BF16),
            pltpu.VMEM((ny, tile // ny, width), BF16),
            pltpu.VMEM((ny, tile // ny, width), BF16),
            dma((4,)),
            dma((4 * steps,)), dma((4 * steps,)),
            dma((moves,)), dma((moves,)),
            dma((units,)), dma((units,)),
            dma((units,)), dma((units,)),
            dma((units,)), dma((units,)),
            dma((units,)), dma((units,)),
            dma((moves,)), dma((moves,)),
            dma((4 * steps,)), dma((4 * steps,)),
            dma((4 * steps,)), dma((4 * steps,)),
            dma((ny,)), dma((ny,)),
        ],
        compiler_params=pltpu.CompilerParams(
            collective_id=0, has_side_effects=True, vmem_limit_bytes=56 * 1024 * 1024
        ),
        cost_estimate=pl.CostEstimate(flops=flops, bytes_accessed=8 << 20, transcendentals=0),
    )(expert_ids.T, route_logits.T, tokens, expert_gate, expert_up, expert_down)


def solution(mesh):
    placed = (
        P("ep", None),
        P("ep", None),
        P("ep", None),
        P("ep", None, "dp"),
        P("ep", None, "dp"),
        P("ep", "dp", None),
    )
    return jax.shard_map(
        on_device, mesh=mesh, in_specs=placed, out_specs=P(("ep", "dp"), None), check_vma=False
    )
```

```python
import functools

import jax
import jax.numpy as jnp
from jax import lax
from jax.experimental import pallas as pl
from jax.experimental.pallas import tpu as pltpu
from jax.sharding import PartitionSpec as P

MESH = pl.DeviceIdType.MESH
F32 = jnp.float32
BF16 = jnp.bfloat16
ROUTE_SCALE = 2.5
CAP = 4
CHIPS_X = 4
CORES = 2
N_DP = 4


def kernel(
    nx, nz, ids_ref, logits_ref, tok_hbm, wg_hbm, wu_hbm, wd_hbm, out_ref,
    wg, wu, wd, zbuf, swbuf, xsend, ybuf, obuf, r1buf, r2buf, xret, rbuf, rbuf0, part, part0,
    zs, zr, ws, wr, fsend, frecv,
    w_sem, s_sem, zag_r, zag_one, x_r, y1_r, y2_r, p1_r, p2_r, b_r, zrs_r, wrs_r, f_r,
):
    nc, ny = CORES, N_DP
    tile, width = tok_hbm.shape
    quarter = width // ny
    top = ids_ref.shape[0]
    col = nz * tile // 2
    near_blocks = nz // 2
    slots = near_blocks * CAP
    both = nc * slots
    offsets = {2: (0, 1), 4: (0, 1, 3, 2)}[nx]
    units = {2: ((1,), (0,)), 4: ((1, 2), (3,), (0,))}[nx]
    last = len(units) - 1
    (zag_s, x_s, y1_s, y2_s, p1_s, p2_s, b_s, home_s, zrs_s, wrs_s, f_s) = [
        s_sem.at[i] for i in range(11)
    ]
    ep = lax.axis_index("ep")
    y = lax.axis_index("dp")
    c = lax.rem(ep, nc)
    z = lax.rem(lax.div(ep, nc), nz)
    x = lax.div(ep, nc * nz)

    def dev(x_, y_, z_, c_):
        return (((x_ * nz + z_) * nc + c_), y_)

    def to_x(g):
        return lax.rem(x + (nx - offsets[g]), nx)

    def from_x(g):
        return lax.rem(x + offsets[g], nx)

    def at_y(o):
        return lax.rem(y + (o + ny), ny)

    def at_z(o):
        return lax.rem(z + (o + nz), nz)

    def place(o):
        return ((o + nz // 4) % nz) * tile

    def rows(start, size):
        if isinstance(start, int):
            return pl.ds(start, size)
        return pl.ds(pl.multiple_of(start, size), size)

    def base(h, g, c_):
        if g == 0:
            return h * both + c_ * slots
        return 2 * both + (h * (nx - 1) + g - 1) * both + c_ * slots

    def span(h, u):
        return base(h, units[u][0], 0), len(units[u]) * both

    def send(src, dst, ssem, rsem, device):
        pltpu.make_async_remote_copy(
            src_ref=src, dst_ref=dst, send_sem=ssem, recv_sem=rsem,
            device_id=device, device_id_type=MESH,
        ).start()

    def awaits(ref, sem):
        return pltpu.make_async_remote_copy(
            src_ref=ref, dst_ref=ref, send_sem=sem, recv_sem=sem,
            device_id=dev(x, y, z, 1 - c), device_id_type=MESH,
        )

    def arrived(ref, sem):
        awaits(ref, sem).wait_recv()

    barrier = pltpu.get_barrier_semaphore()
    peers = [dev(x, y, at_z(o), c) for o in (1, -1, 2, -2)]
    peers += [dev(from_x(g), y, z, c_) for g in range(1, nx) for c_ in range(nc)]
    peers += [dev(x, y, z, 1 - c)]
    peers += [dev(x, at_y(o), z, c) for o in range(1, ny)]
    for peer in peers:
        pl.semaphore_signal(barrier, inc=1, device_id=peer, device_id_type=MESH)

    own = pl.ds(place(0), tile)
    mine = pltpu.make_async_copy(
        tok_hbm.at[:, pl.ds(pl.multiple_of(y * quarter, 128), quarter)],
        zbuf.at[own, pl.ds(0, quarter)], w_sem.at[3],
    )
    mine.start()
    scores = 1.0 / (1.0 + jnp.exp(-logits_ref[...]))
    wts = ROUTE_SCALE * scores / jnp.sum(scores, axis=0, keepdims=True)
    lane = lax.broadcasted_iota(jnp.int32, (top, 128), 1)
    sub = lax.broadcasted_iota(jnp.int32, (top, 128), 0)
    put_id = (lane == sub).astype(BF16)
    put_w = (lane == sub + top).astype(BF16)
    across = (((0,), (0,)), ((), ()))
    meta = lax.dot_general(
        ids_ref[...].astype(F32).astype(BF16), put_id, across, preferred_element_type=F32
    ) + lax.dot_general(wts.astype(BF16), put_w, across, preferred_element_type=F32)
    zbuf[own, quarter : quarter + 128] = meta.astype(BF16)

    loads = [
        pltpu.make_async_copy(s.at[0], d, w_sem.at[i])
        for i, (s, d) in enumerate(((wg_hbm, wg), (wu_hbm, wu), (wd_hbm, wd)))
    ]
    for load in loads:
        load.start()
    mine.wait()
    pl.semaphore_wait(barrier, len(peers))

    steps = nz // 4

    def zslot(d, k):
        return (0 if d > 0 else 1) * steps + (k - 1)

    mid = steps // 2

    def gather_send(k, d):
        o = -d * 2 * (k - 1)
        for hop in (2, 1):
            if hop == 2 and d < 0 and k == steps:
                continue
            rsem = zag_r.at[zslot(d, k)] if hop == 2 else zag_one.at[0 if k <= mid else 1]
            send(
                zbuf.at[pl.ds(place(o), tile), :], zbuf.at[pl.ds(place(o - d * hop), tile), :],
                zag_s, rsem, dev(x, y, at_z(d * hop), c),
            )

    def gather_step(k):
        for d in (1, -1):
            if d > 0 or k < steps:
                arrived(zbuf.at[pl.ds(0, tile), :], zag_r.at[zslot(d, k)])
            if k < steps:
                gather_send(k + 1, d)

    def gather_rest(h):
        count = mid if h == 0 else steps - mid
        arrived(zbuf.at[pl.ds(0, 2 * count * tile), :], zag_one.at[h])

    def routes(h):
        pick = (
            lax.broadcasted_iota(jnp.int32, (2 * top, 128), 0)
            == lax.broadcasted_iota(jnp.int32, (2 * top, 128), 1)
        ).astype(BF16)
        by_token = lax.dot_general(
            pick, zbuf[h * col : (h + 1) * col, quarter : quarter + 128],
            (((1,), (1,)), ((), ())), preferred_element_type=F32,
        )
        lanes = nx * nc
        j = lax.broadcasted_iota(jnp.int32, (lanes, col), 0)
        jg, jc = lax.div(j, nc), lax.rem(j, nc)
        off = jnp.zeros_like(jg)
        for g, o in enumerate(offsets):
            off = jnp.where(jg == g, nx - o, off)
        expert = ((lax.rem(x + off, nx) * nz + z) * nc + jc).astype(F32)
        named = jnp.zeros((lanes, col), F32)
        weight = jnp.zeros((lanes, col), F32)
        for k in range(top):
            hit = by_token[k : k + 1, :] == expert
            named = jnp.where(hit, 1.0, named)
            weight = jnp.where(hit, by_token[top + k : top + k + 1, :], weight)
        t_row = lax.broadcasted_iota(jnp.int32, (col, col), 0)
        t_col = lax.broadcasted_iota(jnp.int32, (col, col), 1)
        before = ((t_row < t_col) & (lax.div(t_row, tile) == lax.div(t_col, tile))).astype(BF16)
        rank = jnp.dot(named.astype(BF16), before, preferred_element_type=F32)
        return jnp.where(named > 0.5, rank, -1.0), weight

    s_row = lax.broadcasted_iota(jnp.int32, (slots, col), 0)
    s_col = lax.broadcasted_iota(jnp.int32, (slots, col), 1)
    in_block = lax.div(s_row, CAP) == lax.div(s_col, tile)
    want = jnp.where(in_block, lax.rem(s_row, CAP).astype(F32), -2.0)

    unit_of = {g: u for u, unit in enumerate(units) for g in unit}

    def x_index(h, g):
        return h * len(units) + unit_of[g]

    def select(h, g, rank, weight):
        chosen = []
        for c_ in range(nc):
            i = g * nc + c_
            hit = rank[i : i + 1, :] == want
            chosen.append(jnp.where(hit, 1.0, 0.0).astype(BF16))
            swbuf[pl.ds(base(h, g, c_), slots), :] = jnp.where(
                hit, weight[i : i + 1, :], 0.0
            ).astype(BF16)
        xsend[pl.ds(base(h, g, 0), nc * slots), :] = jnp.dot(
            jnp.concatenate(chosen, axis=0), zbuf[h * col : (h + 1) * col, 0:quarter],
            preferred_element_type=F32,
        ).astype(BF16)
        land = ybuf.at[y, rows(base(h, g, c), slots), :]
        if g > 0:
            for c_ in range(nc):
                send(
                    xsend.at[pl.ds(base(h, g, c_), slots), :], land, x_s,
                    x_r.at[x_index(h, g)], dev(to_x(g), y, z, c_),
                )
        else:
            other = 1 - c
            send(
                xsend.at[rows(base(h, g, other), slots), :], land, x_s,
                x_r.at[x_index(h, g)], dev(x, y, z, other),
            )
            here = rows(base(h, g, c), slots)
            ybuf[y, here, :] = xsend[here, :]

    def x_wait(h, u):
        start, size = span(h, u)
        size = slots if u == last else size
        arrived(ybuf.at[y, pl.ds(start, size), :], x_r.at[h * len(units) + u])

    def index(h, u):
        return h * len(units) + u

    def spread(h, u):
        x_wait(h, u)
        start, size = span(h, u)
        block = ybuf.at[y, pl.ds(start, size), :]
        for d in (1, -1):
            send(block, block, y1_s, y1_r.at[index(h, u)], dev(x, at_y(d), z, c))

    def forward(h, u):
        start, size = span(h, u)
        arrived(ybuf.at[pl.ds(0, 2), pl.ds(start, size), :], y1_r.at[index(h, u)])
        for n, d in enumerate((1, -1)):
            block = ybuf.at[at_y(-d), pl.ds(start + n * size // 2, size // 2), :]
            send(block, block, y2_s, y2_r.at[index(h, u)], dev(x, at_y(d), z, c))

    def y_wait(h, u):
        arrived(ybuf.at[0, pl.ds(*span(h, u)), :], y2_r.at[index(h, u)])

    def experts(start, size):
        here = pl.ds(start, size)
        gate = jnp.zeros((size, wg.shape[1]), F32)
        upper = jnp.zeros((size, wg.shape[1]), F32)
        for q in range(ny):
            piece = ybuf[q, here, :]
            deep = pl.ds(q * quarter, quarter)
            gate += jnp.dot(piece, wg[deep, :], preferred_element_type=F32)
            upper += jnp.dot(piece, wu[deep, :], preferred_element_type=F32)
        hidden = (gate / (1.0 + jnp.exp(-gate)) * upper).astype(BF16)
        for q in range(ny):
            obuf[q, here, :] = jnp.dot(
                hidden, wd[:, q * quarter : (q + 1) * quarter], preferred_element_type=F32
            ).astype(BF16)

    def compute(h, u):
        y_wait(h, u)
        experts(*span(h, u))

    def compute_home():
        for h in (0, 1):
            y_wait(h, last)
        experts(0, 2 * both)
        for h in (0, 1):
            other = 1 - c
            send(
                obuf.at[:, rows(base(h, 0, other), slots), :],
                rbuf0.at[:, rows(base(h, 0, c), slots), :],
                home_s, b_r.at[index(h, last)], dev(x, y, z, other),
            )
            here = rows(base(h, 0, c), slots)
            for q in range(ny):
                rbuf0[q, here, :] = obuf[q, here, :]

    def combine_home():
        for h in (0, 1):
            arrived(rbuf0.at[:, pl.ds(base(h, 0, 0), slots), :], b_r.at[index(h, last)])
            here = pl.ds(base(h, 0, 0), both)
            for o in range(ny):
                term = lax.dot_general(
                    swbuf[here, :], rbuf0[at_y(o), here, :], across, preferred_element_type=F32
                )
                if o == 0:
                    part[h * col : (h + 1) * col, :] = term
                else:
                    part0[h * col : (h + 1) * col, (o - 1) * quarter : o * quarter] = term

    def give_one(h, u):
        start, size = span(h, u)
        for n, d in enumerate((1, -1)):
            send(
                obuf.at[at_y(2), pl.ds(start + n * size // 2, size // 2), :],
                r1buf.at[n, pl.ds(start // 2, size // 2), :],
                p1_s, p1_r.at[index(h, u)], dev(x, at_y(d), z, c),
            )

    def give_two(h, u):
        start, size = span(h, u)
        arrived(r1buf.at[:, pl.ds(start // 2, size // 2), :], p1_r.at[index(h, u)])
        for n, d in enumerate((1, -1)):
            here = pl.ds(start + n * size // 2, size // 2)
            q = at_y(d)
            got = r1buf[n, pl.ds(start // 2, size // 2), :]
            obuf[q, here, :] = (obuf[q, here, :].astype(F32) + got.astype(F32)).astype(BF16)
            here = pl.ds(start, size)
            send(
                obuf.at[q, here, :], r2buf.at[n, here, :],
                p2_s, p2_r.at[index(h, u)], dev(x, at_y(d), z, c),
            )

    def give_back(h, u):
        here = pl.ds(*span(h, u))
        arrived(r2buf.at[:, here, :], p2_r.at[index(h, u)])
        total = obuf[y, here, :].astype(F32) + r2buf[0, here, :].astype(F32)
        xret[here, :] = (total + r2buf[1, here, :].astype(F32)).astype(BF16)
        for g in units[u]:
            land = rbuf.at[rows(base(h, g, c), slots), :]
            for c_ in range(nc):
                send(
                    xret.at[pl.ds(base(h, g, c_), slots), :], land, b_s,
                    b_r.at[index(h, u)], dev(from_x(g), y, z, c_),
                )

    def combine(h, u):
        here = pl.ds(*span(h, u))
        arrived(rbuf.at[here, :], b_r.at[index(h, u)])
        part[h * col : (h + 1) * col, :] += lax.dot_general(
            swbuf[here, :], rbuf[here, :], across, preferred_element_type=F32
        )

    reach = nz // 2

    def reducer(source, src, dst, ssem, rsem):
        def block_of(o):
            return source[pl.ds(place(o), tile), :]

        def zsend(d, k, hop, value):
            n = zslot(d, k)
            src[n, hop - 1] = value.astype(BF16)
            send(src.at[n, hop - 1], dst.at[n, hop - 1], ssem, rsem.at[n], dev(x, y, at_z(d * hop), c))

        def zget(d, k):
            n = zslot(d, k)
            if d < 0 and k == 1:
                arrived(dst.at[n, 0], rsem.at[n])
                return dst[n, 0].astype(F32)
            arrived(dst.at[n], rsem.at[n])
            return dst[n, 0].astype(F32) + dst[n, 1].astype(F32)

        def own_hop(k):
            if k == 1:
                zsend(1, 1, 2, block_of(reach))
            for d in (1, -1):
                zsend(d, k, 1, block_of(d * (reach + 1 - 2 * k)))

        def next_hop(k):
            for d in (1, -1):
                zsend(d, k + 1, 2, block_of(d * (reach - 2 * k)) + zget(d, k))

        def finish():
            return block_of(0) + zget(1, steps) + zget(-1, steps)

        return own_hop, next_hop, finish

    own_hop, next_hop, finish = reducer(part, zs, zr, zrs_s, zrs_r)
    wide_own, wide_next, wide_finish = reducer(part0, ws, wr, wrs_s, wrs_r)

    near, far = 0, 1
    rest = tuple(range(1, last))

    def wide_step(k):
        if k < steps:
            wide_next(k)
            wide_own(k + 1)

    for d in (1, -1):
        gather_send(1, d)
    for k in range(1, mid + 1):
        gather_step(k)
    gather_rest(near)
    rank, weight = routes(near)
    for g in range(nx):
        select(near, g, rank, weight)
    spread(near, last)
    for k in range(mid + 1, steps):
        gather_step(k)
    spread(near, 0)
    forward(near, last)
    gather_step(steps)
    gather_rest(far)
    rank, weight = routes(far)
    for g in range(nx):
        select(far, g, rank, weight)
    spread(far, last)
    for u in rest:
        spread(near, u)
    forward(near, 0)
    forward(far, last)
    spread(far, 0)
    for u in rest:
        forward(near, u)
        spread(far, u)
    for load in loads:
        load.wait()
    compute_home()
    compute(near, 0)
    give_one(near, 0)
    combine_home()
    wide_own(1)
    forward(far, 0)
    for u in rest:
        compute(near, u)
        give_one(near, u)
        forward(far, u)
    wide_step(1)
    for u in rest:
        give_two(near, u)
    compute(far, 0)
    give_one(far, 0)
    for u in rest:
        compute(far, u)
        give_one(far, u)
    wide_step(2)
    give_two(far, 0)
    for u in rest:
        give_two(far, u)
    give_two(near, 0)
    for k in range(3, steps):
        wide_step(k)
    for u in rest:
        give_back(near, u)
    give_back(far, 0)
    for u in rest:
        give_back(far, u)
    for u in range(last):
        combine(far, u)
    for k in range(1, mid + 1):
        own_hop(k)
    wide = wide_finish()
    for k in range(1, mid):
        next_hop(k)
    give_back(near, 0)
    for u in rest:
        combine(near, u)
    combine(near, 0)
    next_hop(mid)
    for k in range(mid + 1, steps + 1):
        own_hop(k)
    for k in range(mid + 1, steps):
        next_hop(k)
    main = finish()

    count = out_ref.shape[0]
    for o in range(ny):
        share = (main if o == 0 else wide[:, (o - 1) * quarter : o * quarter]).astype(BF16)
        piece = pl.ds(pl.multiple_of(at_y(o) * quarter, 128), quarter)
        for n in range(ny):
            fsend[n, :, piece] = share[n * count : (n + 1) * count, :]
    for o in (2, 1, 3):
        send(fsend.at[at_y(o)], frecv.at[y], f_s, f_r.at[0], dev(x, at_y(o), z, c))
    frecv[y] = fsend[y]
    arrived(frecv.at[pl.ds(0, ny - 1)], f_r.at[0])
    total = frecv[0].astype(F32)
    for q in range(1, ny):
        total += frecv[q].astype(F32)
    out_ref[...] = total.astype(BF16)

    every = ybuf.shape[1]
    moved = every - 2 * both
    for sem, ref in (
        (zag_s, zbuf.at[pl.ds(0, (nz - 1) * tile), :]),
        (x_s, xsend.at[pl.ds(0, 2 * (nx * nc - 1) * slots), :]),
        (y1_s, ybuf.at[pl.ds(0, 2), :, :]),
        (y2_s, ybuf.at[0]),
        (p1_s, ybuf.at[0, pl.ds(0, moved), :]),
        (p2_s, r2buf.at[:, pl.ds(0, moved), :]),
        (b_s, xret.at[pl.ds(0, moved), :]),
        (home_s, rbuf0.at[:, pl.ds(0, 2 * slots), :]),
        (zrs_s, ybuf.at[0, pl.ds(0, (nz - 1) * tile), :]),
        (wrs_s, part0.at[pl.ds(0, (nz - 1) * tile // 2), :]),
        (f_s, fsend.at[pl.ds(0, ny - 1)]),
    ):
        awaits(ref, sem).wait_send()


def on_device(tokens, expert_ids, route_logits, expert_gate, expert_up, expert_down):
    n_ep, ny = lax.axis_size("ep"), N_DP
    nx, nc = CHIPS_X, CORES
    nz = n_ep // (nx * nc)
    tile, width = tokens.shape
    hidden = expert_gate.shape[2]
    quarter = width // ny
    col, slots = nz * tile, nz * CAP
    every = nx * nc * slots
    steps = nz // 4
    dma = pltpu.SemaphoreType.DMA
    vmem = pl.BlockSpec(memory_space=pltpu.VMEM)
    hbm = pl.BlockSpec(memory_space=pl.ANY)
    flops = 6 * every * width * hidden
    units = 2 * (nx // 2 + 1)
    home = 2 * nc * slots // 2
    return pl.pallas_call(
        functools.partial(kernel, nx, nz),
        out_shape=jax.ShapeDtypeStruct((tile // ny, width), BF16),
        in_specs=[vmem, vmem, hbm, hbm, hbm, hbm],
        out_specs=vmem,
        scratch_shapes=[
            pltpu.VMEM((width, hidden), BF16),
            pltpu.VMEM((width, hidden), BF16),
            pltpu.VMEM((hidden, width), BF16),
            pltpu.VMEM((col, quarter + 128), BF16),
            pltpu.VMEM((every, col // 2), BF16),
            pltpu.VMEM((every, quarter), BF16),
            pltpu.VMEM((ny, every, quarter), BF16),
            pltpu.VMEM((ny, every, quarter), BF16),
            pltpu.VMEM((2, every // 2, quarter), BF16),
            pltpu.VMEM((2, every, quarter), BF16),
            pltpu.VMEM((every, quarter), BF16),
            pltpu.VMEM((every, quarter), BF16),
            pltpu.VMEM((ny, home, quarter), BF16),
            pltpu.VMEM((col, quarter), F32),
            pltpu.VMEM((col, width - quarter), F32),
            pltpu.VMEM((2 * steps, 2, tile, quarter), BF16),
            pltpu.VMEM((2 * steps, 2, tile, quarter), BF16),
            pltpu.VMEM((2 * steps, 2, tile, width - quarter), BF16),
            pltpu.VMEM((2 * steps, 2, tile, width - quarter), BF16),
            pltpu.VMEM((ny, tile // ny, width), BF16),
            pltpu.VMEM((ny, tile // ny, width), BF16),
            dma((4,)),
            dma((11,)),
            dma((2 * steps,)), dma((2,)),
            dma((units,)), dma((units,)), dma((units,)), dma((units,)), dma((units,)), dma((units,)),
            dma((2 * steps,)), dma((2 * steps,)), dma((1,)),
        ],
        compiler_params=pltpu.CompilerParams(
            collective_id=0, has_side_effects=True, vmem_limit_bytes=56 * 1024 * 1024
        ),
        cost_estimate=pl.CostEstimate(flops=flops, bytes_accessed=8 << 20, transcendentals=0),
    )(expert_ids.T, route_logits.T, tokens, expert_gate, expert_up, expert_down)


def solution(mesh):
    placed = (
        P("ep", None),
        P("ep", None),
        P("ep", None),
        P("ep", None, "dp"),
        P("ep", None, "dp"),
        P("ep", "dp", None),
    )
    return jax.shard_map(
        on_device, mesh=mesh, in_specs=placed, out_specs=P(("ep", "dp"), None), check_vma=False
    )
```

```python
import functools

import jax
import jax.numpy as jnp
from jax import lax
from jax.experimental import pallas as pl
from jax.experimental.pallas import tpu as pltpu
from jax.sharding import PartitionSpec as P

MESH = pl.DeviceIdType.MESH
F32 = jnp.float32
BF16 = jnp.bfloat16
ROUTE_SCALE = 2.5
CAP = 4
CHIPS_X = 4
CORES = 2
N_DP = 4


def kernel(
    nx, nz, ids_ref, logits_ref, tok_hbm, wg_hbm, wu_hbm, wd_hbm, out_ref,
    wg, wu, wd, zbuf, swbuf, xsend, ybuf, obuf, r1buf, r2buf, xret, rbuf, rbuf0, part, part0,
    zs, zr, ws, wr, fsend, frecv,
    w_sem, s_sem, zag_r, zag_one, x_r, y1_r, y2_r, p1_r, p2_r, b_r, zrs_r, wrs_r, f_r,
):
    nc, ny = CORES, N_DP
    tile, width = tok_hbm.shape
    quarter = width // ny
    top = ids_ref.shape[0]
    steps = nz // 4
    mid = steps // 2
    parts = [(-2, -1, 0, 1)]
    if nz > 8:
        parts.append((2, 3, -4, -3))
    parts.append(tuple(range(nz // 4 if nz > 8 else 2, nz - (4 if nz > 8 else 2))))
    far = len(parts) - 1
    order = [o % nz for part_ in parts for o in part_]
    starts = [sum(len(p) for p in parts[:i]) for i in range(len(parts))]
    slots = [len(p) * CAP for p in parts]
    both = [nc * n for n in slots]
    home_rows = sum(both)
    offsets = {2: (0, 1), 4: (0, 1, 3, 2)}[nx]
    units = [
        {2: ((1,), (0,)), 4: ((1, 2, 3), (0,)) if h < far else ((3,), (1, 2), (0,))}[nx]
        for h in range(len(parts))
    ]
    unit_index = {}
    for h in range(len(parts)):
        for u in range(len(units[h])):
            unit_index[h, u] = len(unit_index)
    (zag_s, x_s, y1_s, y2_s, p1_s, p2_s, b_s, home_s, zrs_s, wrs_s, f_s) = [
        s_sem.at[i] for i in range(11)
    ]
    ep = lax.axis_index("ep")
    y = lax.axis_index("dp")
    c = lax.rem(ep, nc)
    z = lax.rem(lax.div(ep, nc), nz)
    x = lax.div(ep, nc * nz)

    def dev(x_, y_, z_, c_):
        return (((x_ * nz + z_) * nc + c_), y_)

    def to_x(g):
        return lax.rem(x + (nx - offsets[g]), nx)

    def from_x(g):
        return lax.rem(x + offsets[g], nx)

    def at_y(o):
        return lax.rem(y + (o + ny), ny)

    def at_z(o):
        return lax.rem(z + (o + nz), nz)

    def place(o):
        return order.index(o % nz) * tile

    def tokens_of(h):
        return starts[h] * tile, len(parts[h]) * tile

    def rows(start, size):
        if isinstance(start, int):
            return pl.ds(start, size)
        return pl.ds(pl.multiple_of(start, size), size)

    def base(h, g, c_):
        if g == 0:
            return sum(both[:h]) + c_ * slots[h]
        done = sum(both[:h]) * (nx - 1)
        return home_rows + done + (g - 1) * both[h] + c_ * slots[h]

    def span(h, u):
        first = min(units[h][u])
        return base(h, first, 0), len(units[h][u]) * both[h]

    def index(h, u):
        return unit_index[h, u]

    def home(h):
        return len(units[h]) - 1

    def send(src, dst, ssem, rsem, device):
        pltpu.make_async_remote_copy(
            src_ref=src, dst_ref=dst, send_sem=ssem, recv_sem=rsem,
            device_id=device, device_id_type=MESH,
        ).start()

    def awaits(ref, sem):
        return pltpu.make_async_remote_copy(
            src_ref=ref, dst_ref=ref, send_sem=sem, recv_sem=sem,
            device_id=dev(x, y, z, 1 - c), device_id_type=MESH,
        )

    def arrived(ref, sem):
        awaits(ref, sem).wait_recv()

    barrier = pltpu.get_barrier_semaphore()
    peers = [dev(x, y, at_z(o), c) for o in (1, -1, 2, -2)]
    peers += [dev(from_x(g), y, z, c_) for g in range(1, nx) for c_ in range(nc)]
    peers += [dev(x, y, z, 1 - c)]
    peers += [dev(x, at_y(o), z, c) for o in range(1, ny)]
    for peer in peers:
        pl.semaphore_signal(barrier, inc=1, device_id=peer, device_id_type=MESH)

    own = pl.ds(place(0), tile)
    mine = pltpu.make_async_copy(
        tok_hbm.at[:, pl.ds(pl.multiple_of(y * quarter, 128), quarter)],
        zbuf.at[own, pl.ds(0, quarter)], w_sem.at[3],
    )
    mine.start()
    scores = 1.0 / (1.0 + jnp.exp(-logits_ref[...]))
    wts = ROUTE_SCALE * scores / jnp.sum(scores, axis=0, keepdims=True)
    lane = lax.broadcasted_iota(jnp.int32, (top, 128), 1)
    sub = lax.broadcasted_iota(jnp.int32, (top, 128), 0)
    put_id = (lane == sub).astype(BF16)
    put_w = (lane == sub + top).astype(BF16)
    across = (((0,), (0,)), ((), ()))
    meta = lax.dot_general(
        ids_ref[...].astype(F32).astype(BF16), put_id, across, preferred_element_type=F32
    ) + lax.dot_general(wts.astype(BF16), put_w, across, preferred_element_type=F32)
    zbuf[own, quarter : quarter + 128] = meta.astype(BF16)

    loads = [
        pltpu.make_async_copy(s.at[0], d, w_sem.at[i])
        for i, (s, d) in enumerate(((wg_hbm, wg), (wu_hbm, wu), (wd_hbm, wd)))
    ]
    for load in loads:
        load.start()
    mine.wait()
    pl.semaphore_wait(barrier, len(peers))

    def zslot(d, k):
        return (0 if d > 0 else 1) * steps + (k - 1)

    def ready(k):
        return min(k - 1, far)

    def gather_send(k, d):
        o = -d * 2 * (k - 1)
        for hop in (2, 1):
            if hop == 2 and d < 0 and k == steps:
                continue
            rsem = zag_r.at[zslot(d, k)] if hop == 2 else zag_one.at[ready(k)]
            send(
                zbuf.at[pl.ds(place(o), tile), :], zbuf.at[pl.ds(place(o - d * hop), tile), :],
                zag_s, rsem, dev(x, y, at_z(d * hop), c),
            )

    def gather_step(k):
        for d in (1, -1):
            if d > 0 or k < steps:
                arrived(zbuf.at[pl.ds(0, tile), :], zag_r.at[zslot(d, k)])
            if k < steps:
                gather_send(k + 1, d)

    def gather_rest(h):
        count = sum(ready(k) == h for k in range(1, steps + 1))
        arrived(zbuf.at[pl.ds(0, 2 * count * tile), :], zag_one.at[h])

    def routes(h):
        first, col = tokens_of(h)
        pick = (
            lax.broadcasted_iota(jnp.int32, (2 * top, 128), 0)
            == lax.broadcasted_iota(jnp.int32, (2 * top, 128), 1)
        ).astype(BF16)
        by_token = lax.dot_general(
            pick, zbuf[first : first + col, quarter : quarter + 128],
            (((1,), (1,)), ((), ())), preferred_element_type=F32,
        )
        lanes = nx * nc
        j = lax.broadcasted_iota(jnp.int32, (lanes, col), 0)
        jg, jc = lax.div(j, nc), lax.rem(j, nc)
        off = jnp.zeros_like(jg)
        for g, o in enumerate(offsets):
            off = jnp.where(jg == g, nx - o, off)
        expert = ((lax.rem(x + off, nx) * nz + z) * nc + jc).astype(F32)
        named = jnp.zeros((lanes, col), F32)
        weight = jnp.zeros((lanes, col), F32)
        for k in range(top):
            hit = by_token[k : k + 1, :] == expert
            named = jnp.where(hit, 1.0, named)
            weight = jnp.where(hit, by_token[top + k : top + k + 1, :], weight)
        t_row = lax.broadcasted_iota(jnp.int32, (col, col), 0)
        t_col = lax.broadcasted_iota(jnp.int32, (col, col), 1)
        before = ((t_row < t_col) & (lax.div(t_row, tile) == lax.div(t_col, tile))).astype(BF16)
        rank = jnp.dot(named.astype(BF16), before, preferred_element_type=F32)
        return jnp.where(named > 0.5, rank, -1.0), weight

    def unit_of(h, g):
        return [g in unit for unit in units[h]].index(True)

    def select(h, g, rank, weight):
        first, col = tokens_of(h)
        s_row = lax.broadcasted_iota(jnp.int32, (slots[h], col), 0)
        s_col = lax.broadcasted_iota(jnp.int32, (slots[h], col), 1)
        in_block = lax.div(s_row, CAP) == lax.div(s_col, tile)
        want = jnp.where(in_block, lax.rem(s_row, CAP).astype(F32), -2.0)
        recv = x_r.at[index(h, unit_of(h, g))]
        chosen = []
        for c_ in range(nc):
            i = g * nc + c_
            hit = rank[i : i + 1, :] == want
            chosen.append(jnp.where(hit, 1.0, 0.0).astype(BF16))
            swbuf[pl.ds(base(h, g, c_), slots[h]), 0:col] = jnp.where(
                hit, weight[i : i + 1, :], 0.0
            ).astype(BF16)
        xsend[pl.ds(base(h, g, 0), both[h]), :] = jnp.dot(
            jnp.concatenate(chosen, axis=0), zbuf[first : first + col, 0:quarter],
            preferred_element_type=F32,
        ).astype(BF16)
        land = ybuf.at[y, rows(base(h, g, c), slots[h]), :]
        if g > 0:
            for c_ in range(nc):
                send(
                    xsend.at[pl.ds(base(h, g, c_), slots[h]), :], land, x_s,
                    recv, dev(to_x(g), y, z, c_),
                )
        else:
            other = 1 - c
            send(
                xsend.at[rows(base(h, g, other), slots[h]), :], land, x_s,
                recv, dev(x, y, z, other),
            )
            here = rows(base(h, g, c), slots[h])
            ybuf[y, here, :] = xsend[here, :]

    def x_wait(h, u):
        start, size = span(h, u)
        size = slots[h] if u == home(h) else size
        arrived(ybuf.at[y, pl.ds(start, size), :], x_r.at[index(h, u)])

    def spread(h, u):
        x_wait(h, u)
        start, size = span(h, u)
        block = ybuf.at[y, pl.ds(start, size), :]
        for d in (1, -1):
            send(block, block, y1_s, y1_r.at[index(h, u)], dev(x, at_y(d), z, c))

    def forward(h, u):
        start, size = span(h, u)
        arrived(ybuf.at[pl.ds(0, 2), pl.ds(start, size), :], y1_r.at[index(h, u)])
        for n, d in enumerate((1, -1)):
            block = ybuf.at[at_y(-d), pl.ds(start + n * size // 2, size // 2), :]
            send(block, block, y2_s, y2_r.at[index(h, u)], dev(x, at_y(d), z, c))

    def y_wait(h, u):
        arrived(ybuf.at[0, pl.ds(*span(h, u)), :], y2_r.at[index(h, u)])

    def experts(start, size):
        here = pl.ds(start, size)
        gate = jnp.zeros((size, wg.shape[1]), F32)
        upper = jnp.zeros((size, wg.shape[1]), F32)
        for q in range(ny):
            piece = ybuf[q, here, :]
            deep = pl.ds(q * quarter, quarter)
            gate += jnp.dot(piece, wg[deep, :], preferred_element_type=F32)
            upper += jnp.dot(piece, wu[deep, :], preferred_element_type=F32)
        hidden = (gate / (1.0 + jnp.exp(-gate)) * upper).astype(BF16)
        for q in range(ny):
            obuf[q, here, :] = jnp.dot(
                hidden, wd[:, q * quarter : (q + 1) * quarter], preferred_element_type=F32
            ).astype(BF16)

    def compute(h, u):
        y_wait(h, u)
        experts(*span(h, u))

    def compute_home():
        for h in range(len(parts)):
            y_wait(h, home(h))
        experts(0, home_rows)
        for h in range(len(parts)):
            other = 1 - c
            send(
                obuf.at[:, rows(base(h, 0, other), slots[h]), :],
                rbuf0.at[:, rows(base(h, 0, c), slots[h]), :],
                home_s, b_r.at[index(h, home(h))], dev(x, y, z, other),
            )
            here = rows(base(h, 0, c), slots[h])
            for q in range(ny):
                rbuf0[q, here, :] = obuf[q, here, :]

    def combine_home():
        for h in range(len(parts)):
            arrived(rbuf0.at[:, pl.ds(base(h, 0, 0), slots[h]), :], b_r.at[index(h, home(h))])
            here = pl.ds(base(h, 0, 0), both[h])
            first, col = tokens_of(h)
            for o in range(ny):
                term = lax.dot_general(
                    swbuf[here, 0:col], rbuf0[at_y(o), here, :], across, preferred_element_type=F32
                )
                if o == 0:
                    part[first : first + col, :] = term
                else:
                    part0[first : first + col, (o - 1) * quarter : o * quarter] = term

    def give_one(h, u):
        start, size = span(h, u)
        for n, d in enumerate((1, -1)):
            send(
                obuf.at[at_y(2), pl.ds(start + n * size // 2, size // 2), :],
                r1buf.at[n, pl.ds(start // 2, size // 2), :],
                p1_s, p1_r.at[index(h, u)], dev(x, at_y(d), z, c),
            )

    def give_two(h, u):
        start, size = span(h, u)
        arrived(r1buf.at[:, pl.ds(start // 2, size // 2), :], p1_r.at[index(h, u)])
        for n, d in enumerate((1, -1)):
            here = pl.ds(start + n * size // 2, size // 2)
            q = at_y(d)
            got = r1buf[n, pl.ds(start // 2, size // 2), :]
            obuf[q, here, :] = (obuf[q, here, :].astype(F32) + got.astype(F32)).astype(BF16)
            here = pl.ds(start, size)
            send(
                obuf.at[q, here, :], r2buf.at[n, here, :],
                p2_s, p2_r.at[index(h, u)], dev(x, at_y(d), z, c),
            )

    def give_back(h, u):
        here = pl.ds(*span(h, u))
        arrived(r2buf.at[:, here, :], p2_r.at[index(h, u)])
        total = obuf[y, here, :].astype(F32) + r2buf[0, here, :].astype(F32)
        xret[here, :] = (total + r2buf[1, here, :].astype(F32)).astype(BF16)
        for g in units[h][u]:
            land = rbuf.at[rows(base(h, g, c), slots[h]), :]
            for c_ in range(nc):
                send(
                    xret.at[pl.ds(base(h, g, c_), slots[h]), :], land, b_s,
                    b_r.at[index(h, u)], dev(from_x(g), y, z, c_),
                )

    def combine(h, u):
        here = pl.ds(*span(h, u))
        first, col = tokens_of(h)
        arrived(rbuf.at[here, :], b_r.at[index(h, u)])
        part[first : first + col, :] += lax.dot_general(
            swbuf[here, 0:col], rbuf[here, :], across, preferred_element_type=F32
        )

    reach = nz // 2

    def reducer(source, src, dst, ssem, rsem):
        def block_of(o):
            return source[pl.ds(place(o), tile), :]

        def zsend(d, k, hop, value):
            n = zslot(d, k)
            src[n, hop - 1] = value.astype(BF16)
            send(src.at[n, hop - 1], dst.at[n, hop - 1], ssem, rsem.at[n], dev(x, y, at_z(d * hop), c))

        def zget(d, k):
            n = zslot(d, k)
            if d < 0 and k == 1:
                arrived(dst.at[n, 0], rsem.at[n])
                return dst[n, 0].astype(F32)
            arrived(dst.at[n], rsem.at[n])
            return dst[n, 0].astype(F32) + dst[n, 1].astype(F32)

        def own_hop(k):
            if k == 1:
                zsend(1, 1, 2, block_of(reach))
            for d in (1, -1):
                zsend(d, k, 1, block_of(d * (reach + 1 - 2 * k)))

        def next_hop(k):
            for d in (1, -1):
                zsend(d, k + 1, 2, block_of(d * (reach - 2 * k)) + zget(d, k))

        def finish():
            return block_of(0) + zget(1, steps) + zget(-1, steps)

        return own_hop, next_hop, finish

    own_hop, next_hop, finish = reducer(part, zs, zr, zrs_s, zrs_r)
    wide_own, wide_next, wide_finish = reducer(part0, ws, wr, wrs_s, wrs_r)

    def wide_step(k):
        if k < steps:
            wide_next(k)
            wide_own(k + 1)

    def choose(h):
        rank, weight = routes(h)
        for g in range(nx):
            select(h, g, rank, weight)

    near, between = 0, range(1, far)
    outer = range(len(units[far]) - 1)
    for d in (1, -1):
        gather_send(1, d)
    gather_step(1)
    gather_rest(near)
    choose(near)
    spread(near, home(near))
    for h in between:
        gather_step(h + 1)
    spread(near, 0)
    forward(near, home(near))
    for h in between:
        gather_rest(h)
        choose(h)
        spread(h, home(h))
    for k in range(far + 1, steps):
        gather_step(k)
    forward(near, 0)
    for h in between:
        spread(h, 0)
        forward(h, home(h))
    gather_step(steps)
    gather_rest(far)
    choose(far)
    spread(far, home(far))
    for h in between:
        forward(h, 0)
    forward(far, home(far))
    for u in outer:
        spread(far, u)
    for load in loads:
        load.wait()
    for h in range(far):
        compute(h, 0)
    compute_home()
    forward(far, 0)
    combine_home()
    wide_own(1)
    for u in outer[1:]:
        forward(far, u)
    for h in range(far - 1, -1, -1):
        give_one(h, 0)
    for u in outer:
        compute(far, u)
        give_one(far, u)
    wide_step(1)
    for u in outer:
        give_two(far, u)
    for h in range(far - 1, -1, -1):
        give_two(h, 0)
    wide_step(2)
    give_back(far, 0)
    for k in range(3, steps):
        wide_step(k)
    for u in outer[1:]:
        give_back(far, u)
    for h in between:
        give_back(h, 0)
    for u in outer:
        combine(far, u)
    for k in range(1, mid + 1):
        own_hop(k)
    give_back(near, 0)
    for k in range(1, mid):
        next_hop(k)
    wide = wide_finish()
    for h in between:
        combine(h, 0)
        next_hop(mid)
        own_hop(mid + 1)
    combine(near, 0)
    own_hop(steps)
    next_hop(steps - 1)
    main = finish()

    count = out_ref.shape[0]
    for o in range(ny):
        share = (main if o == 0 else wide[:, (o - 1) * quarter : o * quarter]).astype(BF16)
        piece = pl.ds(pl.multiple_of(at_y(o) * quarter, 128), quarter)
        for n in range(ny):
            fsend[n, :, piece] = share[n * count : (n + 1) * count, :]
    for o in (2, 1, 3):
        send(fsend.at[at_y(o)], frecv.at[y], f_s, f_r.at[0], dev(x, at_y(o), z, c))
    frecv[y] = fsend[y]
    arrived(frecv.at[pl.ds(0, ny - 1)], f_r.at[0])
    total = frecv[0].astype(F32)
    for q in range(1, ny):
        total += frecv[q].astype(F32)
    out_ref[...] = total.astype(BF16)

    every = ybuf.shape[1]
    moved = every - home_rows
    sent = sum(slots)
    for sem, ref in (
        (zag_s, zbuf.at[pl.ds(0, (nz - 1) * tile), :]),
        (x_s, xsend.at[pl.ds(0, (nx * nc - 1) * sent), :]),
        (y1_s, ybuf.at[pl.ds(0, 2), :, :]),
        (y2_s, ybuf.at[0]),
        (p1_s, ybuf.at[0, pl.ds(0, moved), :]),
        (p2_s, r2buf.at[:, pl.ds(0, moved), :]),
        (b_s, xret.at[pl.ds(0, moved), :]),
        (home_s, rbuf0.at[:, pl.ds(0, sent), :]),
        (zrs_s, ybuf.at[0, pl.ds(0, (nz - 1) * tile), :]),
        (wrs_s, part0.at[pl.ds(0, (nz - 1) * tile // 2), :]),
        (f_s, fsend.at[pl.ds(0, ny - 1)]),
    ):
        awaits(ref, sem).wait_send()


def on_device(tokens, expert_ids, route_logits, expert_gate, expert_up, expert_down):
    n_ep, ny = lax.axis_size("ep"), N_DP
    nx, nc = CHIPS_X, CORES
    nz = n_ep // (nx * nc)
    tile, width = tokens.shape
    hidden = expert_gate.shape[2]
    quarter = width // ny
    col, slots = nz * tile, nz * CAP
    every = nx * nc * slots
    steps = nz // 4
    dma = pltpu.SemaphoreType.DMA
    vmem = pl.BlockSpec(memory_space=pltpu.VMEM)
    hbm = pl.BlockSpec(memory_space=pl.ANY)
    flops = 6 * every * width * hidden
    units = 7
    home = 2 * nc * slots // 2
    return pl.pallas_call(
        functools.partial(kernel, nx, nz),
        out_shape=jax.ShapeDtypeStruct((tile // ny, width), BF16),
        in_specs=[vmem, vmem, hbm, hbm, hbm, hbm],
        out_specs=vmem,
        scratch_shapes=[
            pltpu.VMEM((width, hidden), BF16),
            pltpu.VMEM((width, hidden), BF16),
            pltpu.VMEM((hidden, width), BF16),
            pltpu.VMEM((col, quarter + 128), BF16),
            pltpu.VMEM((every, col // 2), BF16),
            pltpu.VMEM((every, quarter), BF16),
            pltpu.VMEM((ny, every, quarter), BF16),
            pltpu.VMEM((ny, every, quarter), BF16),
            pltpu.VMEM((2, every // 2, quarter), BF16),
            pltpu.VMEM((2, every, quarter), BF16),
            pltpu.VMEM((every, quarter), BF16),
            pltpu.VMEM((every, quarter), BF16),
            pltpu.VMEM((ny, home, quarter), BF16),
            pltpu.VMEM((col, quarter), F32),
            pltpu.VMEM((col, width - quarter), F32),
            pltpu.VMEM((2 * steps, 2, tile, quarter), BF16),
            pltpu.VMEM((2 * steps, 2, tile, quarter), BF16),
            pltpu.VMEM((2 * steps, 2, tile, width - quarter), BF16),
            pltpu.VMEM((2 * steps, 2, tile, width - quarter), BF16),
            pltpu.VMEM((ny, tile // ny, width), BF16),
            pltpu.VMEM((ny, tile // ny, width), BF16),
            dma((4,)),
            dma((11,)),
            dma((2 * steps,)), dma((3,)),
            dma((units,)), dma((units,)), dma((units,)), dma((units,)), dma((units,)), dma((units,)),
            dma((2 * steps,)), dma((2 * steps,)), dma((1,)),
        ],
        compiler_params=pltpu.CompilerParams(
            collective_id=0, has_side_effects=True, vmem_limit_bytes=56 * 1024 * 1024
        ),
        cost_estimate=pl.CostEstimate(flops=flops, bytes_accessed=8 << 20, transcendentals=0),
    )(expert_ids.T, route_logits.T, tokens, expert_gate, expert_up, expert_down)


def solution(mesh):
    placed = (
        P("ep", None),
        P("ep", None),
        P("ep", None),
        P("ep", None, "dp"),
        P("ep", None, "dp"),
        P("ep", "dp", None),
    )
    return jax.shard_map(
        on_device, mesh=mesh, in_specs=placed, out_specs=P(("ep", "dp"), None), check_vma=False
    )
```

```python
import functools

import jax
import jax.numpy as jnp
from jax import lax
from jax.experimental import pallas as pl
from jax.experimental.pallas import tpu as pltpu
from jax.sharding import PartitionSpec as P

MESH = pl.DeviceIdType.MESH
F32 = jnp.float32
BF16 = jnp.bfloat16
ROUTE_SCALE = 2.5
CAP = 4
CHIPS_X = 4
CORES = 2
N_DP = 4


def kernel(
    nx, nz, ids_hbm, logits_hbm, tok_hbm, wg_hbm, wu_hbm, wd_hbm, out_ref,
    ids_ref, logits_ref, wg, wu, wd, zbuf, swbuf, xsend, ybuf, obuf, r1buf, r2buf, xret, rbuf, rbuf0, part, part0,
    zs, zr, ws, wr, ds, dr, fsend, frecv,
    w_sem, s_sem, zag_r, zag_one, x_r, y1_r, y2_r, p1_r, p2_r, b_r, zrs_r, wrs_r, f_r, d_r,
):
    nc, ny = CORES, N_DP
    tile, width = tok_hbm.shape
    quarter = width // ny
    top = ids_ref.shape[0]
    steps = nz // 4
    mid = steps // 2
    parts = [(-2, -1, 0, 1)]
    if nz > 8:
        parts.append((2, 3, -4, -3))
    parts.append(tuple(range(nz // 4 if nz > 8 else 2, nz - (4 if nz > 8 else 2))))
    far = len(parts) - 1
    order = [o % nz for part_ in parts for o in part_]
    starts = [sum(len(p) for p in parts[:i]) for i in range(len(parts))]
    slots = [len(p) * CAP for p in parts]
    both = [nc * n for n in slots]
    home_rows = sum(both)
    offsets = {2: (0, 1), 4: (0, 1, 3, 2)}[nx]
    units = [
        {2: ((1,), (0,)), 4: ((1, 2, 3), (0,)) if h < far else ((1, 2), (3,), (0,))}[nx]
        for h in range(len(parts))
    ]
    unit_index = {}
    for h in range(len(parts)):
        for u in range(len(units[h])):
            unit_index[h, u] = len(unit_index)
    (zag_s, x_s, y1_s, y2_s, p1_s, p2_s, b_s, home_s, zrs_s, wrs_s, f_s, d_s) = [
        s_sem.at[i] for i in range(12)
    ]
    ep = lax.axis_index("ep")
    y = lax.axis_index("dp")
    c = lax.rem(ep, nc)
    z = lax.rem(lax.div(ep, nc), nz)
    x = lax.div(ep, nc * nz)

    def dev(x_, y_, z_, c_):
        return (((x_ * nz + z_) * nc + c_), y_)

    def to_x(g):
        return lax.rem(x + (nx - offsets[g]), nx)

    def from_x(g):
        return lax.rem(x + offsets[g], nx)

    def at_y(o):
        return lax.rem(y + (o + ny), ny)

    def at_z(o):
        return lax.rem(z + (o + nz), nz)

    def place(o):
        return order.index(o % nz) * tile

    def tokens_of(h):
        return starts[h] * tile, len(parts[h]) * tile

    def rows(start, size):
        if isinstance(start, int):
            return pl.ds(start, size)
        return pl.ds(pl.multiple_of(start, size), size)

    def base(h, g, c_):
        if g == 0:
            return sum(both[:h]) + c_ * slots[h]
        done = sum(both[:h]) * (nx - 1)
        return home_rows + done + (g - 1) * both[h] + c_ * slots[h]

    def span(h, u):
        first = min(units[h][u])
        return base(h, first, 0), len(units[h][u]) * both[h]

    def index(h, u):
        return unit_index[h, u]

    def home(h):
        return len(units[h]) - 1

    def send(src, dst, ssem, rsem, device):
        pltpu.make_async_remote_copy(
            src_ref=src, dst_ref=dst, send_sem=ssem, recv_sem=rsem,
            device_id=device, device_id_type=MESH,
        ).start()

    def awaits(ref, sem):
        return pltpu.make_async_remote_copy(
            src_ref=ref, dst_ref=ref, send_sem=sem, recv_sem=sem,
            device_id=dev(x, y, z, 1 - c), device_id_type=MESH,
        )

    def arrived(ref, sem):
        awaits(ref, sem).wait_recv()

    barrier = pltpu.get_barrier_semaphore()
    peers = [dev(x, y, at_z(o * d), c) for o in range(1, nz // 4 + 1) for d in (1, -1)]
    peers += [dev(from_x(g), y, z, c_) for g in range(1, nx) for c_ in range(nc)]
    peers += [dev(x, y, z, 1 - c)]
    peers += [dev(x, at_y(o), z, c) for o in range(1, ny)]
    for peer in peers:
        pl.semaphore_signal(barrier, inc=1, device_id=peer, device_id_type=MESH)

    own = pl.ds(place(0), tile)
    mine = pltpu.make_async_copy(
        tok_hbm.at[:, pl.ds(pl.multiple_of(y * quarter, 128), quarter)],
        zbuf.at[own, pl.ds(0, quarter)], w_sem.at[3],
    )
    names = [
        pltpu.make_async_copy(ids_hbm, ids_ref, w_sem.at[4]),
        pltpu.make_async_copy(logits_hbm, logits_ref, w_sem.at[5]),
    ]
    for copy in names:
        copy.start()
    mine.start()
    for copy in names:
        copy.wait()
    scores = 1.0 / (1.0 + jnp.exp(-logits_ref[...]))
    wts = ROUTE_SCALE * scores / jnp.sum(scores, axis=0, keepdims=True)
    lane = lax.broadcasted_iota(jnp.int32, (top, 128), 1)
    sub = lax.broadcasted_iota(jnp.int32, (top, 128), 0)
    put_id = (lane == sub).astype(BF16)
    put_w = (lane == sub + top).astype(BF16)
    across = (((0,), (0,)), ((), ()))
    meta = lax.dot_general(
        ids_ref[...].astype(F32).astype(BF16), put_id, across, preferred_element_type=F32
    ) + lax.dot_general(wts.astype(BF16), put_w, across, preferred_element_type=F32)
    zbuf[own, quarter : quarter + 128] = meta.astype(BF16)

    loads = [
        pltpu.make_async_copy(s.at[0], d, w_sem.at[i])
        for i, (s, d) in enumerate(((wg_hbm, wg), (wu_hbm, wu), (wd_hbm, wd)))
    ]
    for load in loads:
        load.start()
    mine.wait()
    pl.semaphore_wait(barrier, len(peers))

    def zslot(d, k):
        return (0 if d > 0 else 1) * steps + (k - 1)

    def ready(k):
        return min(k - 1, far)

    def gather_send(k, d):
        o = -d * 2 * (k - 1)
        for hop in (2, 1):
            if hop == 2 and d < 0 and k == steps:
                continue
            rsem = zag_r.at[zslot(d, k)] if hop == 2 else zag_one.at[ready(k)]
            send(
                zbuf.at[pl.ds(place(o), tile), :], zbuf.at[pl.ds(place(o - d * hop), tile), :],
                zag_s, rsem, dev(x, y, at_z(d * hop), c),
            )

    def gather_step(k):
        for d in (1, -1):
            if d > 0 or k < steps:
                arrived(zbuf.at[pl.ds(0, tile), :], zag_r.at[zslot(d, k)])
            if k < steps:
                gather_send(k + 1, d)

    def gather_rest(h):
        count = sum(ready(k) == h for k in range(1, steps + 1))
        arrived(zbuf.at[pl.ds(0, 2 * count * tile), :], zag_one.at[h])

    def routes(h):
        first, col = tokens_of(h)
        pick = (
            lax.broadcasted_iota(jnp.int32, (2 * top, 128), 0)
            == lax.broadcasted_iota(jnp.int32, (2 * top, 128), 1)
        ).astype(BF16)
        by_token = lax.dot_general(
            pick, zbuf[first : first + col, quarter : quarter + 128],
            (((1,), (1,)), ((), ())), preferred_element_type=F32,
        )
        lanes = nx * nc
        j = lax.broadcasted_iota(jnp.int32, (lanes, col), 0)
        jg, jc = lax.div(j, nc), lax.rem(j, nc)
        off = jnp.zeros_like(jg)
        for g, o in enumerate(offsets):
            off = jnp.where(jg == g, nx - o, off)
        expert = ((lax.rem(x + off, nx) * nz + z) * nc + jc).astype(F32)
        named = jnp.zeros((lanes, col), F32)
        weight = jnp.zeros((lanes, col), F32)
        for k in range(top):
            hit = by_token[k : k + 1, :] == expert
            named = jnp.where(hit, 1.0, named)
            weight = jnp.where(hit, by_token[top + k : top + k + 1, :], weight)
        t_row = lax.broadcasted_iota(jnp.int32, (col, col), 0)
        t_col = lax.broadcasted_iota(jnp.int32, (col, col), 1)
        before = ((t_row < t_col) & (lax.div(t_row, tile) == lax.div(t_col, tile))).astype(BF16)
        rank = jnp.dot(named.astype(BF16), before, preferred_element_type=F32)
        return jnp.where(named > 0.5, rank, -1.0), weight

    def unit_of(h, g):
        return [g in unit for unit in units[h]].index(True)

    def select(h, g, rank, weight):
        first, col = tokens_of(h)
        s_row = lax.broadcasted_iota(jnp.int32, (slots[h], col), 0)
        s_col = lax.broadcasted_iota(jnp.int32, (slots[h], col), 1)
        in_block = lax.div(s_row, CAP) == lax.div(s_col, tile)
        want = jnp.where(in_block, lax.rem(s_row, CAP).astype(F32), -2.0)
        recv = x_r.at[index(h, unit_of(h, g))]
        chosen = []
        for c_ in range(nc):
            i = g * nc + c_
            hit = rank[i : i + 1, :] == want
            chosen.append(jnp.where(hit, 1.0, 0.0).astype(BF16))
            swbuf[pl.ds(base(h, g, c_), slots[h]), 0:col] = jnp.where(
                hit, weight[i : i + 1, :], 0.0
            ).astype(BF16)
        xsend[pl.ds(base(h, g, 0), both[h]), :] = jnp.dot(
            jnp.concatenate(chosen, axis=0), zbuf[first : first + col, 0:quarter],
            preferred_element_type=F32,
        ).astype(BF16)
        land = ybuf.at[y, rows(base(h, g, c), slots[h]), :]
        if g > 0:
            for c_ in range(nc):
                send(
                    xsend.at[pl.ds(base(h, g, c_), slots[h]), :], land, x_s,
                    recv, dev(to_x(g), y, z, c_),
                )
        else:
            other = 1 - c
            send(
                xsend.at[rows(base(h, g, other), slots[h]), :], land, x_s,
                recv, dev(x, y, z, other),
            )
            here = rows(base(h, g, c), slots[h])
            ybuf[y, here, :] = xsend[here, :]

    def x_wait(h, u):
        start, size = span(h, u)
        size = slots[h] if u == home(h) else size
        arrived(ybuf.at[y, pl.ds(start, size), :], x_r.at[index(h, u)])

    def spread(h, u):
        x_wait(h, u)
        start, size = span(h, u)
        block = ybuf.at[y, pl.ds(start, size), :]
        for d in (1, -1):
            send(block, block, y1_s, y1_r.at[index(h, u)], dev(x, at_y(d), z, c))

    def forward(h, u):
        start, size = span(h, u)
        arrived(ybuf.at[pl.ds(0, 2), pl.ds(start, size), :], y1_r.at[index(h, u)])
        for n, d in enumerate((1, -1)):
            block = ybuf.at[at_y(-d), pl.ds(start + n * size // 2, size // 2), :]
            send(block, block, y2_s, y2_r.at[index(h, u)], dev(x, at_y(d), z, c))

    def y_wait(h, u):
        arrived(ybuf.at[0, pl.ds(*span(h, u)), :], y2_r.at[index(h, u)])

    def experts(start, size):
        here = pl.ds(start, size)
        gate = jnp.zeros((size, wg.shape[1]), F32)
        upper = jnp.zeros((size, wg.shape[1]), F32)
        for q in range(ny):
            piece = ybuf[q, here, :]
            deep = pl.ds(q * quarter, quarter)
            gate += jnp.dot(piece, wg[deep, :], preferred_element_type=F32)
            upper += jnp.dot(piece, wu[deep, :], preferred_element_type=F32)
        hidden = (gate / (1.0 + jnp.exp(-gate)) * upper).astype(BF16)
        for q in range(ny):
            obuf[q, here, :] = jnp.dot(
                hidden, wd[:, q * quarter : (q + 1) * quarter], preferred_element_type=F32
            ).astype(BF16)

    def compute(h, u):
        y_wait(h, u)
        experts(*span(h, u))

    def compute_home():
        for h in range(len(parts)):
            y_wait(h, home(h))
        experts(0, home_rows)
        for h in range(len(parts)):
            other = 1 - c
            send(
                obuf.at[:, rows(base(h, 0, other), slots[h]), :],
                rbuf0.at[:, rows(base(h, 0, c), slots[h]), :],
                home_s, b_r.at[index(h, home(h))], dev(x, y, z, other),
            )
            here = rows(base(h, 0, c), slots[h])
            for q in range(ny):
                rbuf0[q, here, :] = obuf[q, here, :]

    def combine_home():
        for h in range(len(parts)):
            arrived(rbuf0.at[:, pl.ds(base(h, 0, 0), slots[h]), :], b_r.at[index(h, home(h))])
            here = pl.ds(base(h, 0, 0), both[h])
            first, col = tokens_of(h)
            for o in range(ny):
                term = lax.dot_general(
                    swbuf[here, 0:col], rbuf0[at_y(o), here, :], across, preferred_element_type=F32
                )
                if o == 0:
                    part[first : first + col, :] = term
                else:
                    part0[first : first + col, (o - 1) * quarter : o * quarter] = term

    def give_one(h, u):
        start, size = span(h, u)
        for n, d in enumerate((1, -1)):
            send(
                obuf.at[at_y(2), pl.ds(start + n * size // 2, size // 2), :],
                r1buf.at[n, pl.ds(start // 2, size // 2), :],
                p1_s, p1_r.at[index(h, u)], dev(x, at_y(d), z, c),
            )

    def give_two(h, u):
        start, size = span(h, u)
        arrived(r1buf.at[:, pl.ds(start // 2, size // 2), :], p1_r.at[index(h, u)])
        for n, d in enumerate((1, -1)):
            here = pl.ds(start + n * size // 2, size // 2)
            q = at_y(d)
            got = r1buf[n, pl.ds(start // 2, size // 2), :]
            obuf[q, here, :] = (obuf[q, here, :].astype(F32) + got.astype(F32)).astype(BF16)
            here = pl.ds(start, size)
            send(
                obuf.at[q, here, :], r2buf.at[n, here, :],
                p2_s, p2_r.at[index(h, u)], dev(x, at_y(d), z, c),
            )

    def give_back(h, u):
        here = pl.ds(*span(h, u))
        arrived(r2buf.at[:, here, :], p2_r.at[index(h, u)])
        total = obuf[y, here, :].astype(F32) + r2buf[0, here, :].astype(F32)
        xret[here, :] = (total + r2buf[1, here, :].astype(F32)).astype(BF16)
        for g in units[h][u]:
            land = rbuf.at[rows(base(h, g, c), slots[h]), :]
            for c_ in range(nc):
                send(
                    xret.at[pl.ds(base(h, g, c_), slots[h]), :], land, b_s,
                    b_r.at[index(h, u)], dev(from_x(g), y, z, c_),
                )

    def combine(h, u):
        here = pl.ds(*span(h, u))
        first, col = tokens_of(h)
        arrived(rbuf.at[here, :], b_r.at[index(h, u)])
        part[first : first + col, :] += lax.dot_general(
            swbuf[here, 0:col], rbuf[here, :], across, preferred_element_type=F32
        )

    reach = nz // 2

    def reducer(source, src, dst, ssem, rsem):
        def block_of(o):
            return source[pl.ds(place(o), tile), :]

        def zsend(d, k, hop, value):
            n = zslot(d, k)
            src[n, hop - 1] = value.astype(BF16)
            send(src.at[n, hop - 1], dst.at[n, hop - 1], ssem, rsem.at[n], dev(x, y, at_z(d * hop), c))

        def zget(d, k):
            n = zslot(d, k)
            if d < 0 and k == 1:
                arrived(dst.at[n, 0], rsem.at[n])
                return dst[n, 0].astype(F32)
            arrived(dst.at[n], rsem.at[n])
            return dst[n, 0].astype(F32) + dst[n, 1].astype(F32)

        def own_hop(k):
            if k == 1:
                zsend(1, 1, 2, block_of(reach))
            for d in (1, -1):
                zsend(d, k, 1, block_of(d * (reach + 1 - 2 * k)))

        def next_hop(k):
            for d in (1, -1):
                zsend(d, k + 1, 2, block_of(d * (reach - 2 * k)) + zget(d, k))

        def finish():
            return block_of(0) + zget(1, steps) + zget(-1, steps)

        return own_hop, next_hop, finish, block_of, zget

    own_hop, next_hop, _, block_of, zget = reducer(part, zs, zr, zrs_s, zrs_r)
    wide_own, wide_next, wide_finish, _, _ = reducer(part0, ws, wr, wrs_s, wrs_r)

    def wide_step(k):
        if k < steps:
            wide_next(k)
            wide_own(k + 1)

    def choose(h):
        rank, weight = routes(h)
        for g in range(nx):
            select(h, g, rank, weight)

    direct = nz // 4

    def straight(o):
        value = block_of(o)
        if abs(o) == direct:
            value = value + zget(1 if o > 0 else -1, mid)
        n = (o if o > 0 else direct - o) - 1
        ds[n] = value.astype(BF16)
        send(ds.at[n], dr.at[n], d_s, d_r.at[0], dev(x, y, at_z(o), c))

    def gathered():
        arrived(dr, d_r.at[0])
        total = block_of(0)
        for n in range(2 * direct):
            total += dr[n].astype(F32)
        return total

    near, between = 0, range(1, far)
    outer = range(len(units[far]) - 1)
    for d in (1, -1):
        gather_send(1, d)
    gather_step(1)
    gather_rest(near)
    choose(near)
    spread(near, home(near))
    for h in between:
        gather_step(h + 1)
    spread(near, 0)
    for h in between:
        gather_rest(h)
        choose(h)
        spread(h, home(h))
    forward(near, home(near))
    for k in range(far + 1, steps):
        gather_step(k)
    for h in between:
        spread(h, 0)
    gather_step(steps)
    gather_rest(far)
    choose(far)
    spread(far, home(far))
    forward(near, 0)
    for h in between:
        forward(h, home(h))
    spread(far, 0)
    for h in between:
        forward(h, 0)
    forward(far, home(far))
    for u in outer[1:]:
        spread(far, u)
    for load in loads:
        load.wait()
    for h in range(far):
        compute(h, 0)
    compute_home()
    forward(far, 0)
    combine_home()
    wide_own(1)
    for u in outer[1:]:
        forward(far, u)
    for h in between:
        give_one(h, 0)
    for u in outer:
        compute(far, u)
        give_one(far, u)
    give_one(near, 0)
    wide_step(1)
    for u in outer:
        give_two(far, u)
    for h in range(far - 1, -1, -1):
        give_two(h, 0)
    wide_step(2)
    for u in outer:
        give_back(far, u)
    for k in range(3, steps):
        wide_step(k)
    for h in between:
        give_back(h, 0)
    for u in outer:
        combine(far, u)
    for k in range(1, mid + 1):
        own_hop(k)
    give_back(near, 0)
    for k in range(1, mid):
        next_hop(k)
    for h in between:
        combine(h, 0)
        for o in (3, -3, 2):
            straight(o)
    wide = wide_finish()
    combine(near, 0)
    for o in range(2 if nz > 8 else 1, 0, -1):
        straight(-o)
    straight(1)
    for o in (direct, -direct):
        straight(o)
    main = gathered()

    count = out_ref.shape[0]
    for o in range(ny):
        share = (main if o == 0 else wide[:, (o - 1) * quarter : o * quarter]).astype(BF16)
        piece = pl.ds(pl.multiple_of(at_y(o) * quarter, 128), quarter)
        for n in range(ny):
            fsend[n, :, piece] = share[n * count : (n + 1) * count, :]
    for o in (2, 1, 3):
        send(fsend.at[at_y(o)], frecv.at[y], f_s, f_r.at[0], dev(x, at_y(o), z, c))
    frecv[y] = fsend[y]
    arrived(frecv.at[pl.ds(0, ny - 1)], f_r.at[0])
    total = frecv[0].astype(F32)
    for q in range(1, ny):
        total += frecv[q].astype(F32)
    out_ref[...] = total.astype(BF16)

    every = ybuf.shape[1]
    moved = every - home_rows
    sent = sum(slots)
    for sem, ref in (
        (zag_s, zbuf.at[pl.ds(0, (nz - 1) * tile), :]),
        (x_s, xsend.at[pl.ds(0, (nx * nc - 1) * sent), :]),
        (y1_s, ybuf.at[pl.ds(0, 2), :, :]),
        (y2_s, ybuf.at[0]),
        (p1_s, ybuf.at[0, pl.ds(0, moved), :]),
        (p2_s, r2buf.at[:, pl.ds(0, moved), :]),
        (b_s, xret.at[pl.ds(0, moved), :]),
        (home_s, rbuf0.at[:, pl.ds(0, sent), :]),
        (zrs_s, ybuf.at[0, pl.ds(0, (4 * mid - 1) * tile), :]),
        (d_s, ds),
        (wrs_s, part0.at[pl.ds(0, (nz - 1) * tile // 2), :]),
        (f_s, fsend.at[pl.ds(0, ny - 1)]),
    ):
        awaits(ref, sem).wait_send()


def on_device(tokens, expert_ids, route_logits, expert_gate, expert_up, expert_down):
    n_ep, ny = lax.axis_size("ep"), N_DP
    nx, nc = CHIPS_X, CORES
    nz = n_ep // (nx * nc)
    tile, width = tokens.shape
    hidden = expert_gate.shape[2]
    quarter = width // ny
    col, slots = nz * tile, nz * CAP
    every = nx * nc * slots
    steps = nz // 4
    dma = pltpu.SemaphoreType.DMA
    vmem = pl.BlockSpec(memory_space=pltpu.VMEM)
    hbm = pl.BlockSpec(memory_space=pl.ANY)
    flops = 6 * every * width * hidden
    units = 7
    home = 2 * nc * slots // 2
    return pl.pallas_call(
        functools.partial(kernel, nx, nz),
        out_shape=jax.ShapeDtypeStruct((tile // ny, width), BF16),
        in_specs=[hbm] * 6,
        out_specs=vmem,
        scratch_shapes=[
            pltpu.VMEM(expert_ids.shape[::-1], jnp.int32),
            pltpu.VMEM(expert_ids.shape[::-1], F32),
            pltpu.VMEM((width, hidden), BF16),
            pltpu.VMEM((width, hidden), BF16),
            pltpu.VMEM((hidden, width), BF16),
            pltpu.VMEM((col, quarter + 128), BF16),
            pltpu.VMEM((every, col // 2), BF16),
            pltpu.VMEM((every, quarter), BF16),
            pltpu.VMEM((ny, every, quarter), BF16),
            pltpu.VMEM((ny, every, quarter), BF16),
            pltpu.VMEM((2, every // 2, quarter), BF16),
            pltpu.VMEM((2, every, quarter), BF16),
            pltpu.VMEM((every, quarter), BF16),
            pltpu.VMEM((every, quarter), BF16),
            pltpu.VMEM((ny, home, quarter), BF16),
            pltpu.VMEM((col, quarter), F32),
            pltpu.VMEM((col, width - quarter), F32),
            pltpu.VMEM((2 * steps, 2, tile, quarter), BF16),
            pltpu.VMEM((2 * steps, 2, tile, quarter), BF16),
            pltpu.VMEM((2 * steps, 2, tile, width - quarter), BF16),
            pltpu.VMEM((2 * steps, 2, tile, width - quarter), BF16),
            pltpu.VMEM((2 * steps, tile, quarter), BF16),
            pltpu.VMEM((2 * steps, tile, quarter), BF16),
            pltpu.VMEM((ny, tile // ny, width), BF16),
            pltpu.VMEM((ny, tile // ny, width), BF16),
            dma((6,)),
            dma((12,)),
            dma((2 * steps,)), dma((3,)),
            dma((units,)), dma((units,)), dma((units,)), dma((units,)), dma((units,)), dma((units,)),
            dma((2 * steps,)), dma((2 * steps,)), dma((1,)), dma((1,)),
        ],
        compiler_params=pltpu.CompilerParams(
            collective_id=0, has_side_effects=True, vmem_limit_bytes=56 * 1024 * 1024
        ),
        cost_estimate=pl.CostEstimate(flops=flops, bytes_accessed=8 << 20, transcendentals=0),
    )(expert_ids.T, route_logits.T, tokens, expert_gate, expert_up, expert_down)


def solution(mesh):
    placed = (
        P("ep", None),
        P("ep", None),
        P("ep", None),
        P("ep", None, "dp"),
        P("ep", None, "dp"),
        P("ep", "dp", None),
    )
    return jax.shard_map(
        on_device, mesh=mesh, in_specs=placed, out_specs=P(("ep", "dp"), None), check_vma=False
    )
```

```python
import functools

import jax
import jax.numpy as jnp
from jax import lax
from jax.experimental import pallas as pl
from jax.experimental.pallas import tpu as pltpu
from jax.sharding import PartitionSpec as P

MESH = pl.DeviceIdType.MESH
F32 = jnp.float32
BF16 = jnp.bfloat16
ROUTE_SCALE = 2.5
CAP = 4
CHIPS_X = 4
CORES = 2
N_DP = 4


def kernel(
    nx, nz, ids_hbm, logits_hbm, tok_hbm, wg_hbm, wu_hbm, wd_hbm, out_ref,
    ids_ref, logits_ref, wg, wu, wd, zbuf, swbuf, xsend, ybuf, obuf, r1buf, r2buf, xret, rbuf, rbuf0, part, part0,
    zs, zr, ws, wr, ds, dr, fsend, frecv,
    w_sem, s_sem, zag_r, zag_one, x_r, y1_r, y2_r, p1_r, p2_r, b_r, zrs_r, wrs_r, f_r, d_r,
):
    nc, ny = CORES, N_DP
    tile, width = tok_hbm.shape
    quarter = width // ny
    top = ids_ref.shape[0]
    steps = nz // 4
    mid = steps // 2
    parts = [(-2, -1, 0, 1)]
    if nz > 8:
        parts.append((2, 3, -4, -3))
    parts.append(tuple(range(nz // 4 if nz > 8 else 2, nz - (4 if nz > 8 else 2))))
    far = len(parts) - 1
    order = [o % nz for part_ in parts for o in part_]
    starts = [sum(len(p) for p in parts[:i]) for i in range(len(parts))]
    slots = [len(p) * CAP for p in parts]
    both = [nc * n for n in slots]
    home_rows = sum(both)
    offsets = {2: (0, 1), 4: (0, 1, 3, 2)}[nx]
    units = [
        {2: ((1,), (0,)), 4: ((1, 2, 3), (0,)) if h < far else ((1, 2), (3,), (0,))}[nx]
        for h in range(len(parts))
    ]
    unit_index = {}
    for h in range(len(parts)):
        for u in range(len(units[h])):
            unit_index[h, u] = len(unit_index)
    (zag_s, x_s, y1_s, y2_s, p1_s, p2_s, b_s, home_s, zrs_s, wrs_s, f_s, d_s) = [
        s_sem.at[i] for i in range(12)
    ]
    ep = lax.axis_index("ep")
    y = lax.axis_index("dp")
    c = lax.rem(ep, nc)
    z = lax.rem(lax.div(ep, nc), nz)
    x = lax.div(ep, nc * nz)

    def dev(x_, y_, z_, c_):
        return (((x_ * nz + z_) * nc + c_), y_)

    def to_x(g):
        return lax.rem(x + (nx - offsets[g]), nx)

    def from_x(g):
        return lax.rem(x + offsets[g], nx)

    def at_y(o):
        return lax.rem(y + (o + ny), ny)

    def at_z(o):
        return lax.rem(z + (o + nz), nz)

    def place(o):
        return order.index(o % nz) * tile

    def tokens_of(h):
        return starts[h] * tile, len(parts[h]) * tile

    def rows(start, size):
        if isinstance(start, int):
            return pl.ds(start, size)
        return pl.ds(pl.multiple_of(start, size), size)

    def base(h, g, c_):
        if g == 0:
            return sum(both[:h]) + c_ * slots[h]
        done = sum(both[:h]) * (nx - 1)
        return home_rows + done + (g - 1) * both[h] + c_ * slots[h]

    def span(h, u):
        first = min(units[h][u])
        return base(h, first, 0), len(units[h][u]) * both[h]

    def index(h, u):
        return unit_index[h, u]

    def home(h):
        return len(units[h]) - 1

    def send(src, dst, ssem, rsem, device):
        pltpu.make_async_remote_copy(
            src_ref=src, dst_ref=dst, send_sem=ssem, recv_sem=rsem,
            device_id=device, device_id_type=MESH,
        ).start()

    def awaits(ref, sem):
        return pltpu.make_async_remote_copy(
            src_ref=ref, dst_ref=ref, send_sem=sem, recv_sem=sem,
            device_id=dev(x, y, z, 1 - c), device_id_type=MESH,
        )

    def arrived(ref, sem):
        awaits(ref, sem).wait_recv()

    barrier = pltpu.get_barrier_semaphore()
    peers = [dev(x, y, at_z(o * d), c) for o in range(1, nz // 4 + 1) for d in (1, -1)]
    peers += [dev(from_x(g), y, z, c_) for g in range(1, nx) for c_ in range(nc)]
    peers += [dev(x, y, z, 1 - c)]
    peers += [dev(x, at_y(o), z, c) for o in range(1, ny)]
    for peer in peers:
        pl.semaphore_signal(barrier, inc=1, device_id=peer, device_id_type=MESH)

    own = pl.ds(place(0), tile)
    mine = pltpu.make_async_copy(
        tok_hbm.at[:, pl.ds(pl.multiple_of(y * quarter, 128), quarter)],
        zbuf.at[own, pl.ds(0, quarter)], w_sem.at[3],
    )
    names = [
        pltpu.make_async_copy(ids_hbm, ids_ref, w_sem.at[4]),
        pltpu.make_async_copy(logits_hbm, logits_ref, w_sem.at[5]),
    ]
    for copy in names:
        copy.start()
    mine.start()
    for copy in names:
        copy.wait()
    scores = 1.0 / (1.0 + jnp.exp(-logits_ref[...]))
    wts = ROUTE_SCALE * scores / jnp.sum(scores, axis=0, keepdims=True)
    lane = lax.broadcasted_iota(jnp.int32, (top, 128), 1)
    sub = lax.broadcasted_iota(jnp.int32, (top, 128), 0)
    put_id = (lane == sub).astype(BF16)
    put_w = (lane == sub + top).astype(BF16)
    across = (((0,), (0,)), ((), ()))
    meta = lax.dot_general(
        ids_ref[...].astype(F32).astype(BF16), put_id, across, preferred_element_type=F32
    ) + lax.dot_general(wts.astype(BF16), put_w, across, preferred_element_type=F32)
    zbuf[own, quarter : quarter + 128] = meta.astype(BF16)

    loads = [
        pltpu.make_async_copy(s.at[0], d, w_sem.at[i])
        for i, (s, d) in enumerate(((wg_hbm, wg), (wu_hbm, wu), (wd_hbm, wd)))
    ]
    for load in loads:
        load.start()
    mine.wait()
    pl.semaphore_wait(barrier, len(peers))

    def zslot(d, k):
        return (0 if d > 0 else 1) * steps + (k - 1)

    def ready(k):
        return min(k - 1, far)

    def gather_send(k, d):
        o = -d * 2 * (k - 1)
        for hop in (2, 1):
            if hop == 2 and d < 0 and k == steps:
                continue
            rsem = zag_r.at[zslot(d, k)] if hop == 2 else zag_one.at[ready(k)]
            send(
                zbuf.at[pl.ds(place(o), tile), :], zbuf.at[pl.ds(place(o - d * hop), tile), :],
                zag_s, rsem, dev(x, y, at_z(d * hop), c),
            )

    def gather_step(k):
        for d in (1, -1):
            if d > 0 or k < steps:
                arrived(zbuf.at[pl.ds(0, tile), :], zag_r.at[zslot(d, k)])
            if k < steps:
                gather_send(k + 1, d)

    def gather_rest(h):
        count = sum(ready(k) == h for k in range(1, steps + 1))
        arrived(zbuf.at[pl.ds(0, 2 * count * tile), :], zag_one.at[h])

    def routes(h):
        first, col = tokens_of(h)
        pick = (
            lax.broadcasted_iota(jnp.int32, (2 * top, 128), 0)
            == lax.broadcasted_iota(jnp.int32, (2 * top, 128), 1)
        ).astype(BF16)
        by_token = lax.dot_general(
            pick, zbuf[first : first + col, quarter : quarter + 128],
            (((1,), (1,)), ((), ())), preferred_element_type=F32,
        )
        lanes = nx * nc
        j = lax.broadcasted_iota(jnp.int32, (lanes, col), 0)
        jg, jc = lax.div(j, nc), lax.rem(j, nc)
        off = jnp.zeros_like(jg)
        for g, o in enumerate(offsets):
            off = jnp.where(jg == g, nx - o, off)
        expert = ((lax.rem(x + off, nx) * nz + z) * nc + jc).astype(F32)
        named = jnp.zeros((lanes, col), F32)
        weight = jnp.zeros((lanes, col), F32)
        for k in range(top):
            hit = by_token[k : k + 1, :] == expert
            named = jnp.where(hit, 1.0, named)
            weight = jnp.where(hit, by_token[top + k : top + k + 1, :], weight)
        t_row = lax.broadcasted_iota(jnp.int32, (col, col), 0)
        t_col = lax.broadcasted_iota(jnp.int32, (col, col), 1)
        before = ((t_row < t_col) & (lax.div(t_row, tile) == lax.div(t_col, tile))).astype(BF16)
        rank = jnp.dot(named.astype(BF16), before, preferred_element_type=F32)
        return jnp.where(named > 0.5, rank, -1.0), weight

    def unit_of(h, g):
        return [g in unit for unit in units[h]].index(True)

    def select(h, g, rank, weight):
        first, col = tokens_of(h)
        s_row = lax.broadcasted_iota(jnp.int32, (slots[h], col), 0)
        s_col = lax.broadcasted_iota(jnp.int32, (slots[h], col), 1)
        in_block = lax.div(s_row, CAP) == lax.div(s_col, tile)
        want = jnp.where(in_block, lax.rem(s_row, CAP).astype(F32), -2.0)
        recv = x_r.at[index(h, unit_of(h, g))]
        chosen = []
        for c_ in range(nc):
            i = g * nc + c_
            hit = rank[i : i + 1, :] == want
            chosen.append(jnp.where(hit, 1.0, 0.0).astype(BF16))
            swbuf[pl.ds(base(h, g, c_), slots[h]), 0:col] = jnp.where(
                hit, weight[i : i + 1, :], 0.0
            ).astype(BF16)
        xsend[pl.ds(base(h, g, 0), both[h]), :] = jnp.dot(
            jnp.concatenate(chosen, axis=0), zbuf[first : first + col, 0:quarter],
            preferred_element_type=F32,
        ).astype(BF16)
        land = ybuf.at[y, rows(base(h, g, c), slots[h]), :]
        if g > 0:
            for c_ in range(nc):
                send(
                    xsend.at[pl.ds(base(h, g, c_), slots[h]), :], land, x_s,
                    recv, dev(to_x(g), y, z, c_),
                )
        else:
            other = 1 - c
            send(
                xsend.at[rows(base(h, g, other), slots[h]), :], land, x_s,
                recv, dev(x, y, z, other),
            )
            here = rows(base(h, g, c), slots[h])
            ybuf[y, here, :] = xsend[here, :]

    def x_wait(h, u):
        start, size = span(h, u)
        size = slots[h] if u == home(h) else size
        arrived(ybuf.at[y, pl.ds(start, size), :], x_r.at[index(h, u)])

    def spread(h, u):
        x_wait(h, u)
        start, size = span(h, u)
        block = ybuf.at[y, pl.ds(start, size), :]
        for d in (1, -1):
            send(block, block, y1_s, y1_r.at[index(h, u)], dev(x, at_y(d), z, c))

    def forward(h, u):
        start, size = span(h, u)
        arrived(ybuf.at[pl.ds(0, 2), pl.ds(start, size), :], y1_r.at[index(h, u)])
        for n, d in enumerate((1, -1)):
            block = ybuf.at[at_y(-d), pl.ds(start + n * size // 2, size // 2), :]
            send(block, block, y2_s, y2_r.at[index(h, u)], dev(x, at_y(d), z, c))

    def y_wait(h, u):
        arrived(ybuf.at[0, pl.ds(*span(h, u)), :], y2_r.at[index(h, u)])

    def experts(start, size):
        here = pl.ds(start, size)
        gate = jnp.zeros((size, wg.shape[1]), F32)
        upper = jnp.zeros((size, wg.shape[1]), F32)
        for q in range(ny):
            piece = ybuf[q, here, :]
            deep = pl.ds(q * quarter, quarter)
            gate += jnp.dot(piece, wg[deep, :], preferred_element_type=F32)
            upper += jnp.dot(piece, wu[deep, :], preferred_element_type=F32)
        hidden = (gate / (1.0 + jnp.exp(-gate)) * upper).astype(BF16)
        for q in range(ny):
            obuf[q, here, :] = jnp.dot(
                hidden, wd[:, q * quarter : (q + 1) * quarter], preferred_element_type=F32
            ).astype(BF16)

    def compute(h, u):
        y_wait(h, u)
        experts(*span(h, u))

    def compute_home():
        for h in range(len(parts)):
            y_wait(h, home(h))
        experts(0, home_rows)
        for h in range(len(parts)):
            other = 1 - c
            send(
                obuf.at[:, rows(base(h, 0, other), slots[h]), :],
                rbuf0.at[:, rows(base(h, 0, c), slots[h]), :],
                home_s, b_r.at[index(h, home(h))], dev(x, y, z, other),
            )
            here = rows(base(h, 0, c), slots[h])
            for q in range(ny):
                rbuf0[q, here, :] = obuf[q, here, :]

    def combine_home():
        for h in range(len(parts)):
            arrived(rbuf0.at[:, pl.ds(base(h, 0, 0), slots[h]), :], b_r.at[index(h, home(h))])
            here = pl.ds(base(h, 0, 0), both[h])
            first, col = tokens_of(h)
            for o in range(ny):
                term = lax.dot_general(
                    swbuf[here, 0:col], rbuf0[at_y(o), here, :], across, preferred_element_type=F32
                )
                if o == 0:
                    part[first : first + col, :] = term
                else:
                    part0[first : first + col, (o - 1) * quarter : o * quarter] = term

    def give_one(h, u):
        start, size = span(h, u)
        for n, d in enumerate((1, -1)):
            send(
                obuf.at[at_y(2), pl.ds(start + n * size // 2, size // 2), :],
                r1buf.at[n, pl.ds(start // 2, size // 2), :],
                p1_s, p1_r.at[index(h, u)], dev(x, at_y(d), z, c),
            )

    def give_two(h, u):
        start, size = span(h, u)
        arrived(r1buf.at[:, pl.ds(start // 2, size // 2), :], p1_r.at[index(h, u)])
        for n, d in enumerate((1, -1)):
            here = pl.ds(start + n * size // 2, size // 2)
            q = at_y(d)
            got = r1buf[n, pl.ds(start // 2, size // 2), :]
            obuf[q, here, :] = (obuf[q, here, :].astype(F32) + got.astype(F32)).astype(BF16)
            here = pl.ds(start, size)
            send(
                obuf.at[q, here, :], r2buf.at[n, here, :],
                p2_s, p2_r.at[index(h, u)], dev(x, at_y(d), z, c),
            )

    def give_back(h, u):
        here = pl.ds(*span(h, u))
        arrived(r2buf.at[:, here, :], p2_r.at[index(h, u)])
        total = obuf[y, here, :].astype(F32) + r2buf[0, here, :].astype(F32)
        xret[here, :] = (total + r2buf[1, here, :].astype(F32)).astype(BF16)
        for g in units[h][u]:
            land = rbuf.at[rows(base(h, g, c), slots[h]), :]
            for c_ in range(nc):
                send(
                    xret.at[pl.ds(base(h, g, c_), slots[h]), :], land, b_s,
                    b_r.at[index(h, u)], dev(from_x(g), y, z, c_),
                )

    def combine(h, u):
        here = pl.ds(*span(h, u))
        first, col = tokens_of(h)
        arrived(rbuf.at[here, :], b_r.at[index(h, u)])
        part[first : first + col, :] += lax.dot_general(
            swbuf[here, 0:col], rbuf[here, :], across, preferred_element_type=F32
        )

    reach = nz // 2

    def reducer(source, src, dst, ssem, rsem):
        def block_of(o):
            return source[pl.ds(place(o), tile), :]

        def zsend(d, k, hop, value):
            n = zslot(d, k)
            src[n, hop - 1] = value.astype(BF16)
            send(src.at[n, hop - 1], dst.at[n, hop - 1], ssem, rsem.at[n], dev(x, y, at_z(d * hop), c))

        def zget(d, k):
            n = zslot(d, k)
            if d < 0 and k == 1:
                arrived(dst.at[n, 0], rsem.at[n])
                return dst[n, 0].astype(F32)
            arrived(dst.at[n], rsem.at[n])
            return dst[n, 0].astype(F32) + dst[n, 1].astype(F32)

        def own_hop(k):
            if k == 1:
                zsend(1, 1, 2, block_of(reach))
            for d in (1, -1):
                zsend(d, k, 1, block_of(d * (reach + 1 - 2 * k)))

        def next_hop(k):
            for d in (1, -1):
                zsend(d, k + 1, 2, block_of(d * (reach - 2 * k)) + zget(d, k))

        def finish():
            return block_of(0) + zget(1, steps) + zget(-1, steps)

        return own_hop, next_hop, finish, block_of, zget

    own_hop, next_hop, _, block_of, zget = reducer(part, zs, zr, zrs_s, zrs_r)
    wide_own, wide_next, wide_finish, _, _ = reducer(part0, ws, wr, wrs_s, wrs_r)

    def wide_step(k):
        if k < steps:
            wide_next(k)
            wide_own(k + 1)

    def choose(h):
        rank, weight = routes(h)
        turns = (0, 3, 1, 2) if nx == 4 and h < far else range(nx)
        for g in turns:
            select(h, g, rank, weight)

    direct = nz // 4

    def straight(o):
        value = block_of(o)
        if abs(o) == direct:
            value = value + zget(1 if o > 0 else -1, mid)
        n = (o if o > 0 else direct - o) - 1
        ds[n] = value.astype(BF16)
        send(ds.at[n], dr.at[n], d_s, d_r.at[0], dev(x, y, at_z(o), c))

    def gathered():
        arrived(dr, d_r.at[0])
        total = block_of(0)
        for n in range(2 * direct):
            total += dr[n].astype(F32)
        return total

    near, between = 0, range(1, far)
    outer = range(len(units[far]) - 1)
    for d in (1, -1):
        gather_send(1, d)
    gather_step(1)
    gather_rest(near)
    choose(near)
    spread(near, home(near))
    for h in between:
        gather_step(h + 1)
        gather_rest(h)
        choose(h)
    spread(near, 0)
    for h in between:
        spread(h, home(h))
    forward(near, home(near))
    for k in range(far + 1, steps):
        gather_step(k)
    for h in between:
        spread(h, 0)
    gather_step(steps)
    gather_rest(far)
    choose(far)
    for h in between:
        forward(h, home(h))
    forward(near, 0)
    spread(far, home(far))
    for h in between:
        forward(h, 0)
    forward(far, home(far))
    for u in outer:
        spread(far, u)
    for load in loads:
        load.wait()
    for h in range(far):
        compute(h, 0)
    compute_home()
    forward(far, 0)
    combine_home()
    wide_own(1)
    for u in outer[1:]:
        forward(far, u)
    for h in between:
        give_one(h, 0)
    for u in outer:
        compute(far, u)
        give_one(far, u)
    give_one(near, 0)
    wide_step(1)
    for u in outer:
        give_two(far, u)
    for h in range(far - 1, -1, -1):
        give_two(h, 0)
    wide_step(2)
    for u in outer:
        give_back(far, u)
    for k in range(3, steps):
        wide_step(k)
    for h in between:
        give_back(h, 0)
    for u in outer:
        combine(far, u)
    for k in range(1, mid + 1):
        own_hop(k)
    give_back(near, 0)
    for k in range(1, mid):
        next_hop(k)
    for h in between:
        combine(h, 0)
        for o in (3, -3, 2):
            straight(o)
    wide = wide_finish()
    combine(near, 0)
    for o in range(2 if nz > 8 else 1, 0, -1):
        straight(-o)
    straight(1)
    for o in (direct, -direct):
        straight(o)
    main = gathered()

    count = out_ref.shape[0]
    for o in range(ny):
        share = (main if o == 0 else wide[:, (o - 1) * quarter : o * quarter]).astype(BF16)
        piece = pl.ds(pl.multiple_of(at_y(o) * quarter, 128), quarter)
        for n in range(ny):
            fsend[n, :, piece] = share[n * count : (n + 1) * count, :]
    for o in (2, 1, 3):
        send(fsend.at[at_y(o)], frecv.at[y], f_s, f_r.at[0], dev(x, at_y(o), z, c))
    frecv[y] = fsend[y]
    arrived(frecv.at[pl.ds(0, ny - 1)], f_r.at[0])
    total = frecv[0].astype(F32)
    for q in range(1, ny):
        total += frecv[q].astype(F32)
    out_ref[...] = total.astype(BF16)

    every = ybuf.shape[1]
    moved = every - home_rows
    sent = sum(slots)
    for sem, ref in (
        (zag_s, zbuf.at[pl.ds(0, (nz - 1) * tile), :]),
        (x_s, xsend.at[pl.ds(0, (nx * nc - 1) * sent), :]),
        (y1_s, ybuf.at[pl.ds(0, 2), :, :]),
        (y2_s, ybuf.at[0]),
        (p1_s, ybuf.at[0, pl.ds(0, moved), :]),
        (p2_s, r2buf.at[:, pl.ds(0, moved), :]),
        (b_s, xret.at[pl.ds(0, moved), :]),
        (home_s, rbuf0.at[:, pl.ds(0, sent), :]),
        (zrs_s, ybuf.at[0, pl.ds(0, (4 * mid - 1) * tile), :]),
        (d_s, ds),
        (wrs_s, part0.at[pl.ds(0, (nz - 1) * tile // 2), :]),
        (f_s, fsend.at[pl.ds(0, ny - 1)]),
    ):
        awaits(ref, sem).wait_send()


def on_device(tokens, expert_ids, route_logits, expert_gate, expert_up, expert_down):
    n_ep, ny = lax.axis_size("ep"), N_DP
    nx, nc = CHIPS_X, CORES
    nz = n_ep // (nx * nc)
    tile, width = tokens.shape
    hidden = expert_gate.shape[2]
    quarter = width // ny
    col, slots = nz * tile, nz * CAP
    every = nx * nc * slots
    steps = nz // 4
    dma = pltpu.SemaphoreType.DMA
    vmem = pl.BlockSpec(memory_space=pltpu.VMEM)
    hbm = pl.BlockSpec(memory_space=pl.ANY)
    flops = 6 * every * width * hidden
    units = 7
    home = 2 * nc * slots // 2
    return pl.pallas_call(
        functools.partial(kernel, nx, nz),
        out_shape=jax.ShapeDtypeStruct((tile // ny, width), BF16),
        in_specs=[hbm] * 6,
        out_specs=vmem,
        scratch_shapes=[
            pltpu.VMEM(expert_ids.shape[::-1], jnp.int32),
            pltpu.VMEM(expert_ids.shape[::-1], F32),
            pltpu.VMEM((width, hidden), BF16),
            pltpu.VMEM((width, hidden), BF16),
            pltpu.VMEM((hidden, width), BF16),
            pltpu.VMEM((col, quarter + 128), BF16),
            pltpu.VMEM((every, col // 2), BF16),
            pltpu.VMEM((every, quarter), BF16),
            pltpu.VMEM((ny, every, quarter), BF16),
            pltpu.VMEM((ny, every, quarter), BF16),
            pltpu.VMEM((2, every // 2, quarter), BF16),
            pltpu.VMEM((2, every, quarter), BF16),
            pltpu.VMEM((every, quarter), BF16),
            pltpu.VMEM((every, quarter), BF16),
            pltpu.VMEM((ny, home, quarter), BF16),
            pltpu.VMEM((col, quarter), F32),
            pltpu.VMEM((col, width - quarter), F32),
            pltpu.VMEM((2 * steps, 2, tile, quarter), BF16),
            pltpu.VMEM((2 * steps, 2, tile, quarter), BF16),
            pltpu.VMEM((2 * steps, 2, tile, width - quarter), BF16),
            pltpu.VMEM((2 * steps, 2, tile, width - quarter), BF16),
            pltpu.VMEM((2 * steps, tile, quarter), BF16),
            pltpu.VMEM((2 * steps, tile, quarter), BF16),
            pltpu.VMEM((ny, tile // ny, width), BF16),
            pltpu.VMEM((ny, tile // ny, width), BF16),
            dma((6,)),
            dma((12,)),
            dma((2 * steps,)), dma((3,)),
            dma((units,)), dma((units,)), dma((units,)), dma((units,)), dma((units,)), dma((units,)),
            dma((2 * steps,)), dma((2 * steps,)), dma((1,)), dma((1,)),
        ],
        compiler_params=pltpu.CompilerParams(
            collective_id=0, has_side_effects=True, vmem_limit_bytes=56 * 1024 * 1024
        ),
        cost_estimate=pl.CostEstimate(flops=flops, bytes_accessed=8 << 20, transcendentals=0),
    )(expert_ids.T, route_logits.T, tokens, expert_gate, expert_up, expert_down)


def solution(mesh):
    placed = (
        P("ep", None),
        P("ep", None),
        P("ep", None),
        P("ep", None, "dp"),
        P("ep", None, "dp"),
        P("ep", "dp", None),
    )
    return jax.shard_map(
        on_device, mesh=mesh, in_specs=placed, out_specs=P(("ep", "dp"), None), check_vma=False
    )
```

```python
import functools

import jax
import jax.numpy as jnp
from jax import lax
from jax.experimental import pallas as pl
from jax.experimental.pallas import tpu as pltpu
from jax.sharding import PartitionSpec as P

MESH = pl.DeviceIdType.MESH
F32 = jnp.float32
BF16 = jnp.bfloat16
ROUTE_SCALE = 2.5
CAP = 4
CHIPS_X = 4
CORES = 2
N_DP = 4


def kernel(
    nx, nz, ids_hbm, logits_hbm, tok_hbm, wg_hbm, wu_hbm, wd_hbm, out_ref,
    ids_ref, logits_ref, wg, wu, wd, zbuf, swbuf, xsend, ybuf, obuf, r1buf, r2buf, xret, rbuf, rbuf0, part, part0,
    zs, zr, ws, wr, ds, dr, fsend, frecv,
    w_sem, s_sem, zag_r, zag_one, x_r, y1_r, y2_r, p1_r, p2_r, b_r, zrs_r, wrs_r, f_r, d_r,
):
    nc, ny = CORES, N_DP
    tile, width = tok_hbm.shape
    quarter = width // ny
    top = ids_ref.shape[0]
    steps = nz // 4
    mid = steps // 2
    parts = [(-2, -1, 0, 1)]
    if nz > 8:
        parts.append((2, 3, -4, -3))
    parts.append(tuple(range(nz // 4 if nz > 8 else 2, nz - (4 if nz > 8 else 2))))
    far = len(parts) - 1
    order = [o % nz for part_ in parts for o in part_]
    starts = [sum(len(p) for p in parts[:i]) for i in range(len(parts))]
    slots = [len(p) * CAP for p in parts]
    both = [nc * n for n in slots]
    home_rows = sum(both)
    offsets = {2: (0, 1), 4: (0, 1, 3, 2)}[nx]
    units = [
        {2: ((1,), (0,)), 4: ((1, 2, 3), (0,)) if h < far else ((1, 2), (3,), (0,))}[nx]
        for h in range(len(parts))
    ]
    unit_index = {}
    for h in range(len(parts)):
        for u in range(len(units[h])):
            unit_index[h, u] = len(unit_index)
    (zag_s, x_s, y1_s, y2_s, p1_s, p2_s, b_s, home_s, zrs_s, wrs_s, f_s, d_s, o_s) = [
        s_sem.at[i] for i in range(13)
    ]
    ep = lax.axis_index("ep")
    y = lax.axis_index("dp")
    c = lax.rem(ep, nc)
    z = lax.rem(lax.div(ep, nc), nz)
    x = lax.div(ep, nc * nz)

    def dev(x_, y_, z_, c_):
        return (((x_ * nz + z_) * nc + c_), y_)

    def to_x(g):
        return lax.rem(x + (nx - offsets[g]), nx)

    def from_x(g):
        return lax.rem(x + offsets[g], nx)

    def at_y(o):
        return lax.rem(y + (o + ny), ny)

    def at_z(o):
        return lax.rem(z + (o + nz), nz)

    def place(o):
        return order.index(o % nz) * tile

    def tokens_of(h):
        return starts[h] * tile, len(parts[h]) * tile

    def rows(start, size):
        if isinstance(start, int):
            return pl.ds(start, size)
        return pl.ds(pl.multiple_of(start, size), size)

    def base(h, g, c_):
        if g == 0:
            return sum(both[:h]) + c_ * slots[h]
        done = sum(both[:h]) * (nx - 1)
        return home_rows + done + (g - 1) * both[h] + c_ * slots[h]

    def span(h, u):
        first = min(units[h][u])
        return base(h, first, 0), len(units[h][u]) * both[h]

    def index(h, u):
        return unit_index[h, u]

    def home(h):
        return len(units[h]) - 1

    def send(src, dst, ssem, rsem, device):
        pltpu.make_async_remote_copy(
            src_ref=src, dst_ref=dst, send_sem=ssem, recv_sem=rsem,
            device_id=device, device_id_type=MESH,
        ).start()

    def awaits(ref, sem):
        return pltpu.make_async_remote_copy(
            src_ref=ref, dst_ref=ref, send_sem=sem, recv_sem=sem,
            device_id=dev(x, y, z, 1 - c), device_id_type=MESH,
        )

    def arrived(ref, sem):
        awaits(ref, sem).wait_recv()

    barrier = pltpu.get_barrier_semaphore()
    peers = [dev(x, y, at_z(o), c) for o in (1, -1, 2, -2)]
    peers += [dev(from_x(g), y, z, c_) for g in range(1, nx) for c_ in range(nc)]
    peers += [dev(x, y, z, 1 - c)]
    peers += [dev(x, at_y(o), z, c) for o in range(1, ny)]
    for peer in peers:
        pl.semaphore_signal(barrier, inc=1, device_id=peer, device_id_type=MESH)

    own = pl.ds(place(0), tile)
    mine = pltpu.make_async_copy(
        tok_hbm.at[:, pl.ds(pl.multiple_of(y * quarter, 128), quarter)],
        zbuf.at[own, pl.ds(0, quarter)], w_sem.at[3],
    )
    names = [
        pltpu.make_async_copy(ids_hbm, ids_ref, w_sem.at[4]),
        pltpu.make_async_copy(logits_hbm, logits_ref, w_sem.at[5]),
    ]
    for copy in names:
        copy.start()
    mine.start()
    for copy in names:
        copy.wait()
    scores = 1.0 / (1.0 + jnp.exp(-logits_ref[...]))
    wts = ROUTE_SCALE * scores / jnp.sum(scores, axis=0, keepdims=True)
    lane = lax.broadcasted_iota(jnp.int32, (top, 128), 1)
    sub = lax.broadcasted_iota(jnp.int32, (top, 128), 0)
    put_id = (lane == sub).astype(BF16)
    put_w = (lane == sub + top).astype(BF16)
    across = (((0,), (0,)), ((), ()))
    meta = lax.dot_general(
        ids_ref[...].astype(F32).astype(BF16), put_id, across, preferred_element_type=F32
    ) + lax.dot_general(wts.astype(BF16), put_w, across, preferred_element_type=F32)
    zbuf[own, quarter : quarter + 128] = meta.astype(BF16)

    loads = [
        pltpu.make_async_copy(s.at[0], d, w_sem.at[i])
        for i, (s, d) in enumerate(((wg_hbm, wg), (wu_hbm, wu), (wd_hbm, wd)))
    ]
    for load in loads:
        load.start()
    mine.wait()
    pl.semaphore_wait(barrier, len(peers))

    def zslot(d, k):
        return (0 if d > 0 else 1) * steps + (k - 1)

    def ready(k):
        return min(k - 1, far)

    def gather_send(k, d):
        o = -d * 2 * (k - 1)
        for hop in (2, 1):
            if hop == 2 and d < 0 and k == steps:
                continue
            rsem = zag_r.at[zslot(d, k)] if hop == 2 else zag_one.at[ready(k)]
            send(
                zbuf.at[pl.ds(place(o), tile), :], zbuf.at[pl.ds(place(o - d * hop), tile), :],
                zag_s, rsem, dev(x, y, at_z(d * hop), c),
            )

    def gather_step(k):
        for d in (1, -1):
            if d > 0 or k < steps:
                arrived(zbuf.at[pl.ds(0, tile), :], zag_r.at[zslot(d, k)])
            if k < steps:
                gather_send(k + 1, d)

    def gather_rest(h):
        count = sum(ready(k) == h for k in range(1, steps + 1))
        arrived(zbuf.at[pl.ds(0, 2 * count * tile), :], zag_one.at[h])

    def routes(h):
        first, col = tokens_of(h)
        pick = (
            lax.broadcasted_iota(jnp.int32, (2 * top, 128), 0)
            == lax.broadcasted_iota(jnp.int32, (2 * top, 128), 1)
        ).astype(BF16)
        by_token = lax.dot_general(
            pick, zbuf[first : first + col, quarter : quarter + 128],
            (((1,), (1,)), ((), ())), preferred_element_type=F32,
        )
        lanes = nx * nc
        j = lax.broadcasted_iota(jnp.int32, (lanes, col), 0)
        jg, jc = lax.div(j, nc), lax.rem(j, nc)
        off = jnp.zeros_like(jg)
        for g, o in enumerate(offsets):
            off = jnp.where(jg == g, nx - o, off)
        expert = ((lax.rem(x + off, nx) * nz + z) * nc + jc).astype(F32)
        named = jnp.zeros((lanes, col), F32)
        weight = jnp.zeros((lanes, col), F32)
        for k in range(top):
            hit = by_token[k : k + 1, :] == expert
            named = jnp.where(hit, 1.0, named)
            weight = jnp.where(hit, by_token[top + k : top + k + 1, :], weight)
        t_row = lax.broadcasted_iota(jnp.int32, (col, col), 0)
        t_col = lax.broadcasted_iota(jnp.int32, (col, col), 1)
        before = ((t_row < t_col) & (lax.div(t_row, tile) == lax.div(t_col, tile))).astype(BF16)
        rank = jnp.dot(named.astype(BF16), before, preferred_element_type=F32)
        return jnp.where(named > 0.5, rank, -1.0), weight

    def unit_of(h, g):
        return [g in unit for unit in units[h]].index(True)

    def select(h, g, rank, weight):
        first, col = tokens_of(h)
        s_row = lax.broadcasted_iota(jnp.int32, (slots[h], col), 0)
        s_col = lax.broadcasted_iota(jnp.int32, (slots[h], col), 1)
        in_block = lax.div(s_row, CAP) == lax.div(s_col, tile)
        want = jnp.where(in_block, lax.rem(s_row, CAP).astype(F32), -2.0)
        recv = x_r.at[index(h, unit_of(h, g))]
        chosen = []
        for c_ in range(nc):
            i = g * nc + c_
            hit = rank[i : i + 1, :] == want
            chosen.append(jnp.where(hit, 1.0, 0.0).astype(BF16))
            swbuf[pl.ds(base(h, g, c_), slots[h]), 0:col] = jnp.where(
                hit, weight[i : i + 1, :], 0.0
            ).astype(BF16)
        xsend[pl.ds(base(h, g, 0), both[h]), :] = jnp.dot(
            jnp.concatenate(chosen, axis=0), zbuf[first : first + col, 0:quarter],
            preferred_element_type=F32,
        ).astype(BF16)
        land = ybuf.at[y, rows(base(h, g, c), slots[h]), :]
        if g > 0:
            for c_ in range(nc):
                send(
                    xsend.at[pl.ds(base(h, g, c_), slots[h]), :], land, x_s,
                    recv, dev(to_x(g), y, z, c_),
                )
        else:
            other = 1 - c
            send(
                xsend.at[rows(base(h, g, other), slots[h]), :], land, x_s,
                recv, dev(x, y, z, other),
            )
            here = rows(base(h, g, c), slots[h])
            ybuf[y, here, :] = xsend[here, :]

    def x_wait(h, u):
        start, size = span(h, u)
        size = slots[h] if u == home(h) else size
        arrived(ybuf.at[y, pl.ds(start, size), :], x_r.at[index(h, u)])

    def spread(h, u):
        x_wait(h, u)
        start, size = span(h, u)
        block = ybuf.at[y, pl.ds(start, size), :]
        for d in (1, -1):
            send(block, block, y1_s, y1_r.at[index(h, u)], dev(x, at_y(d), z, c))

    def forward(h, u):
        start, size = span(h, u)
        arrived(ybuf.at[pl.ds(0, 2), pl.ds(start, size), :], y1_r.at[index(h, u)])
        for n, d in enumerate((1, -1)):
            block = ybuf.at[at_y(-d), pl.ds(start + n * size // 2, size // 2), :]
            send(block, block, y2_s, y2_r.at[index(h, u)], dev(x, at_y(d), z, c))

    def y_wait(h, u):
        arrived(ybuf.at[0, pl.ds(*span(h, u)), :], y2_r.at[index(h, u)])

    def experts(start, size):
        here = pl.ds(start, size)
        gate = jnp.zeros((size, wg.shape[1]), F32)
        upper = jnp.zeros((size, wg.shape[1]), F32)
        for q in range(ny):
            piece = ybuf[q, here, :]
            deep = pl.ds(q * quarter, quarter)
            gate += jnp.dot(piece, wg[deep, :], preferred_element_type=F32)
            upper += jnp.dot(piece, wu[deep, :], preferred_element_type=F32)
        hidden = (gate / (1.0 + jnp.exp(-gate)) * upper).astype(BF16)
        for q in range(ny):
            obuf[q, here, :] = jnp.dot(
                hidden, wd[:, q * quarter : (q + 1) * quarter], preferred_element_type=F32
            ).astype(BF16)

    def compute(h, u):
        y_wait(h, u)
        experts(*span(h, u))

    def compute_home():
        for h in range(len(parts)):
            y_wait(h, home(h))
        experts(0, home_rows)
        for h in range(len(parts)):
            other = 1 - c
            send(
                obuf.at[:, rows(base(h, 0, other), slots[h]), :],
                rbuf0.at[:, rows(base(h, 0, c), slots[h]), :],
                home_s, b_r.at[index(h, home(h))], dev(x, y, z, other),
            )
            here = rows(base(h, 0, c), slots[h])
            for q in range(ny):
                rbuf0[q, here, :] = obuf[q, here, :]

    def combine_home():
        for h in range(len(parts)):
            arrived(rbuf0.at[:, pl.ds(base(h, 0, 0), slots[h]), :], b_r.at[index(h, home(h))])
            here = pl.ds(base(h, 0, 0), both[h])
            first, col = tokens_of(h)
            for o in range(ny):
                term = lax.dot_general(
                    swbuf[here, 0:col], rbuf0[at_y(o), here, :], across, preferred_element_type=F32
                )
                if o == 0:
                    part[first : first + col, :] = term
                else:
                    part0[first : first + col, (o - 1) * quarter : o * quarter] = term

    def give_one(h, u):
        start, size = span(h, u)
        for n, d in enumerate((1, -1)):
            send(
                obuf.at[at_y(2), pl.ds(start + n * size // 2, size // 2), :],
                r1buf.at[n, pl.ds(start // 2, size // 2), :],
                p1_s, p1_r.at[index(h, u)], dev(x, at_y(d), z, c),
            )

    def give_two(h, u):
        start, size = span(h, u)
        arrived(r1buf.at[:, pl.ds(start // 2, size // 2), :], p1_r.at[index(h, u)])
        for n, d in enumerate((1, -1)):
            here = pl.ds(start + n * size // 2, size // 2)
            q = at_y(d)
            got = r1buf[n, pl.ds(start // 2, size // 2), :]
            obuf[q, here, :] = (obuf[q, here, :].astype(F32) + got.astype(F32)).astype(BF16)
            here = pl.ds(start, size)
            send(
                obuf.at[q, here, :], r2buf.at[n, here, :],
                p2_s, p2_r.at[index(h, u)], dev(x, at_y(d), z, c),
            )

    def give_back(h, u):
        here = pl.ds(*span(h, u))
        arrived(r2buf.at[:, here, :], p2_r.at[index(h, u)])
        total = obuf[y, here, :].astype(F32) + r2buf[0, here, :].astype(F32)
        xret[here, :] = (total + r2buf[1, here, :].astype(F32)).astype(BF16)
        for g in units[h][u]:
            land = rbuf.at[rows(base(h, g, c), slots[h]), :]
            for c_ in range(nc):
                send(
                    xret.at[pl.ds(base(h, g, c_), slots[h]), :], land, b_s,
                    b_r.at[index(h, u)], dev(from_x(g), y, z, c_),
                )

    def combine(h, u):
        here = pl.ds(*span(h, u))
        first, col = tokens_of(h)
        arrived(rbuf.at[here, :], b_r.at[index(h, u)])
        part[first : first + col, :] += lax.dot_general(
            swbuf[here, 0:col], rbuf[here, :], across, preferred_element_type=F32
        )

    reach = nz // 2

    def reducer(source, src, dst, ssem, rsem):
        def block_of(o):
            return source[pl.ds(place(o), tile), :]

        def zsend(d, k, hop, value):
            n = zslot(d, k)
            src[n, hop - 1] = value.astype(BF16)
            send(src.at[n, hop - 1], dst.at[n, hop - 1], ssem, rsem.at[n], dev(x, y, at_z(d * hop), c))

        def zget(d, k):
            n = zslot(d, k)
            if d < 0 and k == 1:
                arrived(dst.at[n, 0], rsem.at[n])
                return dst[n, 0].astype(F32)
            arrived(dst.at[n], rsem.at[n])
            return dst[n, 0].astype(F32) + dst[n, 1].astype(F32)

        def own_hop(k):
            if k == 1:
                zsend(1, 1, 2, block_of(reach))
            for d in (1, -1):
                zsend(d, k, 1, block_of(d * (reach + 1 - 2 * k)))

        def next_hop(k):
            for d in (1, -1):
                zsend(d, k + 1, 2, block_of(d * (reach - 2 * k)) + zget(d, k))

        def finish():
            return block_of(0) + zget(1, steps) + zget(-1, steps)

        return own_hop, next_hop, finish, block_of, zget

    own_hop, next_hop, _, block_of, zget = reducer(part, zs, zr, zrs_s, zrs_r)
    wide_own, wide_next, wide_finish, _, _ = reducer(part0, ws, wr, wrs_s, wrs_r)

    def wide_step(k):
        if k < steps:
            wide_next(k)
            wide_own(k + 1)

    def choose(h):
        rank, weight = routes(h)
        turns = (0, 3, 1, 2) if nx == 4 and h < far else range(nx)
        for g in turns:
            select(h, g, rank, weight)

    direct = nz // 4

    count = out_ref.shape[0]

    def straight(o):
        value = block_of(o)
        if abs(o) == direct:
            value = value + zget(1 if o > 0 else -1, mid)
        n = (o if o > 0 else direct - o) - 1 if o else 2 * direct
        for q in range(ny):
            ds[n, q] = value[q * count : (q + 1) * count, :].astype(BF16)
        for r in range(ny) if o else range(1, ny):
            send(
                ds.at[n, at_y(r)], dr.at[y, n], d_s if o else o_s, d_r.at[0 if o else 1],
                dev(x, at_y(r), at_z(o), c),
            )
        if o == 0:
            dr[y, n] = ds[n, y]

    def share_wide():
        wide = wide_finish()
        for q in range(ny):
            fsend[q] = wide[q * count : (q + 1) * count, :].astype(BF16)
        for r in (2, 1, 3):
            send(fsend.at[at_y(r)], frecv.at[y], f_s, f_r.at[0], dev(x, at_y(r), z, c))
        frecv[y] = fsend[y]

    def gathered(j):
        where = at_y(j)
        total = dr[where, 2 * direct].astype(F32)
        for r in range(ny):
            o = (j - r) % ny
            if o:
                total += frecv[at_y(r), :, (o - 1) * quarter : o * quarter].astype(F32)
        for n in range(2 * direct):
            total += dr[where, n].astype(F32)
        return total.astype(BF16)

    near, between = 0, range(1, far)
    outer = range(len(units[far]) - 1)
    for d in (1, -1):
        gather_send(1, d)
    gather_step(1)
    gather_rest(near)
    choose(near)
    spread(near, home(near))
    for h in between:
        gather_step(h + 1)
    spread(near, 0)
    for h in between:
        gather_rest(h)
        choose(h)
        spread(h, home(h))
    forward(near, home(near))
    for k in range(far + 1, steps):
        gather_step(k)
    for h in between:
        spread(h, 0)
    gather_step(steps)
    gather_rest(far)
    choose(far)
    forward(near, 0)
    spread(far, home(far))
    for h in between:
        forward(h, home(h))
        forward(h, 0)
    forward(far, home(far))
    for u in outer:
        spread(far, u)
    for load in loads:
        load.wait()
    for h in range(far):
        compute(h, 0)
    compute_home()
    forward(far, 0)
    combine_home()
    wide_own(1)
    for u in outer[1:]:
        forward(far, u)
    for h in between:
        give_one(h, 0)
    for u in outer:
        compute(far, u)
        give_one(far, u)
    give_one(near, 0)
    wide_step(1)
    for u in outer:
        give_two(far, u)
    for h in range(far - 1, -1, -1):
        give_two(h, 0)
    wide_step(2)
    for u in outer:
        give_back(far, u)
    for k in range(3, steps):
        wide_step(k)
    for h in between:
        give_back(h, 0)
    for u in outer:
        combine(far, u)
    for k in range(1, mid + 1):
        own_hop(k)
    give_back(near, 0)
    for k in range(1, mid):
        next_hop(k)
    for h in between:
        combine(h, 0)
        for o in (3, -3, 2):
            straight(o)
    share_wide()
    combine(near, 0)
    for o in range(2 if nz > 8 else 1, 0, -1):
        straight(-o)
    straight(1)
    straight(0)
    for o in (direct, -direct):
        straight(o)
    arrived(frecv.at[pl.ds(0, ny - 1)], f_r.at[0])
    arrived(dr.at[pl.ds(0, ny - 1), 2 * direct], d_r.at[1])
    arrived(dr.at[:, pl.ds(0, 2 * direct)], d_r.at[0])
    for j in range(ny):
        piece = pl.ds(pl.multiple_of(at_y(j) * quarter, 128), quarter)
        out_ref[:, piece] = gathered(j)

    every = ybuf.shape[1]
    moved = every - home_rows
    sent = sum(slots)
    for sem, ref in (
        (zag_s, zbuf.at[pl.ds(0, (nz - 1) * tile), :]),
        (x_s, xsend.at[pl.ds(0, (nx * nc - 1) * sent), :]),
        (y1_s, ybuf.at[pl.ds(0, 2), :, :]),
        (y2_s, ybuf.at[0]),
        (p1_s, ybuf.at[0, pl.ds(0, moved), :]),
        (p2_s, r2buf.at[:, pl.ds(0, moved), :]),
        (b_s, xret.at[pl.ds(0, moved), :]),
        (home_s, rbuf0.at[:, pl.ds(0, sent), :]),
        (zrs_s, ybuf.at[0, pl.ds(0, (4 * mid - 1) * tile), :]),
        (d_s, ds.at[pl.ds(0, 2 * direct)]),
        (o_s, ds.at[0, pl.ds(0, ny - 1)]),
        (wrs_s, part0.at[pl.ds(0, (nz - 1) * tile // 2), :]),
        (f_s, fsend.at[pl.ds(0, ny - 1)]),
    ):
        awaits(ref, sem).wait_send()


def on_device(tokens, expert_ids, route_logits, expert_gate, expert_up, expert_down):
    n_ep, ny = lax.axis_size("ep"), N_DP
    nx, nc = CHIPS_X, CORES
    nz = n_ep // (nx * nc)
    tile, width = tokens.shape
    hidden = expert_gate.shape[2]
    quarter = width // ny
    col, slots = nz * tile, nz * CAP
    every = nx * nc * slots
    steps = nz // 4
    dma = pltpu.SemaphoreType.DMA
    vmem = pl.BlockSpec(memory_space=pltpu.VMEM)
    hbm = pl.BlockSpec(memory_space=pl.ANY)
    flops = 6 * every * width * hidden
    units = 7
    home = 2 * nc * slots // 2
    return pl.pallas_call(
        functools.partial(kernel, nx, nz),
        out_shape=jax.ShapeDtypeStruct((tile // ny, width), BF16),
        in_specs=[hbm] * 6,
        out_specs=vmem,
        scratch_shapes=[
            pltpu.VMEM(expert_ids.shape[::-1], jnp.int32),
            pltpu.VMEM(expert_ids.shape[::-1], F32),
            pltpu.VMEM((width, hidden), BF16),
            pltpu.VMEM((width, hidden), BF16),
            pltpu.VMEM((hidden, width), BF16),
            pltpu.VMEM((col, quarter + 128), BF16),
            pltpu.VMEM((every, col // 2), BF16),
            pltpu.VMEM((every, quarter), BF16),
            pltpu.VMEM((ny, every, quarter), BF16),
            pltpu.VMEM((ny, every, quarter), BF16),
            pltpu.VMEM((2, every // 2, quarter), BF16),
            pltpu.VMEM((2, every, quarter), BF16),
            pltpu.VMEM((every, quarter), BF16),
            pltpu.VMEM((every, quarter), BF16),
            pltpu.VMEM((ny, home, quarter), BF16),
            pltpu.VMEM((col, quarter), F32),
            pltpu.VMEM((col, width - quarter), F32),
            pltpu.VMEM((2 * steps, 2, tile, quarter), BF16),
            pltpu.VMEM((2 * steps, 2, tile, quarter), BF16),
            pltpu.VMEM((2 * steps, 2, tile, width - quarter), BF16),
            pltpu.VMEM((2 * steps, 2, tile, width - quarter), BF16),
            pltpu.VMEM((2 * steps + 1, ny, tile // ny, quarter), BF16),
            pltpu.VMEM((ny, 2 * steps + 1, tile // ny, quarter), BF16),
            pltpu.VMEM((ny, tile // ny, width - quarter), BF16),
            pltpu.VMEM((ny, tile // ny, width - quarter), BF16),
            dma((6,)),
            dma((13,)),
            dma((2 * steps,)), dma((3,)),
            dma((units,)), dma((units,)), dma((units,)), dma((units,)), dma((units,)), dma((units,)),
            dma((2 * steps,)), dma((2 * steps,)), dma((1,)), dma((2,)),
        ],
        compiler_params=pltpu.CompilerParams(
            collective_id=0, has_side_effects=True, vmem_limit_bytes=56 * 1024 * 1024
        ),
        cost_estimate=pl.CostEstimate(flops=flops, bytes_accessed=8 << 20, transcendentals=0),
    )(expert_ids.T, route_logits.T, tokens, expert_gate, expert_up, expert_down)


def solution(mesh):
    placed = (
        P("ep", None),
        P("ep", None),
        P("ep", None),
        P("ep", None, "dp"),
        P("ep", None, "dp"),
        P("ep", "dp", None),
    )
    return jax.shard_map(
        on_device, mesh=mesh, in_specs=placed, out_specs=P(("ep", "dp"), None), check_vma=False
    )
```

```python
import functools

import jax
import jax.numpy as jnp
from jax import lax
from jax.experimental import pallas as pl
from jax.experimental.pallas import tpu as pltpu
from jax.sharding import PartitionSpec as P

MESH = pl.DeviceIdType.MESH
F32 = jnp.float32
BF16 = jnp.bfloat16
ROUTE_SCALE = 2.5
CAP = 4
CHIPS_X = 4
CORES = 2
N_DP = 4


def kernel(
    nx, nz, ids_hbm, logits_hbm, tok_hbm, wg_hbm, wu_hbm, wd_hbm, out_ref,
    ids_ref, logits_ref, wg, wu, wd, zbuf, swbuf, xsend, ybuf, obuf, r1buf, r2buf, xret, rbuf, rbuf0, part, part0,
    zs, zr, ws, wr, ds, dr, fsend, frecv,
    w_sem, s_sem, zag_r, zag_one, x_r, y1_r, y2_r, p1_r, p2_r, b_r, zrs_r, wrs_r, f_r, d_r,
):
    nc, ny = CORES, N_DP
    tile, width = tok_hbm.shape
    quarter = width // ny
    top = ids_ref.shape[0]
    steps = nz // 4
    mid = steps // 2
    parts = [(-2, -1, 0, 1)]
    if nz > 8:
        parts.append((2, 3, -4, -3))
    parts.append(tuple(range(nz // 4 if nz > 8 else 2, nz - (4 if nz > 8 else 2))))
    far = len(parts) - 1
    order = [o % nz for part_ in parts for o in part_]
    starts = [sum(len(p) for p in parts[:i]) for i in range(len(parts))]
    slots = [len(p) * CAP for p in parts]
    both = [nc * n for n in slots]
    home_rows = sum(both)
    offsets = {2: (0, 1), 4: (0, 1, 3, 2)}[nx]
    units = [
        {2: ((1,), (0,)), 4: ((1, 2, 3), (0,)) if h < far else ((3,), (1, 2), (0,))}[nx]
        for h in range(len(parts))
    ]
    unit_index = {}
    for h in range(len(parts)):
        for u in range(len(units[h])):
            unit_index[h, u] = len(unit_index)
    (zag_s, x_s, y1_s, y2_s, p1_s, p2_s, b_s, home_s, zrs_s, wrs_s, f_s, d_s, o_s) = [
        s_sem.at[i] for i in range(13)
    ]
    ep = lax.axis_index("ep")
    y = lax.axis_index("dp")
    c = lax.rem(ep, nc)
    z = lax.rem(lax.div(ep, nc), nz)
    x = lax.div(ep, nc * nz)

    def dev(x_, y_, z_, c_):
        return (((x_ * nz + z_) * nc + c_), y_)

    def to_x(g):
        return lax.rem(x + (nx - offsets[g]), nx)

    def from_x(g):
        return lax.rem(x + offsets[g], nx)

    def at_y(o):
        return lax.rem(y + (o + ny), ny)

    def at_z(o):
        return lax.rem(z + (o + nz), nz)

    def place(o):
        return order.index(o % nz) * tile

    def tokens_of(h):
        return starts[h] * tile, len(parts[h]) * tile

    def rows(start, size):
        if isinstance(start, int):
            return pl.ds(start, size)
        return pl.ds(pl.multiple_of(start, size), size)

    def base(h, g, c_):
        if g == 0:
            return sum(both[:h]) + c_ * slots[h]
        done = sum(both[:h]) * (nx - 1)
        return home_rows + done + (g - 1) * both[h] + c_ * slots[h]

    def span(h, u):
        first = min(units[h][u])
        return base(h, first, 0), len(units[h][u]) * both[h]

    def index(h, u):
        return unit_index[h, u]

    def home(h):
        return len(units[h]) - 1

    def send(src, dst, ssem, rsem, device):
        pltpu.make_async_remote_copy(
            src_ref=src, dst_ref=dst, send_sem=ssem, recv_sem=rsem,
            device_id=device, device_id_type=MESH,
        ).start()

    def awaits(ref, sem):
        return pltpu.make_async_remote_copy(
            src_ref=ref, dst_ref=ref, send_sem=sem, recv_sem=sem,
            device_id=dev(x, y, z, 1 - c), device_id_type=MESH,
        )

    def arrived(ref, sem):
        awaits(ref, sem).wait_recv()

    barrier = pltpu.get_barrier_semaphore()
    peers = [dev(x, y, at_z(o), c) for o in (1, -1, 2, -2)]
    peers += [dev(from_x(g), y, z, c_) for g in range(1, nx) for c_ in range(nc)]
    peers += [dev(x, y, z, 1 - c)]
    peers += [dev(x, at_y(o), z, c) for o in range(1, ny)]
    for peer in peers:
        pl.semaphore_signal(barrier, inc=1, device_id=peer, device_id_type=MESH)

    own = pl.ds(place(0), tile)
    mine = pltpu.make_async_copy(
        tok_hbm.at[:, pl.ds(pl.multiple_of(y * quarter, 128), quarter)],
        zbuf.at[own, pl.ds(0, quarter)], w_sem.at[3],
    )
    names = [
        pltpu.make_async_copy(ids_hbm, ids_ref, w_sem.at[4]),
        pltpu.make_async_copy(logits_hbm, logits_ref, w_sem.at[5]),
    ]
    for copy in names:
        copy.start()
    mine.start()
    for copy in names:
        copy.wait()
    scores = 1.0 / (1.0 + jnp.exp(-logits_ref[...]))
    wts = ROUTE_SCALE * scores / jnp.sum(scores, axis=0, keepdims=True)
    lane = lax.broadcasted_iota(jnp.int32, (top, 128), 1)
    sub = lax.broadcasted_iota(jnp.int32, (top, 128), 0)
    put_id = (lane == sub).astype(BF16)
    put_w = (lane == sub + top).astype(BF16)
    across = (((0,), (0,)), ((), ()))
    meta = lax.dot_general(
        ids_ref[...].astype(F32).astype(BF16), put_id, across, preferred_element_type=F32
    ) + lax.dot_general(wts.astype(BF16), put_w, across, preferred_element_type=F32)
    zbuf[own, quarter : quarter + 128] = meta.astype(BF16)

    loads = [
        pltpu.make_async_copy(s.at[0], d, w_sem.at[i])
        for i, (s, d) in enumerate(((wg_hbm, wg), (wu_hbm, wu), (wd_hbm, wd)))
    ]
    for load in loads:
        load.start()
    mine.wait()
    pl.semaphore_wait(barrier, len(peers))

    def zslot(d, k):
        return (0 if d > 0 else 1) * steps + (k - 1)

    def ready(k):
        return min(k - 1, far)

    def gather_send(k, d):
        o = -d * 2 * (k - 1)
        for hop in (2, 1):
            if hop == 2 and d < 0 and k == steps:
                continue
            rsem = zag_r.at[zslot(d, k)] if hop == 2 else zag_one.at[ready(k)]
            send(
                zbuf.at[pl.ds(place(o), tile), :], zbuf.at[pl.ds(place(o - d * hop), tile), :],
                zag_s, rsem, dev(x, y, at_z(d * hop), c),
            )

    def gather_step(k):
        for d in (1, -1):
            if d > 0 or k < steps:
                arrived(zbuf.at[pl.ds(0, tile), :], zag_r.at[zslot(d, k)])
            if k < steps:
                gather_send(k + 1, d)

    def gather_rest(h):
        count = sum(ready(k) == h for k in range(1, steps + 1))
        arrived(zbuf.at[pl.ds(0, 2 * count * tile), :], zag_one.at[h])

    def routes(h):
        first, col = tokens_of(h)
        pick = (
            lax.broadcasted_iota(jnp.int32, (2 * top, 128), 0)
            == lax.broadcasted_iota(jnp.int32, (2 * top, 128), 1)
        ).astype(BF16)
        by_token = lax.dot_general(
            pick, zbuf[first : first + col, quarter : quarter + 128],
            (((1,), (1,)), ((), ())), preferred_element_type=F32,
        )
        lanes = nx * nc
        j = lax.broadcasted_iota(jnp.int32, (lanes, col), 0)
        jg, jc = lax.div(j, nc), lax.rem(j, nc)
        off = jnp.zeros_like(jg)
        for g, o in enumerate(offsets):
            off = jnp.where(jg == g, nx - o, off)
        expert = ((lax.rem(x + off, nx) * nz + z) * nc + jc).astype(F32)
        named = jnp.zeros((lanes, col), F32)
        weight = jnp.zeros((lanes, col), F32)
        for k in range(top):
            hit = by_token[k : k + 1, :] == expert
            named = jnp.where(hit, 1.0, named)
            weight = jnp.where(hit, by_token[top + k : top + k + 1, :], weight)
        t_row = lax.broadcasted_iota(jnp.int32, (col, col), 0)
        t_col = lax.broadcasted_iota(jnp.int32, (col, col), 1)
        before = ((t_row < t_col) & (lax.div(t_row, tile) == lax.div(t_col, tile))).astype(BF16)
        rank = jnp.dot(named.astype(BF16), before, preferred_element_type=F32)
        return jnp.where(named > 0.5, rank, -1.0), weight

    def unit_of(h, g):
        return [g in unit for unit in units[h]].index(True)

    def select(h, g, rank, weight):
        first, col = tokens_of(h)
        s_row = lax.broadcasted_iota(jnp.int32, (slots[h], col), 0)
        s_col = lax.broadcasted_iota(jnp.int32, (slots[h], col), 1)
        in_block = lax.div(s_row, CAP) == lax.div(s_col, tile)
        want = jnp.where(in_block, lax.rem(s_row, CAP).astype(F32), -2.0)
        recv = x_r.at[index(h, unit_of(h, g))]
        chosen = []
        for c_ in range(nc):
            i = g * nc + c_
            hit = rank[i : i + 1, :] == want
            chosen.append(jnp.where(hit, 1.0, 0.0).astype(BF16))
            swbuf[pl.ds(base(h, g, c_), slots[h]), 0:col] = jnp.where(
                hit, weight[i : i + 1, :], 0.0
            ).astype(BF16)
        xsend[pl.ds(base(h, g, 0), both[h]), :] = jnp.dot(
            jnp.concatenate(chosen, axis=0), zbuf[first : first + col, 0:quarter],
            preferred_element_type=F32,
        ).astype(BF16)
        land = ybuf.at[y, rows(base(h, g, c), slots[h]), :]
        if g > 0:
            for c_ in range(nc):
                send(
                    xsend.at[pl.ds(base(h, g, c_), slots[h]), :], land, x_s,
                    recv, dev(to_x(g), y, z, c_),
                )
        else:
            other = 1 - c
            send(
                xsend.at[rows(base(h, g, other), slots[h]), :], land, x_s,
                recv, dev(x, y, z, other),
            )
            here = rows(base(h, g, c), slots[h])
            ybuf[y, here, :] = xsend[here, :]

    def x_wait(h, u):
        start, size = span(h, u)
        size = slots[h] if u == home(h) else size
        arrived(ybuf.at[y, pl.ds(start, size), :], x_r.at[index(h, u)])

    def spread(h, u):
        x_wait(h, u)
        start, size = span(h, u)
        block = ybuf.at[y, pl.ds(start, size), :]
        for d in (1, -1):
            send(block, block, y1_s, y1_r.at[index(h, u)], dev(x, at_y(d), z, c))

    def forward(h, u):
        start, size = span(h, u)
        arrived(ybuf.at[pl.ds(0, 2), pl.ds(start, size), :], y1_r.at[index(h, u)])
        for n, d in enumerate((1, -1)):
            block = ybuf.at[at_y(-d), pl.ds(start + n * size // 2, size // 2), :]
            send(block, block, y2_s, y2_r.at[index(h, u)], dev(x, at_y(d), z, c))

    def y_wait(h, u):
        arrived(ybuf.at[0, pl.ds(*span(h, u)), :], y2_r.at[index(h, u)])

    def experts(start, size):
        here = pl.ds(start, size)
        gate = jnp.zeros((size, wg.shape[1]), F32)
        upper = jnp.zeros((size, wg.shape[1]), F32)
        for q in range(ny):
            piece = ybuf[q, here, :]
            deep = pl.ds(q * quarter, quarter)
            gate += jnp.dot(piece, wg[deep, :], preferred_element_type=F32)
            upper += jnp.dot(piece, wu[deep, :], preferred_element_type=F32)
        hidden = (gate / (1.0 + jnp.exp(-gate)) * upper).astype(BF16)
        for q in range(ny):
            obuf[q, here, :] = jnp.dot(
                hidden, wd[:, q * quarter : (q + 1) * quarter], preferred_element_type=F32
            ).astype(BF16)

    def compute(h, u):
        y_wait(h, u)
        experts(*span(h, u))

    def compute_home():
        for h in range(len(parts)):
            y_wait(h, home(h))
        experts(0, home_rows)
        for h in range(len(parts)):
            other = 1 - c
            send(
                obuf.at[:, rows(base(h, 0, other), slots[h]), :],
                rbuf0.at[:, rows(base(h, 0, c), slots[h]), :],
                home_s, b_r.at[index(h, home(h))], dev(x, y, z, other),
            )
            here = rows(base(h, 0, c), slots[h])
            for q in range(ny):
                rbuf0[q, here, :] = obuf[q, here, :]

    def combine_home():
        for h in range(len(parts)):
            arrived(rbuf0.at[:, pl.ds(base(h, 0, 0), slots[h]), :], b_r.at[index(h, home(h))])
            here = pl.ds(base(h, 0, 0), both[h])
            first, col = tokens_of(h)
            for o in range(ny):
                term = lax.dot_general(
                    swbuf[here, 0:col], rbuf0[at_y(o), here, :], across, preferred_element_type=F32
                )
                if o == 0:
                    part[first : first + col, :] = term
                else:
                    part0[first : first + col, (o - 1) * quarter : o * quarter] = term

    def give_one(h, u):
        start, size = span(h, u)
        for n, d in enumerate((1, -1)):
            send(
                obuf.at[at_y(2), pl.ds(start + n * size // 2, size // 2), :],
                r1buf.at[n, pl.ds(start // 2, size // 2), :],
                p1_s, p1_r.at[index(h, u)], dev(x, at_y(d), z, c),
            )

    def give_two(h, u):
        start, size = span(h, u)
        arrived(r1buf.at[:, pl.ds(start // 2, size // 2), :], p1_r.at[index(h, u)])
        for n, d in enumerate((1, -1)):
            here = pl.ds(start + n * size // 2, size // 2)
            q = at_y(d)
            got = r1buf[n, pl.ds(start // 2, size // 2), :]
            obuf[q, here, :] = (obuf[q, here, :].astype(F32) + got.astype(F32)).astype(BF16)
            here = pl.ds(start, size)
            send(
                obuf.at[q, here, :], r2buf.at[n, here, :],
                p2_s, p2_r.at[index(h, u)], dev(x, at_y(d), z, c),
            )

    def give_back(h, u):
        here = pl.ds(*span(h, u))
        arrived(r2buf.at[:, here, :], p2_r.at[index(h, u)])
        total = obuf[y, here, :].astype(F32) + r2buf[0, here, :].astype(F32)
        xret[here, :] = (total + r2buf[1, here, :].astype(F32)).astype(BF16)
        for g in units[h][u]:
            land = rbuf.at[rows(base(h, g, c), slots[h]), :]
            for c_ in range(nc):
                send(
                    xret.at[pl.ds(base(h, g, c_), slots[h]), :], land, b_s,
                    b_r.at[index(h, u)], dev(from_x(g), y, z, c_),
                )

    def combine(h, u):
        here = pl.ds(*span(h, u))
        first, col = tokens_of(h)
        arrived(rbuf.at[here, :], b_r.at[index(h, u)])
        part[first : first + col, :] += lax.dot_general(
            swbuf[here, 0:col], rbuf[here, :], across, preferred_element_type=F32
        )

    reach = nz // 2

    def reducer(source, src, dst, ssem, rsem):
        def block_of(o):
            return source[pl.ds(place(o), tile), :]

        def zsend(d, k, hop, value):
            n = zslot(d, k)
            src[n, hop - 1] = value.astype(BF16)
            send(src.at[n, hop - 1], dst.at[n, hop - 1], ssem, rsem.at[n], dev(x, y, at_z(d * hop), c))

        def zget(d, k):
            n = zslot(d, k)
            if d < 0 and k == 1:
                arrived(dst.at[n, 0], rsem.at[n])
                return dst[n, 0].astype(F32)
            arrived(dst.at[n], rsem.at[n])
            return dst[n, 0].astype(F32) + dst[n, 1].astype(F32)

        def own_hop(k):
            if k == 1:
                zsend(1, 1, 2, block_of(reach))
            for d in (1, -1):
                zsend(d, k, 1, block_of(d * (reach + 1 - 2 * k)))

        def next_hop(k):
            for d in (1, -1):
                zsend(d, k + 1, 2, block_of(d * (reach - 2 * k)) + zget(d, k))

        def finish():
            return block_of(0) + zget(1, steps) + zget(-1, steps)

        return own_hop, next_hop, finish, block_of, zget

    own_hop, next_hop, _, block_of, zget = reducer(part, zs, zr, zrs_s, zrs_r)
    wide_own, wide_next, wide_finish, _, _ = reducer(part0, ws, wr, wrs_s, wrs_r)

    def wide_step(k):
        if k < steps:
            wide_next(k)
            wide_own(k + 1)

    def choose(h):
        rank, weight = routes(h)
        turns = (0, 3, 1, 2) if nx == 4 and h < far else range(nx)
        for g in turns:
            select(h, g, rank, weight)

    direct = nz // 4

    count = out_ref.shape[0]

    def straight(o):
        value = block_of(o)
        if abs(o) == direct:
            value = value + zget(1 if o > 0 else -1, mid)
        n = (o if o > 0 else direct - o) - 1 if o else 2 * direct
        for q in range(ny):
            ds[n, q] = value[q * count : (q + 1) * count, :].astype(BF16)
        for r in range(ny) if o else range(1, ny):
            send(
                ds.at[n, at_y(r)], dr.at[y, n], d_s if o else o_s, d_r.at[0 if o else 1],
                dev(x, at_y(r), at_z(o), c),
            )
        if o == 0:
            dr[y, n] = ds[n, y]

    def share_wide():
        wide = wide_finish()
        for q in range(ny):
            fsend[q] = wide[q * count : (q + 1) * count, :].astype(BF16)
        for r in (2, 1, 3):
            send(fsend.at[at_y(r)], frecv.at[y], f_s, f_r.at[0], dev(x, at_y(r), z, c))
        frecv[y] = fsend[y]

    def gathered(j):
        where = at_y(j)
        total = dr[where, 2 * direct].astype(F32)
        for r in range(ny):
            o = (j - r) % ny
            if o:
                total += frecv[at_y(r), :, (o - 1) * quarter : o * quarter].astype(F32)
        for n in range(2 * direct):
            total += dr[where, n].astype(F32)
        return total.astype(BF16)

    near, between = 0, range(1, far)
    outer = range(len(units[far]) - 1)
    for d in (1, -1):
        gather_send(1, d)
    gather_step(1)
    gather_rest(near)
    choose(near)
    spread(near, home(near))
    for h in between:
        gather_step(h + 1)
    spread(near, 0)
    for h in between:
        gather_rest(h)
        choose(h)
        spread(h, home(h))
    forward(near, home(near))
    for k in range(far + 1, steps):
        gather_step(k)
    for h in between:
        spread(h, 0)
    gather_step(steps)
    gather_rest(far)
    choose(far)
    forward(near, 0)
    spread(far, home(far))
    for h in between:
        forward(h, home(h))
        forward(h, 0)
    forward(far, home(far))
    for u in outer:
        spread(far, u)
    for load in loads:
        load.wait()
    for h in range(far):
        compute(h, 0)
    compute_home()
    forward(far, 0)
    combine_home()
    wide_own(1)
    for u in outer[1:]:
        forward(far, u)
    for u in outer:
        compute(far, u)
        give_one(far, u)
        if u == 0:
            for h in between:
                give_one(h, 0)
    wide_step(1)
    for u in outer:
        give_two(far, u)
    give_one(near, 0)
    for h in range(far - 1, -1, -1):
        give_two(h, 0)
    wide_step(2)
    for u in outer:
        give_back(far, u)
    for k in range(3, steps):
        wide_step(k)
    for u in outer:
        combine(far, u)
    for k in range(1, mid + 1):
        own_hop(k)
    for h in between:
        give_back(h, 0)
    for k in range(1, mid):
        next_hop(k)
    give_back(near, 0)
    for h in between:
        combine(h, 0)
        for o in (3, -3, 2):
            straight(o)
    share_wide()
    combine(near, 0)
    for o in range(2 if nz > 8 else 1, 0, -1):
        straight(-o)
    straight(1)
    straight(0)
    for o in (direct, -direct):
        straight(o)
    arrived(frecv.at[pl.ds(0, ny - 1)], f_r.at[0])
    arrived(dr.at[pl.ds(0, ny - 1), 2 * direct], d_r.at[1])
    arrived(dr.at[:, pl.ds(0, 2 * direct)], d_r.at[0])
    for j in range(ny):
        piece = pl.ds(pl.multiple_of(at_y(j) * quarter, 128), quarter)
        out_ref[:, piece] = gathered(j)

    every = ybuf.shape[1]
    moved = every - home_rows
    sent = sum(slots)
    for sem, ref in (
        (zag_s, zbuf.at[pl.ds(0, (nz - 1) * tile), :]),
        (x_s, xsend.at[pl.ds(0, (nx * nc - 1) * sent), :]),
        (y1_s, ybuf.at[pl.ds(0, 2), :, :]),
        (y2_s, ybuf.at[0]),
        (p1_s, ybuf.at[0, pl.ds(0, moved), :]),
        (p2_s, r2buf.at[:, pl.ds(0, moved), :]),
        (b_s, xret.at[pl.ds(0, moved), :]),
        (home_s, rbuf0.at[:, pl.ds(0, sent), :]),
        (zrs_s, ybuf.at[0, pl.ds(0, (4 * mid - 1) * tile), :]),
        (d_s, ds.at[pl.ds(0, 2 * direct)]),
        (o_s, ds.at[0, pl.ds(0, ny - 1)]),
        (wrs_s, part0.at[pl.ds(0, (nz - 1) * tile // 2), :]),
        (f_s, fsend.at[pl.ds(0, ny - 1)]),
    ):
        awaits(ref, sem).wait_send()


def on_device(tokens, expert_ids, route_logits, expert_gate, expert_up, expert_down):
    n_ep, ny = lax.axis_size("ep"), N_DP
    nx, nc = CHIPS_X, CORES
    nz = n_ep // (nx * nc)
    tile, width = tokens.shape
    hidden = expert_gate.shape[2]
    quarter = width // ny
    col, slots = nz * tile, nz * CAP
    every = nx * nc * slots
    steps = nz // 4
    dma = pltpu.SemaphoreType.DMA
    vmem = pl.BlockSpec(memory_space=pltpu.VMEM)
    hbm = pl.BlockSpec(memory_space=pl.ANY)
    flops = 6 * every * width * hidden
    units = 7
    home = 2 * nc * slots // 2
    return pl.pallas_call(
        functools.partial(kernel, nx, nz),
        out_shape=jax.ShapeDtypeStruct((tile // ny, width), BF16),
        in_specs=[hbm] * 6,
        out_specs=vmem,
        scratch_shapes=[
            pltpu.VMEM(expert_ids.shape[::-1], jnp.int32),
            pltpu.VMEM(expert_ids.shape[::-1], F32),
            pltpu.VMEM((width, hidden), BF16),
            pltpu.VMEM((width, hidden), BF16),
            pltpu.VMEM((hidden, width), BF16),
            pltpu.VMEM((col, quarter + 128), BF16),
            pltpu.VMEM((every, col // 2), BF16),
            pltpu.VMEM((every, quarter), BF16),
            pltpu.VMEM((ny, every, quarter), BF16),
            pltpu.VMEM((ny, every, quarter), BF16),
            pltpu.VMEM((2, every // 2, quarter), BF16),
            pltpu.VMEM((2, every, quarter), BF16),
            pltpu.VMEM((every, quarter), BF16),
            pltpu.VMEM((every, quarter), BF16),
            pltpu.VMEM((ny, home, quarter), BF16),
            pltpu.VMEM((col, quarter), F32),
            pltpu.VMEM((col, width - quarter), F32),
            pltpu.VMEM((2 * steps, 2, tile, quarter), BF16),
            pltpu.VMEM((2 * steps, 2, tile, quarter), BF16),
            pltpu.VMEM((2 * steps, 2, tile, width - quarter), BF16),
            pltpu.VMEM((2 * steps, 2, tile, width - quarter), BF16),
            pltpu.VMEM((2 * steps + 1, ny, tile // ny, quarter), BF16),
            pltpu.VMEM((ny, 2 * steps + 1, tile // ny, quarter), BF16),
            pltpu.VMEM((ny, tile // ny, width - quarter), BF16),
            pltpu.VMEM((ny, tile // ny, width - quarter), BF16),
            dma((6,)),
            dma((13,)),
            dma((2 * steps,)), dma((3,)),
            dma((units,)), dma((units,)), dma((units,)), dma((units,)), dma((units,)), dma((units,)),
            dma((2 * steps,)), dma((2 * steps,)), dma((1,)), dma((2,)),
        ],
        compiler_params=pltpu.CompilerParams(
            collective_id=0, has_side_effects=True, vmem_limit_bytes=56 * 1024 * 1024
        ),
        cost_estimate=pl.CostEstimate(flops=flops, bytes_accessed=8 << 20, transcendentals=0),
    )(expert_ids.T, route_logits.T, tokens, expert_gate, expert_up, expert_down)


def solution(mesh):
    placed = (
        P("ep", None),
        P("ep", None),
        P("ep", None),
        P("ep", None, "dp"),
        P("ep", None, "dp"),
        P("ep", "dp", None),
    )
    return jax.shard_map(
        on_device, mesh=mesh, in_specs=placed, out_specs=P(("ep", "dp"), None), check_vma=False
    )
```

```python
import functools

import jax
import jax.numpy as jnp
from jax import lax
from jax.experimental import pallas as pl
from jax.experimental.pallas import tpu as pltpu
from jax.sharding import PartitionSpec as P

MESH = pl.DeviceIdType.MESH
F32 = jnp.float32
BF16 = jnp.bfloat16
ROUTE_SCALE = 2.5
CAP = 4
CHIPS_X = 4
CORES = 2
N_DP = 4


def kernel(
    nx, nz, ids_hbm, logits_hbm, tok_hbm, wg_hbm, wu_hbm, wd_hbm, out_ref,
    ids_ref, logits_ref, wg, wu, wd, zbuf, swbuf, xsend, ybuf, obuf, r1buf, r2buf, xret, rbuf, rbuf0, part, part0,
    zs, zr, ws, wr, ds, dr, fsend, frecv,
    w_sem, s_sem, zag_r, zag_one, x_r, y1_r, y2_r, p1_r, p2_r, b_r, zrs_r, wrs_r, f_r, d_r,
):
    nc, ny = CORES, N_DP
    tile, width = tok_hbm.shape
    quarter = width // ny
    top = ids_ref.shape[0]
    steps = nz // 4
    mid = steps // 2
    parts = [(-2, -1, 0, 1)]
    if nz > 8:
        parts.append((2, 3, -4, -3))
    parts.append(tuple(range(nz // 4 if nz > 8 else 2, nz - (4 if nz > 8 else 2))))
    far = len(parts) - 1
    order = [o % nz for part_ in parts for o in part_]
    starts = [sum(len(p) for p in parts[:i]) for i in range(len(parts))]
    slots = [len(p) * CAP for p in parts]
    both = [nc * n for n in slots]
    home_rows = sum(both)
    offsets = {2: (0, 1), 4: (0, 1, 3, 2)}[nx]
    units = [
        {2: ((1,), (0,)), 4: ((1, 2, 3), (0,)) if h < far else ((3,), (1, 2), (0,))}[nx]
        for h in range(len(parts))
    ]
    unit_index = {}
    for h in range(len(parts)):
        for u in range(len(units[h])):
            unit_index[h, u] = len(unit_index)
    (zag_s, x_s, y1_s, y2_s, p1_s, p2_s, b_s, home_s, zrs_s, wrs_s, f_s, d_s, o_s) = [
        s_sem.at[i] for i in range(13)
    ]
    ep = lax.axis_index("ep")
    y = lax.axis_index("dp")
    c = lax.rem(ep, nc)
    z = lax.rem(lax.div(ep, nc), nz)
    x = lax.div(ep, nc * nz)

    def dev(x_, y_, z_, c_):
        return (((x_ * nz + z_) * nc + c_), y_)

    def to_x(g):
        return lax.rem(x + (nx - offsets[g]), nx)

    def from_x(g):
        return lax.rem(x + offsets[g], nx)

    def at_y(o):
        return lax.rem(y + (o + ny), ny)

    def at_z(o):
        return lax.rem(z + (o + nz), nz)

    def place(o):
        return order.index(o % nz) * tile

    def tokens_of(h):
        return starts[h] * tile, len(parts[h]) * tile

    def rows(start, size):
        if isinstance(start, int):
            return pl.ds(start, size)
        return pl.ds(pl.multiple_of(start, size), size)

    def base(h, g, c_):
        if g == 0:
            return sum(both[:h]) + c_ * slots[h]
        done = sum(both[:h]) * (nx - 1)
        return home_rows + done + (g - 1) * both[h] + c_ * slots[h]

    def span(h, u):
        first = min(units[h][u])
        return base(h, first, 0), len(units[h][u]) * both[h]

    def index(h, u):
        return unit_index[h, u]

    def home(h):
        return len(units[h]) - 1

    def send(src, dst, ssem, rsem, device):
        pltpu.make_async_remote_copy(
            src_ref=src, dst_ref=dst, send_sem=ssem, recv_sem=rsem,
            device_id=device, device_id_type=MESH,
        ).start()

    def awaits(ref, sem):
        return pltpu.make_async_remote_copy(
            src_ref=ref, dst_ref=ref, send_sem=sem, recv_sem=sem,
            device_id=dev(x, y, z, 1 - c), device_id_type=MESH,
        )

    def arrived(ref, sem):
        awaits(ref, sem).wait_recv()

    barrier = pltpu.get_barrier_semaphore()
    peers = [dev(x, y, at_z(o), c) for o in (1, -1, 2, -2)]
    peers += [dev(from_x(g), y, z, c_) for g in range(1, nx) for c_ in range(nc)]
    peers += [dev(x, y, z, 1 - c)]
    peers += [dev(x, at_y(o), z, c) for o in range(1, ny)]
    for peer in peers:
        pl.semaphore_signal(barrier, inc=1, device_id=peer, device_id_type=MESH)

    own = pl.ds(place(0), tile)
    mine = pltpu.make_async_copy(
        tok_hbm.at[:, pl.ds(pl.multiple_of(y * quarter, 128), quarter)],
        zbuf.at[own, pl.ds(0, quarter)], w_sem.at[3],
    )
    names = [
        pltpu.make_async_copy(ids_hbm, ids_ref, w_sem.at[4]),
        pltpu.make_async_copy(logits_hbm, logits_ref, w_sem.at[5]),
    ]
    for copy in names:
        copy.start()
    mine.start()
    for copy in names:
        copy.wait()
    scores = 1.0 / (1.0 + jnp.exp(-logits_ref[...]))
    wts = ROUTE_SCALE * scores / jnp.sum(scores, axis=0, keepdims=True)
    lane = lax.broadcasted_iota(jnp.int32, (top, 128), 1)
    sub = lax.broadcasted_iota(jnp.int32, (top, 128), 0)
    put_id = (lane == sub).astype(BF16)
    put_w = (lane == sub + top).astype(BF16)
    across = (((0,), (0,)), ((), ()))
    meta = lax.dot_general(
        ids_ref[...].astype(F32).astype(BF16), put_id, across, preferred_element_type=F32
    ) + lax.dot_general(wts.astype(BF16), put_w, across, preferred_element_type=F32)
    zbuf[own, quarter : quarter + 128] = meta.astype(BF16)

    loads = [
        pltpu.make_async_copy(s.at[0], d, w_sem.at[i])
        for i, (s, d) in enumerate(((wg_hbm, wg), (wu_hbm, wu), (wd_hbm, wd)))
    ]
    for load in loads:
        load.start()
    mine.wait()
    pl.semaphore_wait(barrier, len(peers))

    def zslot(d, k):
        return (0 if d > 0 else 1) * steps + (k - 1)

    def ready(k):
        return min(k - 1, far)

    def gather_send(k, d):
        o = -d * 2 * (k - 1)
        for hop in (2, 1):
            if hop == 2 and d < 0 and k == steps:
                continue
            rsem = zag_r.at[zslot(d, k)] if hop == 2 else zag_one.at[ready(k)]
            send(
                zbuf.at[pl.ds(place(o), tile), :], zbuf.at[pl.ds(place(o - d * hop), tile), :],
                zag_s, rsem, dev(x, y, at_z(d * hop), c),
            )

    def gather_step(k):
        for d in (1, -1):
            if d > 0 or k < steps:
                arrived(zbuf.at[pl.ds(0, tile), :], zag_r.at[zslot(d, k)])
            if k < steps:
                gather_send(k + 1, d)

    def gather_rest(h):
        count = sum(ready(k) == h for k in range(1, steps + 1))
        arrived(zbuf.at[pl.ds(0, 2 * count * tile), :], zag_one.at[h])

    def routes(h):
        first, col = tokens_of(h)
        pick = (
            lax.broadcasted_iota(jnp.int32, (2 * top, 128), 0)
            == lax.broadcasted_iota(jnp.int32, (2 * top, 128), 1)
        ).astype(BF16)
        by_token = lax.dot_general(
            pick, zbuf[first : first + col, quarter : quarter + 128],
            (((1,), (1,)), ((), ())), preferred_element_type=F32,
        )
        lanes = nx * nc
        j = lax.broadcasted_iota(jnp.int32, (lanes, col), 0)
        jg, jc = lax.div(j, nc), lax.rem(j, nc)
        off = jnp.zeros_like(jg)
        for g, o in enumerate(offsets):
            off = jnp.where(jg == g, nx - o, off)
        expert = ((lax.rem(x + off, nx) * nz + z) * nc + jc).astype(F32)
        named = jnp.zeros((lanes, col), F32)
        weight = jnp.zeros((lanes, col), F32)
        for k in range(top):
            hit = by_token[k : k + 1, :] == expert
            named = jnp.where(hit, 1.0, named)
            weight = jnp.where(hit, by_token[top + k : top + k + 1, :], weight)
        t_row = lax.broadcasted_iota(jnp.int32, (col, col), 0)
        t_col = lax.broadcasted_iota(jnp.int32, (col, col), 1)
        before = ((t_row < t_col) & (lax.div(t_row, tile) == lax.div(t_col, tile))).astype(BF16)
        rank = jnp.dot(named.astype(BF16), before, preferred_element_type=F32)
        return jnp.where(named > 0.5, rank, -1.0), weight

    def unit_of(h, g):
        return [g in unit for unit in units[h]].index(True)

    def select(h, g, rank, weight):
        first, col = tokens_of(h)
        s_row = lax.broadcasted_iota(jnp.int32, (slots[h], col), 0)
        s_col = lax.broadcasted_iota(jnp.int32, (slots[h], col), 1)
        in_block = lax.div(s_row, CAP) == lax.div(s_col, tile)
        want = jnp.where(in_block, lax.rem(s_row, CAP).astype(F32), -2.0)
        recv = x_r.at[index(h, unit_of(h, g))]
        chosen = []
        for c_ in range(nc):
            i = g * nc + c_
            hit = rank[i : i + 1, :] == want
            chosen.append(jnp.where(hit, 1.0, 0.0).astype(BF16))
            swbuf[pl.ds(base(h, g, c_), slots[h]), 0:col] = jnp.where(
                hit, weight[i : i + 1, :], 0.0
            ).astype(BF16)
        xsend[pl.ds(base(h, g, 0), both[h]), :] = jnp.dot(
            jnp.concatenate(chosen, axis=0), zbuf[first : first + col, 0:quarter],
            preferred_element_type=F32,
        ).astype(BF16)
        land = ybuf.at[y, rows(base(h, g, c), slots[h]), :]
        if g > 0:
            for c_ in range(nc):
                send(
                    xsend.at[pl.ds(base(h, g, c_), slots[h]), :], land, x_s,
                    recv, dev(to_x(g), y, z, c_),
                )
        else:
            other = 1 - c
            send(
                xsend.at[rows(base(h, g, other), slots[h]), :], land, x_s,
                recv, dev(x, y, z, other),
            )
            here = rows(base(h, g, c), slots[h])
            ybuf[y, here, :] = xsend[here, :]

    def x_wait(h, u):
        start, size = span(h, u)
        size = slots[h] if u == home(h) else size
        arrived(ybuf.at[y, pl.ds(start, size), :], x_r.at[index(h, u)])

    def spread(h, u):
        x_wait(h, u)
        start, size = span(h, u)
        block = ybuf.at[y, pl.ds(start, size), :]
        for d in (1, -1):
            send(block, block, y1_s, y1_r.at[index(h, u)], dev(x, at_y(d), z, c))

    def forward(h, u):
        start, size = span(h, u)
        arrived(ybuf.at[pl.ds(0, 2), pl.ds(start, size), :], y1_r.at[index(h, u)])
        for n, d in enumerate((1, -1)):
            block = ybuf.at[at_y(-d), pl.ds(start + n * size // 2, size // 2), :]
            send(block, block, y2_s, y2_r.at[index(h, u)], dev(x, at_y(d), z, c))

    def y_wait(h, u):
        arrived(ybuf.at[0, pl.ds(*span(h, u)), :], y2_r.at[index(h, u)])

    def experts(start, size):
        here = pl.ds(start, size)
        gate = jnp.zeros((size, wg.shape[1]), F32)
        upper = jnp.zeros((size, wg.shape[1]), F32)
        for q in range(ny):
            piece = ybuf[q, here, :]
            deep = pl.ds(q * quarter, quarter)
            gate += jnp.dot(piece, wg[deep, :], preferred_element_type=F32)
            upper += jnp.dot(piece, wu[deep, :], preferred_element_type=F32)
        hidden = (gate / (1.0 + jnp.exp(-gate)) * upper).astype(BF16)
        for q in range(ny):
            obuf[q, here, :] = jnp.dot(
                hidden, wd[:, q * quarter : (q + 1) * quarter], preferred_element_type=F32
            ).astype(BF16)

    def compute(h, u):
        y_wait(h, u)
        experts(*span(h, u))

    def compute_home():
        for h in range(len(parts)):
            y_wait(h, home(h))
        experts(0, home_rows)
        for h in range(len(parts)):
            other = 1 - c
            send(
                obuf.at[:, rows(base(h, 0, other), slots[h]), :],
                rbuf0.at[:, rows(base(h, 0, c), slots[h]), :],
                home_s, b_r.at[index(h, home(h))], dev(x, y, z, other),
            )
            here = rows(base(h, 0, c), slots[h])
            for q in range(ny):
                rbuf0[q, here, :] = obuf[q, here, :]

    def combine_home():
        for h in range(len(parts)):
            arrived(rbuf0.at[:, pl.ds(base(h, 0, 0), slots[h]), :], b_r.at[index(h, home(h))])
            here = pl.ds(base(h, 0, 0), both[h])
            first, col = tokens_of(h)
            for o in range(ny):
                term = lax.dot_general(
                    swbuf[here, 0:col], rbuf0[at_y(o), here, :], across, preferred_element_type=F32
                )
                if o == 0:
                    part[first : first + col, :] = term
                else:
                    part0[first : first + col, (o - 1) * quarter : o * quarter] = term

    def give_one(h, u):
        start, size = span(h, u)
        for n, d in enumerate((1, -1)):
            send(
                obuf.at[at_y(2), pl.ds(start + n * size // 2, size // 2), :],
                r1buf.at[n, pl.ds(start // 2, size // 2), :],
                p1_s, p1_r.at[index(h, u)], dev(x, at_y(d), z, c),
            )

    def give_two(h, u):
        start, size = span(h, u)
        arrived(r1buf.at[:, pl.ds(start // 2, size // 2), :], p1_r.at[index(h, u)])
        for n, d in enumerate((1, -1)):
            here = pl.ds(start + n * size // 2, size // 2)
            q = at_y(d)
            got = r1buf[n, pl.ds(start // 2, size // 2), :]
            obuf[q, here, :] = (obuf[q, here, :].astype(F32) + got.astype(F32)).astype(BF16)
            here = pl.ds(start, size)
            send(
                obuf.at[q, here, :], r2buf.at[n, here, :],
                p2_s, p2_r.at[index(h, u)], dev(x, at_y(d), z, c),
            )

    def give_back(h, u):
        here = pl.ds(*span(h, u))
        arrived(r2buf.at[:, here, :], p2_r.at[index(h, u)])
        total = obuf[y, here, :].astype(F32) + r2buf[0, here, :].astype(F32)
        xret[here, :] = (total + r2buf[1, here, :].astype(F32)).astype(BF16)
        for g in units[h][u]:
            land = rbuf.at[rows(base(h, g, c), slots[h]), :]
            for c_ in range(nc):
                send(
                    xret.at[pl.ds(base(h, g, c_), slots[h]), :], land, b_s,
                    b_r.at[index(h, u)], dev(from_x(g), y, z, c_),
                )

    def combine(h, u):
        here = pl.ds(*span(h, u))
        first, col = tokens_of(h)
        arrived(rbuf.at[here, :], b_r.at[index(h, u)])
        part[first : first + col, :] += lax.dot_general(
            swbuf[here, 0:col], rbuf[here, :], across, preferred_element_type=F32
        )

    reach = nz // 2

    def reducer(source, src, dst, ssem, rsem):
        def block_of(o):
            return source[pl.ds(place(o), tile), :]

        def zsend(d, k, hop, value):
            n = zslot(d, k)
            src[n, hop - 1] = value.astype(BF16)
            send(src.at[n, hop - 1], dst.at[n, hop - 1], ssem, rsem.at[n], dev(x, y, at_z(d * hop), c))

        def zget(d, k):
            n = zslot(d, k)
            if d < 0 and k == 1:
                arrived(dst.at[n, 0], rsem.at[n])
                return dst[n, 0].astype(F32)
            arrived(dst.at[n], rsem.at[n])
            return dst[n, 0].astype(F32) + dst[n, 1].astype(F32)

        def own_hop(k):
            if k == 1:
                zsend(1, 1, 2, block_of(reach))
            for d in (1, -1):
                zsend(d, k, 1, block_of(d * (reach + 1 - 2 * k)))

        def next_hop(k):
            for d in (1, -1):
                zsend(d, k + 1, 2, block_of(d * (reach - 2 * k)) + zget(d, k))

        def finish():
            return block_of(0) + zget(1, steps) + zget(-1, steps)

        return own_hop, next_hop, finish, block_of, zget

    own_hop, next_hop, _, block_of, zget = reducer(part, zs, zr, zrs_s, zrs_r)
    wide_own, wide_next, wide_finish, _, _ = reducer(part0, ws, wr, wrs_s, wrs_r)

    def wide_step(k):
        if k < steps:
            wide_next(k)
            wide_own(k + 1)

    def choose(h):
        rank, weight = routes(h)
        turns = (0, 3, 1, 2) if nx == 4 and h < far else range(nx)
        for g in turns:
            select(h, g, rank, weight)

    direct = nz // 4

    count = out_ref.shape[0]

    def straight(o):
        value = block_of(o)
        if abs(o) == direct:
            value = value + zget(1 if o > 0 else -1, mid)
        n = (o if o > 0 else direct - o) - 1 if o else 2 * direct
        for q in range(ny):
            ds[n, q] = value[q * count : (q + 1) * count, :].astype(BF16)
        for r in range(ny) if o else range(1, ny):
            send(
                ds.at[n, at_y(r)], dr.at[y, n], d_s if o else o_s, d_r.at[0 if o else 1],
                dev(x, at_y(r), at_z(o), c),
            )
        if o == 0:
            dr[y, n] = ds[n, y]

    def share_wide():
        wide = wide_finish()
        for q in range(ny):
            fsend[q] = wide[q * count : (q + 1) * count, :].astype(BF16)
        for r in (2, 1, 3):
            send(fsend.at[at_y(r)], frecv.at[y], f_s, f_r.at[0], dev(x, at_y(r), z, c))
        frecv[y] = fsend[y]

    def gathered(j):
        where = at_y(j)
        total = dr[where, 2 * direct].astype(F32)
        for r in range(ny):
            o = (j - r) % ny
            if o:
                total += frecv[at_y(r), :, (o - 1) * quarter : o * quarter].astype(F32)
        for n in range(2 * direct):
            total += dr[where, n].astype(F32)
        return total.astype(BF16)

    near, between = 0, range(1, far)
    outer = range(len(units[far]) - 1)
    for d in (1, -1):
        gather_send(1, d)
    gather_step(1)
    gather_rest(near)
    choose(near)
    spread(near, home(near))
    for h in between:
        gather_step(h + 1)
    spread(near, 0)
    for h in between:
        gather_rest(h)
        choose(h)
        spread(h, home(h))
    forward(near, home(near))
    for k in range(far + 1, steps):
        gather_step(k)
    for h in between:
        spread(h, 0)
    gather_step(steps)
    gather_rest(far)
    choose(far)
    forward(near, 0)
    spread(far, home(far))
    for h in between:
        forward(h, home(h))
        forward(h, 0)
    forward(far, home(far))
    for u in outer:
        spread(far, u)
    for load in loads:
        load.wait()
    for h in range(far):
        compute(h, 0)
    compute_home()
    forward(far, 0)
    combine_home()
    wide_own(1)
    for u in outer[1:]:
        forward(far, u)
    for u in outer:
        compute(far, u)
        give_one(far, u)
        if u == 0:
            for h in between:
                give_one(h, 0)
    wide_step(1)
    give_two(far, 0)
    give_one(near, 0)
    for u in outer[1:]:
        give_two(far, u)
    for h in between:
        give_two(h, 0)
    wide_step(2)
    give_back(far, 0)
    give_two(near, 0)
    for u in outer[1:]:
        give_back(far, u)
    for k in range(3, steps):
        wide_step(k)
    combine(far, 0)
    for h in between:
        give_back(h, 0)
    for u in outer[1:]:
        combine(far, u)
    for k in range(1, mid + 1):
        own_hop(k)
    give_back(near, 0)
    for k in range(1, mid):
        next_hop(k)
    for h in between:
        combine(h, 0)
        for o in (3, -3, 2):
            straight(o)
    share_wide()
    combine(near, 0)
    for o in range(2 if nz > 8 else 1, 0, -1):
        straight(-o)
    straight(1)
    straight(0)
    for o in (direct, -direct):
        straight(o)
    arrived(frecv.at[pl.ds(0, ny - 1)], f_r.at[0])
    arrived(dr.at[pl.ds(0, ny - 1), 2 * direct], d_r.at[1])
    arrived(dr.at[:, pl.ds(0, 2 * direct)], d_r.at[0])
    for j in range(ny):
        piece = pl.ds(pl.multiple_of(at_y(j) * quarter, 128), quarter)
        out_ref[:, piece] = gathered(j)

    every = ybuf.shape[1]
    moved = every - home_rows
    sent = sum(slots)
    for sem, ref in (
        (zag_s, zbuf.at[pl.ds(0, (nz - 1) * tile), :]),
        (x_s, xsend.at[pl.ds(0, (nx * nc - 1) * sent), :]),
        (y1_s, ybuf.at[pl.ds(0, 2), :, :]),
        (y2_s, ybuf.at[0]),
        (p1_s, ybuf.at[0, pl.ds(0, moved), :]),
        (p2_s, r2buf.at[:, pl.ds(0, moved), :]),
        (b_s, xret.at[pl.ds(0, moved), :]),
        (home_s, rbuf0.at[:, pl.ds(0, sent), :]),
        (zrs_s, ybuf.at[0, pl.ds(0, (4 * mid - 1) * tile), :]),
        (d_s, ds.at[pl.ds(0, 2 * direct)]),
        (o_s, ds.at[0, pl.ds(0, ny - 1)]),
        (wrs_s, part0.at[pl.ds(0, (nz - 1) * tile // 2), :]),
        (f_s, fsend.at[pl.ds(0, ny - 1)]),
    ):
        awaits(ref, sem).wait_send()


def on_device(tokens, expert_ids, route_logits, expert_gate, expert_up, expert_down):
    n_ep, ny = lax.axis_size("ep"), N_DP
    nx, nc = CHIPS_X, CORES
    nz = n_ep // (nx * nc)
    tile, width = tokens.shape
    hidden = expert_gate.shape[2]
    quarter = width // ny
    col, slots = nz * tile, nz * CAP
    every = nx * nc * slots
    steps = nz // 4
    dma = pltpu.SemaphoreType.DMA
    vmem = pl.BlockSpec(memory_space=pltpu.VMEM)
    hbm = pl.BlockSpec(memory_space=pl.ANY)
    flops = 6 * every * width * hidden
    units = 7
    home = 2 * nc * slots // 2
    return pl.pallas_call(
        functools.partial(kernel, nx, nz),
        out_shape=jax.ShapeDtypeStruct((tile // ny, width), BF16),
        in_specs=[hbm] * 6,
        out_specs=vmem,
        scratch_shapes=[
            pltpu.VMEM(expert_ids.shape[::-1], jnp.int32),
            pltpu.VMEM(expert_ids.shape[::-1], F32),
            pltpu.VMEM((width, hidden), BF16),
            pltpu.VMEM((width, hidden), BF16),
            pltpu.VMEM((hidden, width), BF16),
            pltpu.VMEM((col, quarter + 128), BF16),
            pltpu.VMEM((every, col // 2), BF16),
            pltpu.VMEM((every, quarter), BF16),
            pltpu.VMEM((ny, every, quarter), BF16),
            pltpu.VMEM((ny, every, quarter), BF16),
            pltpu.VMEM((2, every // 2, quarter), BF16),
            pltpu.VMEM((2, every, quarter), BF16),
            pltpu.VMEM((every, quarter), BF16),
            pltpu.VMEM((every, quarter), BF16),
            pltpu.VMEM((ny, home, quarter), BF16),
            pltpu.VMEM((col, quarter), F32),
            pltpu.VMEM((col, width - quarter), F32),
            pltpu.VMEM((2 * steps, 2, tile, quarter), BF16),
            pltpu.VMEM((2 * steps, 2, tile, quarter), BF16),
            pltpu.VMEM((2 * steps, 2, tile, width - quarter), BF16),
            pltpu.VMEM((2 * steps, 2, tile, width - quarter), BF16),
            pltpu.VMEM((2 * steps + 1, ny, tile // ny, quarter), BF16),
            pltpu.VMEM((ny, 2 * steps + 1, tile // ny, quarter), BF16),
            pltpu.VMEM((ny, tile // ny, width - quarter), BF16),
            pltpu.VMEM((ny, tile // ny, width - quarter), BF16),
            dma((6,)),
            dma((13,)),
            dma((2 * steps,)), dma((3,)),
            dma((units,)), dma((units,)), dma((units,)), dma((units,)), dma((units,)), dma((units,)),
            dma((2 * steps,)), dma((2 * steps,)), dma((1,)), dma((2,)),
        ],
        compiler_params=pltpu.CompilerParams(
            collective_id=0, has_side_effects=True, vmem_limit_bytes=56 * 1024 * 1024
        ),
        cost_estimate=pl.CostEstimate(flops=flops, bytes_accessed=8 << 20, transcendentals=0),
    )(expert_ids.T, route_logits.T, tokens, expert_gate, expert_up, expert_down)


def solution(mesh):
    placed = (
        P("ep", None),
        P("ep", None),
        P("ep", None),
        P("ep", None, "dp"),
        P("ep", None, "dp"),
        P("ep", "dp", None),
    )
    return jax.shard_map(
        on_device, mesh=mesh, in_specs=placed, out_specs=P(("ep", "dp"), None), check_vma=False
    )
```

```python
import functools

import jax
import jax.numpy as jnp
from jax import lax
from jax.experimental import pallas as pl
from jax.experimental.pallas import tpu as pltpu
from jax.sharding import PartitionSpec as P

MESH = pl.DeviceIdType.MESH
F32 = jnp.float32
BF16 = jnp.bfloat16
ROUTE_SCALE = 2.5
CAP = 4
CHIPS_X = 4
CORES = 2
N_DP = 4


def kernel(
    nx, nz, ids_hbm, logits_hbm, tok_hbm, wg_hbm, wu_hbm, wd_hbm, out_ref,
    ids_ref, logits_ref, wg, wu, wd, zbuf, swbuf, xsend, ybuf, obuf, r1buf, r2buf, xret, rbuf, rbuf0, part, part0,
    zs, zr, ws, wr, ds, dr, fsend, frecv,
    w_sem, s_sem, zag_r, zag_one, x_r, y1_r, y2_r, p1_r, p2_r, b_r, zrs_r, wrs_r, f_r, d_r,
):
    nc, ny = CORES, N_DP
    tile, width = tok_hbm.shape
    quarter = width // ny
    top = ids_ref.shape[0]
    steps = nz // 4
    mid = steps // 2
    parts = [(-2, -1, 0, 1)]
    if nz > 8:
        parts.append((2, 3, -4, -3))
    parts.append(tuple(range(nz // 4 if nz > 8 else 2, nz - (4 if nz > 8 else 2))))
    far = len(parts) - 1
    order = [o % nz for part_ in parts for o in part_]
    starts = [sum(len(p) for p in parts[:i]) for i in range(len(parts))]
    slots = [len(p) * CAP for p in parts]
    both = [nc * n for n in slots]
    home_rows = sum(both)
    offsets = {2: (0, 1), 4: (0, 1, 3, 2)}[nx]
    units = [
        {2: ((1,), (0,)), 4: ((1, 2), (3,), (0,))}[nx] for h in range(len(parts))
    ]
    unit_index = {}
    for h in range(len(parts)):
        for u in range(len(units[h])):
            unit_index[h, u] = len(unit_index)
    (zag_s, x_s, y1_s, y2_s, p1_s, p2_s, b_s, home_s, zrs_s, wrs_s, f_s, d_s, o_s) = [
        s_sem.at[i] for i in range(13)
    ]
    ep = lax.axis_index("ep")
    y = lax.axis_index("dp")
    c = lax.rem(ep, nc)
    z = lax.rem(lax.div(ep, nc), nz)
    x = lax.div(ep, nc * nz)

    def dev(x_, y_, z_, c_):
        return (((x_ * nz + z_) * nc + c_), y_)

    def to_x(g):
        return lax.rem(x + (nx - offsets[g]), nx)

    def from_x(g):
        return lax.rem(x + offsets[g], nx)

    def at_y(o):
        return lax.rem(y + (o + ny), ny)

    def at_z(o):
        return lax.rem(z + (o + nz), nz)

    def place(o):
        return order.index(o % nz) * tile

    def tokens_of(h):
        return starts[h] * tile, len(parts[h]) * tile

    def rows(start, size):
        if isinstance(start, int):
            return pl.ds(start, size)
        return pl.ds(pl.multiple_of(start, size), size)

    def base(h, g, c_):
        if g == 0:
            return sum(both[:h]) + c_ * slots[h]
        done = sum(both[:h]) * (nx - 1)
        return home_rows + done + (g - 1) * both[h] + c_ * slots[h]

    def span(h, u):
        first = min(units[h][u])
        return base(h, first, 0), len(units[h][u]) * both[h]

    def index(h, u):
        return unit_index[h, u]

    def home(h):
        return len(units[h]) - 1

    def send(src, dst, ssem, rsem, device):
        pltpu.make_async_remote_copy(
            src_ref=src, dst_ref=dst, send_sem=ssem, recv_sem=rsem,
            device_id=device, device_id_type=MESH,
        ).start()

    def awaits(ref, sem):
        return pltpu.make_async_remote_copy(
            src_ref=ref, dst_ref=ref, send_sem=sem, recv_sem=sem,
            device_id=dev(x, y, z, 1 - c), device_id_type=MESH,
        )

    def arrived(ref, sem):
        awaits(ref, sem).wait_recv()

    barrier = pltpu.get_barrier_semaphore()
    peers = [dev(x, y, at_z(o), c) for o in (1, -1, 2, -2)]
    peers += [dev(from_x(g), y, z, c_) for g in range(1, nx) for c_ in range(nc)]
    peers += [dev(x, y, z, 1 - c)]
    peers += [dev(x, at_y(o), z, c) for o in range(1, ny)]
    for peer in peers:
        pl.semaphore_signal(barrier, inc=1, device_id=peer, device_id_type=MESH)

    own = pl.ds(place(0), tile)
    mine = pltpu.make_async_copy(
        tok_hbm.at[:, pl.ds(pl.multiple_of(y * quarter, 128), quarter)],
        zbuf.at[own, pl.ds(0, quarter)], w_sem.at[3],
    )
    names = [
        pltpu.make_async_copy(ids_hbm, ids_ref, w_sem.at[4]),
        pltpu.make_async_copy(logits_hbm, logits_ref, w_sem.at[5]),
    ]
    for copy in names:
        copy.start()
    mine.start()
    for copy in names:
        copy.wait()
    scores = 1.0 / (1.0 + jnp.exp(-logits_ref[...]))
    wts = ROUTE_SCALE * scores / jnp.sum(scores, axis=0, keepdims=True)
    lane = lax.broadcasted_iota(jnp.int32, (top, 128), 1)
    sub = lax.broadcasted_iota(jnp.int32, (top, 128), 0)
    put_id = (lane == sub).astype(BF16)
    put_w = (lane == sub + top).astype(BF16)
    across = (((0,), (0,)), ((), ()))
    meta = lax.dot_general(
        ids_ref[...].astype(F32).astype(BF16), put_id, across, preferred_element_type=F32
    ) + lax.dot_general(wts.astype(BF16), put_w, across, preferred_element_type=F32)
    zbuf[own, quarter : quarter + 128] = meta.astype(BF16)

    loads = [
        pltpu.make_async_copy(s.at[0], d, w_sem.at[i])
        for i, (s, d) in enumerate(((wg_hbm, wg), (wu_hbm, wu), (wd_hbm, wd)))
    ]
    for load in loads:
        load.start()
    mine.wait()
    pl.semaphore_wait(barrier, len(peers))

    def zslot(d, k):
        return (0 if d > 0 else 1) * steps + (k - 1)

    def ready(k):
        return min(k - 1, far)

    def gather_send(k, d):
        o = -d * 2 * (k - 1)
        for hop in (2, 1):
            if hop == 2 and d < 0 and k == steps:
                continue
            rsem = zag_r.at[zslot(d, k)] if hop == 2 else zag_one.at[ready(k)]
            send(
                zbuf.at[pl.ds(place(o), tile), :], zbuf.at[pl.ds(place(o - d * hop), tile), :],
                zag_s, rsem, dev(x, y, at_z(d * hop), c),
            )

    def gather_step(k):
        for d in (1, -1):
            if d > 0 or k < steps:
                arrived(zbuf.at[pl.ds(0, tile), :], zag_r.at[zslot(d, k)])
            if k < steps:
                gather_send(k + 1, d)

    def gather_rest(h):
        count = sum(ready(k) == h for k in range(1, steps + 1))
        arrived(zbuf.at[pl.ds(0, 2 * count * tile), :], zag_one.at[h])

    def routes(h):
        first, col = tokens_of(h)
        pick = (
            lax.broadcasted_iota(jnp.int32, (2 * top, 128), 0)
            == lax.broadcasted_iota(jnp.int32, (2 * top, 128), 1)
        ).astype(BF16)
        by_token = lax.dot_general(
            pick, zbuf[first : first + col, quarter : quarter + 128],
            (((1,), (1,)), ((), ())), preferred_element_type=F32,
        )
        lanes = nx * nc
        j = lax.broadcasted_iota(jnp.int32, (lanes, col), 0)
        jg, jc = lax.div(j, nc), lax.rem(j, nc)
        off = jnp.zeros_like(jg)
        for g, o in enumerate(offsets):
            off = jnp.where(jg == g, nx - o, off)
        expert = ((lax.rem(x + off, nx) * nz + z) * nc + jc).astype(F32)
        named = jnp.zeros((lanes, col), F32)
        weight = jnp.zeros((lanes, col), F32)
        for k in range(top):
            hit = by_token[k : k + 1, :] == expert
            named = jnp.where(hit, 1.0, named)
            weight = jnp.where(hit, by_token[top + k : top + k + 1, :], weight)
        t_row = lax.broadcasted_iota(jnp.int32, (col, col), 0)
        t_col = lax.broadcasted_iota(jnp.int32, (col, col), 1)
        before = ((t_row < t_col) & (lax.div(t_row, tile) == lax.div(t_col, tile))).astype(BF16)
        rank = jnp.dot(named.astype(BF16), before, preferred_element_type=F32)
        return jnp.where(named > 0.5, rank, -1.0), weight

    def unit_of(h, g):
        return [g in unit for unit in units[h]].index(True)

    def select(h, g, rank, weight):
        first, col = tokens_of(h)
        s_row = lax.broadcasted_iota(jnp.int32, (slots[h], col), 0)
        s_col = lax.broadcasted_iota(jnp.int32, (slots[h], col), 1)
        in_block = lax.div(s_row, CAP) == lax.div(s_col, tile)
        want = jnp.where(in_block, lax.rem(s_row, CAP).astype(F32), -2.0)
        recv = x_r.at[index(h, unit_of(h, g))]
        chosen = []
        for c_ in range(nc):
            i = g * nc + c_
            hit = rank[i : i + 1, :] == want
            chosen.append(jnp.where(hit, 1.0, 0.0).astype(BF16))
            swbuf[pl.ds(base(h, g, c_), slots[h]), 0:col] = jnp.where(
                hit, weight[i : i + 1, :], 0.0
            ).astype(BF16)
        xsend[pl.ds(base(h, g, 0), both[h]), :] = jnp.dot(
            jnp.concatenate(chosen, axis=0), zbuf[first : first + col, 0:quarter],
            preferred_element_type=F32,
        ).astype(BF16)
        land = ybuf.at[y, rows(base(h, g, c), slots[h]), :]
        if g > 0:
            for c_ in range(nc):
                send(
                    xsend.at[pl.ds(base(h, g, c_), slots[h]), :], land, x_s,
                    recv, dev(to_x(g), y, z, c_),
                )
        else:
            other = 1 - c
            send(
                xsend.at[rows(base(h, g, other), slots[h]), :], land, x_s,
                recv, dev(x, y, z, other),
            )
            here = rows(base(h, g, c), slots[h])
            ybuf[y, here, :] = xsend[here, :]

    def x_wait(h, u):
        start, size = span(h, u)
        size = slots[h] if u == home(h) else size
        arrived(ybuf.at[y, pl.ds(start, size), :], x_r.at[index(h, u)])

    def spread(h, u):
        x_wait(h, u)
        start, size = span(h, u)
        block = ybuf.at[y, pl.ds(start, size), :]
        for d in (1, -1):
            send(block, block, y1_s, y1_r.at[index(h, u)], dev(x, at_y(d), z, c))

    def forward(h, u):
        start, size = span(h, u)
        arrived(ybuf.at[pl.ds(0, 2), pl.ds(start, size), :], y1_r.at[index(h, u)])
        for n, d in enumerate((1, -1)):
            block = ybuf.at[at_y(-d), pl.ds(start + n * size // 2, size // 2), :]
            send(block, block, y2_s, y2_r.at[index(h, u)], dev(x, at_y(d), z, c))

    def y_wait(h, u):
        arrived(ybuf.at[0, pl.ds(*span(h, u)), :], y2_r.at[index(h, u)])

    def experts(start, size):
        here = pl.ds(start, size)
        gate = jnp.zeros((size, wg.shape[1]), F32)
        upper = jnp.zeros((size, wg.shape[1]), F32)
        for q in range(ny):
            piece = ybuf[q, here, :]
            deep = pl.ds(q * quarter, quarter)
            gate += jnp.dot(piece, wg[deep, :], preferred_element_type=F32)
            upper += jnp.dot(piece, wu[deep, :], preferred_element_type=F32)
        hidden = (gate / (1.0 + jnp.exp(-gate)) * upper).astype(BF16)
        for q in range(ny):
            obuf[q, here, :] = jnp.dot(
                hidden, wd[:, q * quarter : (q + 1) * quarter], preferred_element_type=F32
            ).astype(BF16)

    def compute(h, u):
        y_wait(h, u)
        experts(*span(h, u))

    def compute_all(h):
        for u in range(home(h)):
            y_wait(h, u)
        start, _ = span(h, 0)
        experts(start, (nx - 1) * both[h])

    def compute_home():
        for h in range(len(parts)):
            y_wait(h, home(h))
        experts(0, home_rows)
        for h in range(len(parts)):
            other = 1 - c
            send(
                obuf.at[:, rows(base(h, 0, other), slots[h]), :],
                rbuf0.at[:, rows(base(h, 0, c), slots[h]), :],
                home_s, b_r.at[index(h, home(h))], dev(x, y, z, other),
            )
            here = rows(base(h, 0, c), slots[h])
            for q in range(ny):
                rbuf0[q, here, :] = obuf[q, here, :]

    def combine_home():
        for h in range(len(parts)):
            arrived(rbuf0.at[:, pl.ds(base(h, 0, 0), slots[h]), :], b_r.at[index(h, home(h))])
            here = pl.ds(base(h, 0, 0), both[h])
            first, col = tokens_of(h)
            for o in range(ny):
                term = lax.dot_general(
                    swbuf[here, 0:col], rbuf0[at_y(o), here, :], across, preferred_element_type=F32
                )
                if o == 0:
                    part[first : first + col, :] = term
                else:
                    part0[first : first + col, (o - 1) * quarter : o * quarter] = term

    def give_one(h, u):
        start, size = span(h, u)
        for n, d in enumerate((1, -1)):
            send(
                obuf.at[at_y(2), pl.ds(start + n * size // 2, size // 2), :],
                r1buf.at[n, pl.ds(start // 2, size // 2), :],
                p1_s, p1_r.at[index(h, u)], dev(x, at_y(d), z, c),
            )

    def give_two(h, u):
        start, size = span(h, u)
        arrived(r1buf.at[:, pl.ds(start // 2, size // 2), :], p1_r.at[index(h, u)])
        for n, d in enumerate((1, -1)):
            here = pl.ds(start + n * size // 2, size // 2)
            q = at_y(d)
            got = r1buf[n, pl.ds(start // 2, size // 2), :]
            obuf[q, here, :] = (obuf[q, here, :].astype(F32) + got.astype(F32)).astype(BF16)
            here = pl.ds(start, size)
            send(
                obuf.at[q, here, :], r2buf.at[n, here, :],
                p2_s, p2_r.at[index(h, u)], dev(x, at_y(d), z, c),
            )

    def give_back(h, u):
        here = pl.ds(*span(h, u))
        arrived(r2buf.at[:, here, :], p2_r.at[index(h, u)])
        total = obuf[y, here, :].astype(F32) + r2buf[0, here, :].astype(F32)
        xret[here, :] = (total + r2buf[1, here, :].astype(F32)).astype(BF16)
        for g in units[h][u]:
            land = rbuf.at[rows(base(h, g, c), slots[h]), :]
            for c_ in range(nc):
                send(
                    xret.at[pl.ds(base(h, g, c_), slots[h]), :], land, b_s,
                    b_r.at[index(h, u)], dev(from_x(g), y, z, c_),
                )

    def combine(h, u):
        here = pl.ds(*span(h, u))
        first, col = tokens_of(h)
        arrived(rbuf.at[here, :], b_r.at[index(h, u)])
        part[first : first + col, :] += lax.dot_general(
            swbuf[here, 0:col], rbuf[here, :], across, preferred_element_type=F32
        )

    reach = nz // 2

    def reducer(source, src, dst, ssem, rsem):
        def block_of(o):
            return source[pl.ds(place(o), tile), :]

        def zsend(d, k, hop, value):
            n = zslot(d, k)
            src[n, hop - 1] = value.astype(BF16)
            send(src.at[n, hop - 1], dst.at[n, hop - 1], ssem, rsem.at[n], dev(x, y, at_z(d * hop), c))

        def zget(d, k):
            n = zslot(d, k)
            if d < 0 and k == 1:
                arrived(dst.at[n, 0], rsem.at[n])
                return dst[n, 0].astype(F32)
            arrived(dst.at[n], rsem.at[n])
            return dst[n, 0].astype(F32) + dst[n, 1].astype(F32)

        def own_hop(k):
            if k == 1:
                zsend(1, 1, 2, block_of(reach))
            for d in (1, -1):
                zsend(d, k, 1, block_of(d * (reach + 1 - 2 * k)))

        def next_hop(k):
            for d in (1, -1):
                zsend(d, k + 1, 2, block_of(d * (reach - 2 * k)) + zget(d, k))

        def finish():
            return block_of(0) + zget(1, steps) + zget(-1, steps)

        return own_hop, next_hop, finish, block_of, zget

    own_hop, next_hop, _, block_of, zget = reducer(part, zs, zr, zrs_s, zrs_r)
    wide_own, wide_next, wide_finish, _, _ = reducer(part0, ws, wr, wrs_s, wrs_r)

    def wide_step(k):
        if k < steps:
            wide_next(k)
            wide_own(k + 1)

    def choose(h):
        rank, weight = routes(h)
        for g in range(nx):
            select(h, g, rank, weight)

    direct = nz // 4

    count = out_ref.shape[0]

    def straight(o):
        value = block_of(o)
        if abs(o) == direct:
            value = value + zget(1 if o > 0 else -1, mid)
        n = (o if o > 0 else direct - o) - 1 if o else 2 * direct
        for q in range(ny):
            ds[n, q] = value[q * count : (q + 1) * count, :].astype(BF16)
        for r in range(ny) if o else range(1, ny):
            send(
                ds.at[n, at_y(r)], dr.at[y, n], d_s if o else o_s, d_r.at[0 if o else 1],
                dev(x, at_y(r), at_z(o), c),
            )
        if o == 0:
            dr[y, n] = ds[n, y]

    def share_wide():
        wide = wide_finish()
        for q in range(ny):
            fsend[q] = wide[q * count : (q + 1) * count, :].astype(BF16)
        for r in (2, 1, 3):
            send(fsend.at[at_y(r)], frecv.at[y], f_s, f_r.at[0], dev(x, at_y(r), z, c))
        frecv[y] = fsend[y]

    def gathered(j):
        where = at_y(j)
        total = dr[where, 2 * direct].astype(F32)
        for r in range(ny):
            o = (j - r) % ny
            if o:
                total += frecv[at_y(r), :, (o - 1) * quarter : o * quarter].astype(F32)
        for n in range(2 * direct):
            total += dr[where, n].astype(F32)
        return total.astype(BF16)

    near, between = 0, range(1, far)
    outer = range(len(units[far]) - 1)
    for d in (1, -1):
        gather_send(1, d)
    gather_step(1)
    gather_rest(near)
    choose(near)
    spread(near, home(near))
    for h in between:
        gather_step(h + 1)
    spread(near, 0)
    for h in between:
        gather_rest(h)
        choose(h)
        spread(h, home(h))
    for u in outer[1:]:
        spread(near, u)
    forward(near, home(near))
    for k in range(far + 1, steps):
        gather_step(k)
    for h in between:
        spread(h, 0)
    gather_step(steps)
    gather_rest(far)
    choose(far)
    forward(near, 0)
    spread(far, home(far))
    for u in outer[1:]:
        forward(near, u)
        for h in between:
            spread(h, u)
    for h in between:
        forward(h, home(h))
        forward(h, 0)
    forward(far, home(far))
    for u in outer[1:]:
        for h in between:
            forward(h, u)
    for u in outer:
        spread(far, u)
    for load in loads:
        load.wait()
    for h in range(far):
        compute_all(h)
    compute_home()
    forward(far, 0)
    combine_home()
    wide_own(1)
    for u in outer[1:]:
        forward(far, u)
    for h in between:
        for u in outer:
            give_one(h, u)
    for u in outer:
        compute(far, u)
        give_one(far, u)
    for u in outer:
        give_one(near, u)
    wide_step(1)
    for u in outer:
        give_two(far, u)
    for h in range(far - 1, -1, -1):
        for u in outer:
            give_two(h, u)
    wide_step(2)
    for u in outer:
        give_back(far, u)
    for k in range(3, steps):
        wide_step(k)
    for h in between:
        for u in outer:
            give_back(h, u)
    for u in outer:
        combine(far, u)
    for k in range(1, mid + 1):
        own_hop(k)
    for u in outer:
        give_back(near, u)
    for k in range(1, mid):
        next_hop(k)
    for h in between:
        for u in outer:
            combine(h, u)
        for o in (3, -3, 2):
            straight(o)
    share_wide()
    for u in outer:
        combine(near, u)
    for o in range(2 if nz > 8 else 1, 0, -1):
        straight(-o)
    straight(1)
    straight(0)
    for o in (direct, -direct):
        straight(o)
    arrived(frecv.at[pl.ds(0, ny - 1)], f_r.at[0])
    arrived(dr.at[pl.ds(0, ny - 1), 2 * direct], d_r.at[1])
    arrived(dr.at[:, pl.ds(0, 2 * direct)], d_r.at[0])
    for j in range(ny):
        piece = pl.ds(pl.multiple_of(at_y(j) * quarter, 128), quarter)
        out_ref[:, piece] = gathered(j)

    every = ybuf.shape[1]
    moved = every - home_rows
    sent = sum(slots)
    for sem, ref in (
        (zag_s, zbuf.at[pl.ds(0, (nz - 1) * tile), :]),
        (x_s, xsend.at[pl.ds(0, (nx * nc - 1) * sent), :]),
        (y1_s, ybuf.at[pl.ds(0, 2), :, :]),
        (y2_s, ybuf.at[0]),
        (p1_s, ybuf.at[0, pl.ds(0, moved), :]),
        (p2_s, r2buf.at[:, pl.ds(0, moved), :]),
        (b_s, xret.at[pl.ds(0, moved), :]),
        (home_s, rbuf0.at[:, pl.ds(0, sent), :]),
        (zrs_s, ybuf.at[0, pl.ds(0, (4 * mid - 1) * tile), :]),
        (d_s, ds.at[pl.ds(0, 2 * direct)]),
        (o_s, ds.at[0, pl.ds(0, ny - 1)]),
        (wrs_s, part0.at[pl.ds(0, (nz - 1) * tile // 2), :]),
        (f_s, fsend.at[pl.ds(0, ny - 1)]),
    ):
        awaits(ref, sem).wait_send()


def on_device(tokens, expert_ids, route_logits, expert_gate, expert_up, expert_down):
    n_ep, ny = lax.axis_size("ep"), N_DP
    nx, nc = CHIPS_X, CORES
    nz = n_ep // (nx * nc)
    tile, width = tokens.shape
    hidden = expert_gate.shape[2]
    quarter = width // ny
    col, slots = nz * tile, nz * CAP
    every = nx * nc * slots
    steps = nz // 4
    dma = pltpu.SemaphoreType.DMA
    vmem = pl.BlockSpec(memory_space=pltpu.VMEM)
    hbm = pl.BlockSpec(memory_space=pl.ANY)
    flops = 6 * every * width * hidden
    units = 9
    home = 2 * nc * slots // 2
    return pl.pallas_call(
        functools.partial(kernel, nx, nz),
        out_shape=jax.ShapeDtypeStruct((tile // ny, width), BF16),
        in_specs=[hbm] * 6,
        out_specs=vmem,
        scratch_shapes=[
            pltpu.VMEM(expert_ids.shape[::-1], jnp.int32),
            pltpu.VMEM(expert_ids.shape[::-1], F32),
            pltpu.VMEM((width, hidden), BF16),
            pltpu.VMEM((width, hidden), BF16),
            pltpu.VMEM((hidden, width), BF16),
            pltpu.VMEM((col, quarter + 128), BF16),
            pltpu.VMEM((every, col // 2), BF16),
            pltpu.VMEM((every, quarter), BF16),
            pltpu.VMEM((ny, every, quarter), BF16),
            pltpu.VMEM((ny, every, quarter), BF16),
            pltpu.VMEM((2, every // 2, quarter), BF16),
            pltpu.VMEM((2, every, quarter), BF16),
            pltpu.VMEM((every, quarter), BF16),
            pltpu.VMEM((every, quarter), BF16),
            pltpu.VMEM((ny, home, quarter), BF16),
            pltpu.VMEM((col, quarter), F32),
            pltpu.VMEM((col, width - quarter), F32),
            pltpu.VMEM((2 * steps, 2, tile, quarter), BF16),
            pltpu.VMEM((2 * steps, 2, tile, quarter), BF16),
            pltpu.VMEM((2 * steps, 2, tile, width - quarter), BF16),
            pltpu.VMEM((2 * steps, 2, tile, width - quarter), BF16),
            pltpu.VMEM((2 * steps + 1, ny, tile // ny, quarter), BF16),
            pltpu.VMEM((ny, 2 * steps + 1, tile // ny, quarter), BF16),
            pltpu.VMEM((ny, tile // ny, width - quarter), BF16),
            pltpu.VMEM((ny, tile // ny, width - quarter), BF16),
            dma((6,)),
            dma((13,)),
            dma((2 * steps,)), dma((3,)),
            dma((units,)), dma((units,)), dma((units,)), dma((units,)), dma((units,)), dma((units,)),
            dma((2 * steps,)), dma((2 * steps,)), dma((1,)), dma((2,)),
        ],
        compiler_params=pltpu.CompilerParams(
            collective_id=0, has_side_effects=True, vmem_limit_bytes=56 * 1024 * 1024
        ),
        cost_estimate=pl.CostEstimate(flops=flops, bytes_accessed=8 << 20, transcendentals=0),
    )(expert_ids.T, route_logits.T, tokens, expert_gate, expert_up, expert_down)


def solution(mesh):
    placed = (
        P("ep", None),
        P("ep", None),
        P("ep", None),
        P("ep", None, "dp"),
        P("ep", None, "dp"),
        P("ep", "dp", None),
    )
    return jax.shard_map(
        on_device, mesh=mesh, in_specs=placed, out_specs=P(("ep", "dp"), None), check_vma=False
    )
```
